128 devices in a mesh: gx: 4 (over x), gy: 4 (over z), gz: 8 (over y, core).
Axes of the slice: x: 4, y: 4, z: 4, core: 2. Of those that a mesh axis runs over, the one named last changes fastest.
Arguments:
- right_side: float32 [3, 32, 128, 1024], P(None, 'gx', 'gy', 'gz'), may hold values from -6 to 6
- mass_coef: float32 [3, 32, 128, 1024], P(None, 'gx', 'gy', 'gz'), may hold values from 0.3 to 3
- curl_coef: float32 [3, 32, 128, 1024], P(None, 'gx', 'gy', 'gz'), may hold values from 0.5 to 5
Outputs:
- solution: float32 [3, 32, 128, 1024], P(None, 'gx', 'gy', 'gz')
- residual: float32 [3, 32, 128, 1024], P(None, 'gx', 'gy', 'gz')
The draws below stay inside these ranges and needn't reach their ends.
All inputs are finite; a program needn't handle non-finite values.
Results may differ from the reference program's by a relative error of at most 0.0003.
Values sent between devices are 32-bit elements; how exact they have to be, the bound alone decides.
No kernel may reach another device: no remote copies, remote signals or barrier semaphores. Data moves between devices by JAX's collectives and lax.ppermute only.
A program may use at most 64 MiB of HBM per device.

```python
import math
import jax
import jax.numpy as jnp
from jax import lax

ITERS = 4
NX = 32
NY = 128
NZ = 1024


def block_levels(own_key, dims, split, smallest, largest):
    gain = 1.0
    for axis_at, parts in split:
        draws = jax.random.uniform(jax.random.fold_in(jax.random.fold_in(own_key, 6), axis_at), (parts,), jnp.float32, smallest / len(split), largest / len(split))
        gain = gain * jnp.repeat(jnp.exp(draws), dims[axis_at] // parts).reshape((-1,) + (1,) * (len(dims) - 1 - axis_at))
    return gain


def bell_draw(own_key, extent, spread, limit, split=(), held_as=jnp.bfloat16):
    loudness = block_levels(own_key, extent, split, -0.22, 0.18) if split else 1.0
    result = jax.random.normal(own_key, extent, jnp.float32) * spread * loudness
    return jnp.minimum(jnp.maximum(result, -limit), limit).astype(held_as)


def setup_inputs(seed: int = 0) -> dict:
    keys = jax.random.split(jax.random.key(seed), 4)
    return {
        "right_side": bell_draw(keys[0], (3, NX, NY, NZ), 1.0, 6.0, ((1, 4), (2, 4), (3, 8)), jnp.float32),
        "mass_coef": jnp.clip(jnp.exp(math.log(3.0) - 2.3025851 * jax.random.uniform(keys[1], (3, NX, NY, NZ), jnp.float32) ** block_levels(keys[1], (3, NX, NY, NZ), ((1, 4), (2, 4), (3, 8)), -0.2, 0.2)), 0.3, 3.0),
        "curl_coef": jnp.clip(jnp.exp(math.log(5.0) - 2.3025851 * jax.random.uniform(keys[2], (3, NX, NY, NZ), jnp.float32) ** block_levels(keys[2], (3, NX, NY, NZ), ((1, 4), (2, 4), (3, 8)), -0.2, 0.2)), 0.5, 5.0),
    }


def region(values, start, size):
    return lax.slice(values, tuple(start), tuple(s + n for s, n in zip(start, size)))


def shifted(values, size, base, dim, delta):
    start = [base, base, base]
    if dim >= 0:
        start[dim] = start[dim] + delta
    return region(values, start, size)


def apply_curl(padded, sigma_pad, mu_pad):
    inner = tuple(n - 2 for n in padded.shape[1:])
    faces = tuple(n - 1 for n in padded.shape[1:])
    along_x, along_y, along_z = padded[0], padded[1], padded[2]

    def face_at(values, dim):
        return shifted(values, faces, 0, dim, 1)

    def out_at(values, dim):
        return shifted(values, inner, 1, dim, -1)

    flux_x = (face_at(along_z, 1) - face_at(along_z, -1)) - (face_at(along_y, 2) - face_at(along_y, -1))
    flux_y = (face_at(along_x, 2) - face_at(along_x, -1)) - (face_at(along_z, 0) - face_at(along_z, -1))
    flux_z = (face_at(along_y, 0) - face_at(along_y, -1)) - (face_at(along_x, 1) - face_at(along_x, -1))
    weighted_x = face_at(mu_pad[0], -1) * flux_x
    weighted_y = face_at(mu_pad[1], -1) * flux_y
    weighted_z = face_at(mu_pad[2], -1) * flux_z
    result_x = (out_at(weighted_y, 2) - out_at(weighted_y, -1)) - (out_at(weighted_z, 1) - out_at(weighted_z, -1)) + out_at(sigma_pad[0], -1) * out_at(along_x, -1)
    result_y = (out_at(weighted_z, 0) - out_at(weighted_z, -1)) - (out_at(weighted_x, 2) - out_at(weighted_x, -1)) + out_at(sigma_pad[1], -1) * out_at(along_y, -1)
    result_z = (out_at(weighted_x, 1) - out_at(weighted_x, -1)) - (out_at(weighted_y, 0) - out_at(weighted_y, -1)) + out_at(sigma_pad[2], -1) * out_at(along_z, -1)
    return jnp.stack([result_x, result_y, result_z])


def edge_inverse(sigma_pad, mu_pad):
    inner = tuple(n - 2 for n in sigma_pad.shape[1:])

    def out_at(values, dim):
        return shifted(values, inner, 1, dim, -1)

    diag_x = out_at(sigma_pad[0], -1) + out_at(mu_pad[1], -1) + out_at(mu_pad[1], 2) + out_at(mu_pad[2], -1) + out_at(mu_pad[2], 1)
    diag_y = out_at(sigma_pad[1], -1) + out_at(mu_pad[2], -1) + out_at(mu_pad[2], 0) + out_at(mu_pad[0], -1) + out_at(mu_pad[0], 2)
    diag_z = out_at(sigma_pad[2], -1) + out_at(mu_pad[0], -1) + out_at(mu_pad[0], 1) + out_at(mu_pad[1], -1) + out_at(mu_pad[1], 0)
    return 1.0 / jnp.stack([diag_x, diag_y, diag_z])


def node_inverse(sigma_pad):
    nodes = tuple(n - 1 for n in sigma_pad.shape[1:])
    total = jnp.zeros(nodes, jnp.float32)
    for comp in range(3):
        total = total + shifted(sigma_pad[comp], nodes, 1, -1, 0) + shifted(sigma_pad[comp], nodes, 1, comp, -1)
    return 1.0 / total


def apply_aux(padded, edge_inv, node_inv):
    nodes = tuple(n - 1 for n in padded.shape[1:])
    inner = tuple(n - 2 for n in padded.shape[1:])
    nodal = jnp.zeros(nodes, jnp.float32)
    for comp in range(3):
        nodal = nodal + shifted(padded[comp], nodes, 1, comp, -1) - shifted(padded[comp], nodes, 1, -1, 0)
    potential = nodal * node_inv
    gradient = jnp.stack([shifted(potential, inner, 0, comp, 1) - shifted(potential, inner, 0, -1, 0) for comp in range(3)])
    return padded[:, 1:-1, 1:-1, 1:-1] * edge_inv + gradient


def wrap_pad(values):
    return jnp.pad(values, ((0, 0), (1, 1), (1, 1), (1, 1)), mode="wrap")


def reference(right_side, mass_coef, curl_coef):
    sigma_pad = wrap_pad(mass_coef)
    mu_pad = wrap_pad(curl_coef)
    edge_inv = edge_inverse(sigma_pad, mu_pad)
    node_inv = node_inverse(sigma_pad)

    def pair(values):
        precond = apply_aux(wrap_pad(values), edge_inv, node_inv)
        return precond, apply_curl(wrap_pad(precond), sigma_pad, mu_pad)

    solution = jnp.zeros_like(right_side)
    residual = right_side
    precond_res, image_res = pair(residual)
    direction = jnp.zeros_like(right_side)
    dir_image = jnp.zeros_like(right_side)
    dir_precond = jnp.zeros_like(right_side)
    dir_double = jnp.zeros_like(right_side)
    gamma_old = jnp.float32(1.0)
    alpha_old = jnp.float32(1.0)
    for iteration in range(ITERS):
        gamma_now = jnp.sum(residual * precond_res)
        delta_now = jnp.sum(image_res * precond_res)
        precond_img, image_img = pair(image_res)
        if iteration == 0:
            beta_now = jnp.float32(0.0)
            alpha_now = gamma_now / delta_now
        else:
            beta_now = gamma_now / gamma_old
            alpha_now = gamma_now / (delta_now - beta_now * gamma_now / alpha_old)
        dir_double = image_img + beta_now * dir_double
        dir_precond = precond_img + beta_now * dir_precond
        dir_image = image_res + beta_now * dir_image
        direction = precond_res + beta_now * direction
        solution = solution + alpha_now * direction
        residual = residual - alpha_now * dir_image
        precond_res = precond_res - alpha_now * dir_precond
        image_res = image_res - alpha_now * dir_double
        gamma_old = gamma_now
        alpha_old = alpha_now
    return solution, residual
```

```python
import jax
import jax.numpy as jnp
from jax import lax
from jax.experimental import pallas as pl
from jax.experimental.pallas import tpu as pltpu
from jax.sharding import PartitionSpec as P


HALO = 4
X, Y = 16, 64
OWN = 16
LO, ROWS = 8, 48
WEIGHT = (0.0, 0.5, 0.25, 0.25, 0.25)
VMEM = pl.BlockSpec(memory_space=pltpu.VMEM)


def params(mib):
    return pltpu.CompilerParams(vmem_limit_bytes=mib * 1024 * 1024)


def cost(ns_like):
    return pl.CostEstimate(flops=ns_like, bytes_accessed=1 << 20, transcendentals=0)


def pick(refs, comp):
    return refs[comp // 3], comp % 3


def pack_x(right, mass, curl, low, high):
    refs = (right, mass, curl)
    for comp in range(9):
        ref, c = pick(refs, comp)
        low[comp] = ref[c, 0:4]
        high[comp] = ref[c, 4:8]
    high[4, 0] = mass[1, 4] + curl[2, 3]
    high[5, 0] = mass[2, 4] + curl[1, 3]


def row_tile(refs, below, above, comp, x, y):
    if x < 4:
        return below[comp, x, y : y + 8]
    if x >= 12:
        return above[comp, x - 12, y : y + 8]
    ref, c = pick(refs, comp)
    return ref[c, x - 4, y : y + 8]


def pack_y(right, mass, curl, below, above, low, high):
    refs = (right, mass, curl)
    sub = lax.broadcasted_iota(jnp.int32, (8, 128), 0)
    for comp in range(9):
        for p in range(8):
            a = row_tile(refs, below, above, comp, p, 0)
            b = row_tile(refs, below, above, comp, p + 8, 0)
            low[comp, p] = jnp.where(sub < 4, a, pltpu.roll(b, 4, 0))
            pair = []
            for x in (p, p + 8):
                t = row_tile(refs, below, above, comp, x, 24)
                other = {3: 8, 5: 6}.get(comp)
                if other is not None:
                    t = t + jnp.where(sub == 4, pltpu.roll(row_tile(refs, below, above, other, x, 24), 1, 0), 0.0)
                pair.append(t)
            high[comp, p] = jnp.where(sub < 4, pltpu.roll(pair[0], 4, 0), pair[1])


def halo_tiles(ylow, yhigh, comp, x, sub):
    p = x % 8
    lower, upper = ylow[comp, p], yhigh[comp, p]
    if x < 8:
        lower = pltpu.roll(lower, 4, 0)
    else:
        upper = pltpu.roll(upper, 4, 0)
    return jnp.where(sub >= 4, lower, 0.0), jnp.where(sub < 4, upper, 0.0)


def pack_z(right, mass, curl, below, above, ylow, yhigh, low, high):
    refs = (right, mass, curl)
    sub = lax.broadcasted_iota(jnp.int32, (8, 128), 0)
    lane = lax.broadcasted_iota(jnp.int32, (8, 128), 1)

    def tile(comp, x, o):
        if o == 0:
            return halo_tiles(ylow, yhigh, comp, x, sub)[0]
        if o == 5:
            return halo_tiles(ylow, yhigh, comp, x, sub)[1]
        return row_tile(refs, below, above, comp, x, 8 * (o - 1))

    for comp in range(9):
        other = {3: 7, 4: 6}.get(comp)
        for o in range(6):
            first = jnp.zeros((8, 128), jnp.float32)
            last = first
            for x in range(X):
                t = tile(comp, x, o)
                first = jnp.where((lane // 4) == 2 * x + 1, pltpu.roll(t, 8 * x + 4, 1), first)
                if other is not None:
                    t = t + jnp.where(lane == 124, pltpu.roll(tile(other, x, o), 1, 1), 0.0)
                last = jnp.where((lane // 4) == 2 * x, pltpu.roll(t, (8 * x + 4) % 128, 1), last)
            low[comp, 8 * o : 8 * o + 8] = first
            high[comp, 8 * o : 8 * o + 8] = last


def main(right, mass, curl, below, above, ylow, yhigh, zown_low, zown_high, zlow, zhigh,
         vectors, precond, partial,
         field, coef, diag, node, s, phi, g, fieldS, coefS, diagS, nodeS, sS, phiS, gS):
    f32 = jnp.float32
    sub = lax.broadcasted_iota(jnp.int32, (8, 128), 0)
    lane = lax.broadcasted_iota(jnp.int32, (ROWS, 128), 1)
    first_lane, last_lane = lane == 0, lane == 127

    for comp in range(9):
        ref, c = pick((right, mass, curl), comp)
        to = field.at[0, comp] if comp < 3 else coef.at[comp - 3]
        if comp >= 3:
            to[0] = jnp.zeros((Y, 128), f32)
        to[1:5, OWN : OWN + 32] = below[comp]
        to[5:13, OWN : OWN + 32] = ref[c]
        to[13:17, OWN : OWN + 32] = above[comp]
        for x in range(X):
            lower, upper = halo_tiles(ylow, yhigh, comp, x, sub)
            to[x + 1, OWN - 8 : OWN] = lower
            to[x + 1, OWN + 32 : OWN + 40] = upper
        toS = fieldS.at[0, comp] if comp < 3 else coefS.at[comp - 3]
        toS[0, LO : LO + ROWS] = zown_low[comp] + zlow[comp]
        toS[1, LO : LO + ROWS] = zown_high[comp] + zhigh[comp]

    def at(ref, dy=0):
        return ref[pl.ds(LO + dy, ROWS), :]

    def put(ref, value):
        ref[pl.ds(LO, ROWS), :] = value

    def z_up(value, strip, x):
        return jnp.where(last_lane, pltpu.roll(at(strip), 123 - 8 * x, 1), pltpu.roll(value, 127, 1))

    def z_down(value, strip, x):
        return jnp.where(first_lane, pltpu.roll(at(strip), 125 - 8 * x, 1), pltpu.roll(value, 1, 1))

    def diagonals(m, c, cy, cx, cz, mx, my, mz):
        d0 = m[0] + c[1] + cz[1] + c[2] + cy[2]
        d1 = m[1] + c[2] + cx[2] + c[0] + cz[0]
        d2 = m[2] + c[0] + cy[0] + c[1] + cx[1]
        dn = m[0] + mx + m[1] + my + m[2] + mz
        return 1.0 / d0, 1.0 / d1, 1.0 / d2, 1.0 / dn

    for t in range(2):
        m = [at(coefS.at[c, t]) for c in range(3)]
        c_ = [at(coefS.at[3 + c, t]) for c in range(3)]
        cy = [at(coefS.at[3 + c, t], -1) for c in range(3)]
        cx = [jnp.where(lane < 8, 0.0, pltpu.roll(v, 8, 1)) for v in c_]
        cz = [jnp.where(lane % 8 == 0, 0.0, pltpu.roll(v, 1, 1)) for v in c_]
        out = diagonals(m, c_, cy, cx, cz, pltpu.roll(m[0], 8, 1), at(coefS.at[1, t], -1), pltpu.roll(m[2], 1, 1))
        for c in range(3):
            put(diagS.at[c, t], out[c])
        put(nodeS.at[t], out[3])

    def setup(x, _):
        m = [at(coef.at[c, x + 1]) for c in range(3)]
        c_ = [at(coef.at[3 + c, x + 1]) for c in range(3)]
        cy = [at(coef.at[3 + c, x + 1], -1) for c in range(3)]
        cx = [at(coef.at[3 + c, x]) for c in range(3)]
        cz = [z_down(c_[c], coefS.at[3 + c, 0], x) for c in range(2)]
        out = diagonals(m, c_, cy, cx, cz, at(coef.at[0, x]), at(coef.at[1, x + 1], -1), z_down(m[2], coefS.at[2, 0], x))
        for c in range(3):
            put(diag.at[c, x + 1], out[c])
        put(node.at[x + 1], out[3])
        return 0

    lax.fori_loop(0, X, setup, 0)

    def fluxes(coefs, e, e0y, e0z, e1x, e1z, e2x, e2y):
        return (coefs[0] * ((e2y - e[2]) - (e1z - e[1])),
                coefs[1] * ((e0z - e[0]) - (e2x - e[2])),
                coefs[2] * ((e1x - e[1]) - (e0y - e[0])))

    def curl_back(gv, g0y, g0z, g1x, g1z, g2x, g2y):
        return ((g1z - gv[1]) - (g2y - gv[2]), (g2x - gv[2]) - (g0z - gv[0]), (g0y - gv[0]) - (g1x - gv[1]))

    for k in range(4):
        now, later, before = k % 3, (k + 1) % 3, (k + 2) % 3

        def advance(c, w, r, old):
            v = w - r
            return v if k == 0 else v - WEIGHT[k] * old

        for t in range(2):
            r = [at(fieldS.at[now, c, t]) for c in range(3)]
            q = ((pltpu.roll(r[0], 8, 1) - r[0]) + (at(fieldS.at[now, 1, t], -1) - r[1])) + (pltpu.roll(r[2], 1, 1) - r[2])
            put(phiS.at[t], q * at(nodeS.at[t]))
            for c in range(3):
                put(sS.at[c, t], r[c] * at(diagS.at[c, t]))
        for t in range(2):
            e = [at(sS.at[c, t]) for c in range(3)]
            out = fluxes([at(coefS.at[3 + c, t]) for c in range(3)], e,
                         at(sS.at[0, t], 1), pltpu.roll(e[0], 127, 1), pltpu.roll(e[1], 120, 1),
                         pltpu.roll(e[1], 127, 1), pltpu.roll(e[2], 120, 1), at(sS.at[2, t], 1))
            for c in range(3):
                put(gS.at[c, t], out[c])

        def first(x, _):
            r = [at(field.at[now, c, x + 1]) for c in range(3)]
            q = ((at(field.at[now, 0, x]) - r[0]) + (at(field.at[now, 1, x + 1], -1) - r[1])) + (
                z_down(r[2], fieldS.at[now, 2, 0], x) - r[2])
            put(phi.at[x + 1], q * at(node.at[x + 1]))
            for c in range(3):
                put(s.at[c, x + 1], r[c] * at(diag.at[c, x + 1]))
            return 0

        lax.fori_loop(k, 16 - k, first, 0)

        def second(x, _):
            e = [at(s.at[c, x + 1]) for c in range(3)]
            out = fluxes([at(coef.at[3 + c, x + 1]) for c in range(3)], e,
                         at(s.at[0, x + 1], 1), z_up(e[0], sS.at[0, 1], x), at(s.at[1, x + 2]),
                         z_up(e[1], sS.at[1, 1], x), at(s.at[2, x + 2]), at(s.at[2, x + 1], 1))
            for c in range(3):
                put(g.at[c, x + 1], out[c])
            return 0

        lax.fori_loop(k, 15 - k, second, 0)

        def third(x, own, sums):
            gv = [at(g.at[c, x + 1]) for c in range(3)]
            w = curl_back(gv, at(g.at[0, x + 1], -1), z_down(gv[0], gS.at[0, 0], x), at(g.at[1, x]),
                          z_down(gv[1], gS.at[1, 0], x), at(g.at[2, x]), at(g.at[2, x + 1], -1))
            p = at(phi.at[x + 1])
            up = (at(phi.at[x + 2]), at(phi.at[x + 1], 1), z_up(p, phiS.at[1], x))
            for c in range(3):
                u = at(s.at[c, x + 1]) + (up[c] - p)
                r = at(field.at[now, c, x + 1])
                old = None if k == 0 else at(field.at[before, c, x + 1])
                v = advance(c, w[c] + at(coef.at[c, x + 1]) * u, r, old)
                put(field.at[later, c, x + 1], v)
                if own:
                    u, r, v = (a[OWN - LO : OWN - LO + 32] for a in (u, r, v))
                    vectors[k, c, x - 4] = v
                    precond[k, c, x - 4] = u
                    ru, vu = r * u, v * u
                    sums = (sums[0] + ((ru[0:8] + ru[8:16]) + (ru[16:24] + ru[24:32])),
                            sums[1] + ((vu[0:8] + vu[8:16]) + (vu[16:24] + vu[24:32])))
            return sums

        def outside(x, carry):
            third(x, False, None)
            return carry

        zero = jnp.zeros((8, 128), f32)
        lax.fori_loop(k + 1, 4, outside, 0)
        sums = lax.fori_loop(4, 12, lambda x, carry: third(x, True, carry), (zero, zero))
        lax.fori_loop(12, 15 - k, outside, 0)
        for i in range(2):
            partial[2 * k + i] = sums[i]

        if k < 3:
            for t in range(2):
                gv = [at(gS.at[c, t]) for c in range(3)]
                w = curl_back(gv, at(gS.at[0, t], -1), pltpu.roll(gv[0], 1, 1), pltpu.roll(gv[1], 8, 1),
                              pltpu.roll(gv[1], 1, 1), pltpu.roll(gv[2], 8, 1), at(gS.at[2, t], -1))
                p = at(phiS.at[t])
                up = (pltpu.roll(p, 120, 1), at(phiS.at[t], 1), pltpu.roll(p, 127, 1))
                for c in range(3):
                    u = at(sS.at[c, t]) + (up[c] - p)
                    old = None if k == 0 else at(fieldS.at[before, c, t])
                    put(fieldS.at[later, c, t],
                        advance(c, w[c] + at(coefS.at[c, t]) * u, at(fieldS.at[now, c, t]), old))


def fold(partial, out):
    lane = lax.broadcasted_iota(jnp.int32, (1, 128), 1)
    row = jnp.zeros((1, 128), jnp.float32)
    for d in range(8):
        t = jnp.sum(partial[d], axis=0, keepdims=True)
        for shift in (64, 32, 16):
            t = t + pltpu.roll(t, shift, 1)
        row = jnp.where(lane // 16 == d, t, row)
    out[...] = jnp.broadcast_to(row, out.shape)


def finish(everyone, right, vectors, precond, solution_out, residual_out):
    total = jnp.sum(everyone[...], axis=0, keepdims=True)
    lane = lax.broadcasted_iota(jnp.int32, (1, 128), 1)
    dots = [jnp.broadcast_to(jnp.sum(jnp.where(lane // 16 == d, total, 0.0), axis=1, keepdims=True), (8, 128))
            for d in range(8)]
    size = [1.0] + [2.0 ** (1 - k) for k in range(1, 9)]
    moment = [dots[0], dots[1]]
    for k in range(1, 4):
        moment.append((dots[2 * k] * (2.0 / size[k] ** 2) - moment[0]) * size[2 * k])
        moment.append((dots[2 * k + 1] * (2.0 / (size[k] * size[k + 1])) - moment[1]) * size[2 * k + 1])
    row, earlier = moment, None
    alpha, beta = [row[1] / row[0]], [None]
    for k in range(1, 4):
        following = [None] * 8
        for l in range(k, 8 - k):
            t = row[l + 1] - alpha[k - 1] * row[l] + WEIGHT[l if l < 2 else 2] * row[l - 1]
            if k > 1:
                t = t - beta[k - 1] * earlier[l]
            following[l] = t
        alpha.append(following[k + 1] / following[k] - row[k] / row[k - 1])
        beta.append(following[k] / row[k - 1])
        row, earlier = following, row
    zero = jnp.zeros((8, 128), jnp.float32)
    older, newer = [zero] * 6, [zero + 1.0] + [zero] * 5
    value_older, value = zero, zero + 1.0
    weight = lambda l: WEIGHT[min(l, 2)]
    for k in range(4):
        nxt = []
        for l in range(6):
            t = -alpha[k] * newer[l]
            if l > 0:
                t = t + newer[l - 1]
            if l < 5:
                t = t + weight(l + 1) * newer[l + 1]
            if k > 0:
                t = t - beta[k] * older[l]
            nxt.append(t)
        step = (-1.0 - alpha[k]) * value
        if k > 0:
            step = step - beta[k] * value_older
        older, newer, value_older, value = newer, nxt, value, step
    inverse = 1.0 / value
    e = [newer[l] * inverse for l in range(5)]
    S = [None] * 4
    S[3] = -e[4]
    S[2] = -e[3] - S[3]
    S[1] = -e[2] - S[2] - weight(3) * S[3]
    S[0] = -e[1] - S[1] - weight(2) * S[2]
    e = [v[0:1] for v in e]
    S = [v[0:1] for v in S]

    def combine(x, _):
        for c in range(3):
            residual_out[c, x] = (e[0] * right[c, x] + e[1] * vectors[0, c, x]) + (
                e[2] * vectors[1, c, x] + e[3] * vectors[2, c, x]) + e[4] * vectors[3, c, x]
            solution_out[c, x] = (S[0] * precond[0, c, x] + S[1] * precond[1, c, x]) + (
                S[2] * precond[2, c, x] + S[3] * precond[3, c, x])
        return 0

    lax.fori_loop(0, 8, combine, 0)


def shape(*dims):
    return jax.ShapeDtypeStruct(dims, jnp.float32)


def call(kernel, outs, ins, mib, scratch=(), flops=1000000):
    return pl.pallas_call(
        kernel, out_shape=outs, in_specs=[VMEM] * len(ins), out_specs=jax.tree.map(lambda _: VMEM, outs),
        scratch_shapes=list(scratch), compiler_params=params(mib), cost_estimate=cost(flops))(*ins)


def exchange(low, high, axis):
    n = lax.axis_size(axis)
    up = [(i, (i + 1) % n) for i in range(n)]
    return lax.ppermute(high, axis, up), lax.ppermute(low, axis, [(j, i) for i, j in up])


def body(right, mass, curl):
    args = (right, mass, curl)
    low, high = call(pack_x, (shape(9, 4, 32, 128),) * 2, args, 8)
    args += exchange(low, high, "gx")
    low, high = call(pack_y, (shape(9, 8, 8, 128),) * 2, args, 12)
    args += exchange(low, high, "gy")
    low, high = call(pack_z, (shape(9, ROWS, 128),) * 2, args, 16)
    args += (low, high) + exchange(low, high, "gz")
    V = pltpu.VMEM
    f32 = jnp.float32
    vectors, precond, partial = call(
        main, (shape(4, 3, 8, 32, 128), shape(4, 3, 8, 32, 128), shape(8, 8, 128)), args, 46,
        [V((3, 3, 18, Y, 128), f32), V((6, 18, Y, 128), f32), V((3, 18, Y, 128), f32), V((18, Y, 128), f32),
         V((3, 18, Y, 128), f32), V((18, Y, 128), f32), V((3, 18, Y, 128), f32),
         V((3, 3, 2, Y, 128), f32), V((6, 2, Y, 128), f32), V((3, 2, Y, 128), f32), V((2, Y, 128), f32),
         V((3, 2, Y, 128), f32), V((2, Y, 128), f32), V((3, 2, Y, 128), f32)])
    axes = ("gx", "gy", "gz")
    devices = lax.axis_size(axes)
    (rows,) = call(fold, (shape(devices, 128),), (partial,), 4)
    everyone = lax.all_to_all(rows.reshape(devices, 1, 128), axes, 0, 0, tiled=True).reshape(devices, 128)
    return call(finish, (shape(3, 8, 32, 128),) * 2, (everyone, right, vectors, precond), 16)


def solution(mesh):
    spec = P(None, "gx", "gy", "gz")
    return jax.shard_map(body, mesh=mesh, in_specs=(spec,) * 3, out_specs=(spec,) * 2, check_vma=False)
```

```python
import jax
import jax.numpy as jnp
from jax import lax
from jax.experimental import pallas as pl
from jax.experimental.pallas import tpu as pltpu
from jax.sharding import PartitionSpec as P


X, Y = 24, 64
OFF, OWN = 4, 16
LO, ROWS = 8, 48
WEIGHT = (0.0, 0.5, 0.25, 0.25, 0.25)
VMEM = pl.BlockSpec(memory_space=pltpu.VMEM)


def load(source, own, low, high):
    def move(c, _):
        for to, x in ((low, 0), (high, 4)):
            value = source[c, x : x + 4]
            own[c, x : x + 4] = value
            to[c] = value
        return 0

    lax.fori_loop(0, 3, move, 0)


def load_mass(source, curl, own, low, high):
    load(source, own, low, high)
    high[1, 0] = source[1, 4] + curl[2, 3]
    high[2, 0] = source[2, 4] + curl[1, 3]


def row_tile(parts, c, x, y):
    own, below, above = parts
    if x < 4:
        return below[c, x, y : y + 8]
    if x >= 12:
        return above[c, x - 12, y : y + 8]
    return own[c, x - 4, y : y + 8]


def pack_y(*refs):
    blocks, (low, high) = (refs[0:3], refs[3:6], refs[6:9]), refs[9:]
    sub = lax.broadcasted_iota(jnp.int32, (8, 128), 0)

    def pack(c, _):
        for n, parts in enumerate(blocks):
            for p in range(8):
                a = row_tile(parts, c, p, 0)
                b = row_tile(parts, c, p + 8, 0)
                low[3 * n + c, p] = jnp.where(sub < 4, a, pltpu.roll(b, 4, 0))
                a = row_tile(parts, c, p, 24)
                b = row_tile(parts, c, p + 8, 24)
                high[3 * n + c, p] = jnp.where(sub < 4, pltpu.roll(a, 4, 0), b)
        return 0

    lax.fori_loop(0, 3, pack, 0)

    def corrected(i, _):
        c, other = 2 * i, 2 - 2 * i
        for p in range(8):
            a = pltpu.roll(row_tile(blocks[2], other, p, 24), 5, 0)
            b = pltpu.roll(row_tile(blocks[2], other, p + 8, 24), 1, 0)
            high[3 + c, p] = high[3 + c, p] + jnp.where(sub == 0, a, jnp.where(sub == 4, b, 0.0))
        return 0

    lax.fori_loop(0, 2, corrected, 0)


def pack_z(*refs):
    blocks, (ylow, yhigh, low, high, field, coef) = (refs[0:3], refs[3:6], refs[6:9]), refs[9:]
    f32 = jnp.float32
    sub = lax.broadcasted_iota(jnp.int32, (8, 128), 0)

    def assemble(c, _):
        for n, (own, below, above) in enumerate(blocks):
            to = field.at[c] if n == 0 else coef.at[3 * n - 3 + c]
            if n > 0:
                to[OFF - 1] = jnp.zeros((Y, 128), f32)
            to[OFF : OFF + 4, OWN : OWN + 32] = below[c]
            to[OFF + 4 : OFF + 12, OWN : OWN + 32] = own[c]
            to[OFF + 12 : OFF + 16, OWN : OWN + 32] = above[c]
            for p in range(8):
                lower, upper = ylow[3 * n + c, p], yhigh[3 * n + c, p]
                to[OFF + p, OWN - 8 : OWN] = jnp.where(sub >= 4, pltpu.roll(lower, 4, 0), 0.0)
                to[OFF + p + 8, OWN - 8 : OWN] = jnp.where(sub >= 4, lower, 0.0)
                to[OFF + p, OWN + 32 : OWN + 40] = jnp.where(sub < 4, upper, 0.0)
                to[OFF + p + 8, OWN + 32 : OWN + 40] = jnp.where(sub < 4, pltpu.roll(upper, 4, 0), 0.0)
        return 0

    lax.fori_loop(0, 3, assemble, 0)

    lane = lax.broadcasted_iota(jnp.int32, (8, 128), 1)
    group = lane >> 2

    def rows(o):
        return pl.ds(pl.multiple_of(LO + 8 * o, 8), 8), pl.ds(pl.multiple_of(8 * o, 8), 8)

    def strips(i, _, source, base):
        comp, o = i // 6, i % 6
        here, to = rows(o)
        first, last = (jnp.zeros((8, 128), f32),) * 2
        for x in range(16):
            t = source[comp, OFF + x, here, :]
            first = jnp.where(group == 2 * x + 1, pltpu.roll(t, 8 * x + 4, 1), first)
            last = jnp.where(group == 2 * x, pltpu.roll(t, (8 * x + 4) % 128, 1), last)
        low[comp + base, to, :] = first
        high[comp + base, to, :] = last
        return 0

    lax.fori_loop(0, 18, lambda i, c: strips(i, c, field, 0), 0)
    lax.fori_loop(0, 36, lambda i, c: strips(i, c, coef, 3), 0)

    def corrected(i, _):
        which, o = i // 6, i % 6
        here, to = rows(o)
        last = jnp.zeros((8, 128), f32)
        for x in range(16):
            t = coef[4 - which, OFF + x, here, :]
            last = jnp.where(lane == 8 * x, pltpu.roll(t, (8 * x + 5) % 128, 1), last)
        high[3 + which, to, :] = high[3 + which, to, :] + last
        return 0

    lax.fori_loop(0, 12, corrected, 0)


def main(field0, coef, zown_low, zown_high, zlow, zhigh, vectors, precond, partial, sink,
         field, diag, node, s, phi, g, fieldS, coefS, diagS, nodeS, sS, phiS, gS):
    f32 = jnp.float32
    lane = lax.broadcasted_iota(jnp.int32, (ROWS, 128), 1)
    first_lane, last_lane = lane == 0, lane == 127

    def at(ref, dy=0):
        return ref[pl.ds(LO + dy, ROWS), :]

    def put(ref, value):
        ref[pl.ds(LO, ROWS), :] = value

    def z_up(value, strip, x):
        return jnp.where(last_lane, pltpu.roll(strip, (123 - 8 * x) & 127, 1), pltpu.roll(value, 127, 1))

    def z_down(value, strip, x):
        return jnp.where(first_lane, pltpu.roll(strip, (125 - 8 * x) & 127, 1), pltpu.roll(value, 1, 1))

    def clear(x, _):
        for c in range(3):
            put(field.at[2, c, x], jnp.zeros((ROWS, 128), f32))
            put(field.at[0, c, x], at(field0.at[c, x]))
        return 0

    lax.fori_loop(0, X, clear, 0)
    for t in range(2):
        own, other = ((zown_low, zlow), (zown_high, zhigh))[t]
        for comp in range(3):
            put(fieldS.at[0, comp, t], own[comp] + other[comp])
            put(fieldS.at[2, comp, t], jnp.zeros((ROWS, 128), f32))
        for comp in range(6):
            put(coefS.at[comp, t], own[comp + 3] + other[comp + 3])

    def diagonals(m, c, cy, cx, cz, mx, my, mz):
        d0 = m[0] + c[1] + cz[1] + c[2] + cy[2]
        d1 = m[1] + c[2] + cx[2] + c[0] + cz[0]
        d2 = m[2] + c[0] + cy[0] + c[1] + cx[1]
        dn = m[0] + mx + m[1] + my + m[2] + mz
        return 1.0 / d0, 1.0 / d1, 1.0 / d2, 1.0 / dn

    def setup_strip(t, _):
        m = [at(coefS.at[c, t]) for c in range(3)]
        c_ = [at(coefS.at[3 + c, t]) for c in range(3)]
        cy = [at(coefS.at[3 + c, t], -1) for c in range(3)]
        cx = [jnp.where(lane < 8, 0.0, pltpu.roll(v, 8, 1)) for v in c_]
        cz = [jnp.where((lane & 7) == 0, 0.0, pltpu.roll(v, 1, 1)) for v in c_]
        out = diagonals(m, c_, cy, cx, cz, pltpu.roll(m[0], 8, 1), at(coefS.at[1, t], -1), pltpu.roll(m[2], 1, 1))
        for c in range(3):
            put(diagS.at[c, t], out[c])
        put(nodeS.at[t], out[3])
        return 0

    lax.fori_loop(0, 2, setup_strip, 0)

    def setup(x, _):
        i = x + OFF
        m = [at(coef.at[c, i]) for c in range(3)]
        c_ = [at(coef.at[3 + c, i]) for c in range(3)]
        cy = [at(coef.at[3 + c, i], -1) for c in range(3)]
        cx = [at(coef.at[3 + c, i - 1]) for c in range(3)]
        cz = [z_down(c_[c], at(coefS.at[3 + c, 0]), x) for c in range(2)]
        out = diagonals(m, c_, cy, cx, cz, at(coef.at[0, i - 1]), at(coef.at[1, i], -1),
                        z_down(m[2], at(coefS.at[2, 0]), x))
        for c in range(3):
            put(diag.at[c, i], out[c])
        put(node.at[i], out[3])
        return 0

    lax.fori_loop(0, 16, setup, 0)

    def fluxes(coefs, e, e0y, e0z, e1x, e1z, e2x, e2y):
        return (coefs[0] * ((e2y - e[2]) - (e1z - e[1])),
                coefs[1] * ((e0z - e[0]) - (e2x - e[2])),
                coefs[2] * ((e1x - e[1]) - (e0y - e[0])))

    def curl_back(gv, g0y, g0z, g1x, g1z, g2x, g2y):
        return ((g1z - gv[1]) - (g2y - gv[2]), (g2x - gv[2]) - (g0z - gv[0]), (g0y - gv[0]) - (g1x - gv[1]))

    def operator_step(k, turns):
        now, later, before = turns
        weight = jnp.where(k == 0, 0.0, jnp.where(k == 1, 0.5, 0.25))

        def strip_first(t, _):
            r = [at(fieldS.at[now, c, t]) for c in range(3)]
            q = ((pltpu.roll(r[0], 8, 1) - r[0]) + (at(fieldS.at[now, 1, t], -1) - r[1])) + (pltpu.roll(r[2], 1, 1) - r[2])
            put(phiS.at[t], q * at(nodeS.at[t]))
            for c in range(3):
                put(sS.at[c, t], r[c] * at(diagS.at[c, t]))
            return 0

        def strip_second(t, _):
            e = [at(sS.at[c, t]) for c in range(3)]
            out = fluxes([at(coefS.at[3 + c, t]) for c in range(3)], e,
                         at(sS.at[0, t], 1), pltpu.roll(e[0], 127, 1), pltpu.roll(e[1], 120, 1),
                         pltpu.roll(e[1], 127, 1), pltpu.roll(e[2], 120, 1), at(sS.at[2, t], 1))
            for c in range(3):
                put(gS.at[c, t], out[c])
            return 0

        def strip_third(t, _):
            gv = [at(gS.at[c, t]) for c in range(3)]
            w = curl_back(gv, at(gS.at[0, t], -1), pltpu.roll(gv[0], 1, 1), pltpu.roll(gv[1], 8, 1),
                          pltpu.roll(gv[1], 1, 1), pltpu.roll(gv[2], 8, 1), at(gS.at[2, t], -1))
            p = at(phiS.at[t])
            up = (pltpu.roll(p, 120, 1), at(phiS.at[t], 1), pltpu.roll(p, 127, 1))
            for c in range(3):
                u = at(sS.at[c, t]) + (up[c] - p)
                put(fieldS.at[later, c, t], (w[c] + at(coefS.at[c, t]) * u - at(fieldS.at[now, c, t]))
                    - weight * at(fieldS.at[before, c, t]))
            return 0

        for part in (strip_first, strip_second, strip_third):
            lax.fori_loop(0, 2, part, 0)

        def row(n_row, sums):
            i = n_row + k + 1
            x = i - OFF
            g_own = [at(g.at[c, i]) for c in range(3)]
            g_x = [at(g.at[c, i - 1]) for c in (1, 2)]
            g_y = [at(g.at[c, i], -1) for c in (0, 2)]
            p, p_x, p_y = at(phi.at[i]), at(phi.at[i + 1]), at(phi.at[i], 1)
            s_own = [at(s.at[c, i]) for c in range(3)]
            r = [at(field.at[now, c, i]) for c in range(3)]
            old = [at(field.at[before, c, i]) for c in range(3)]
            mass = [at(coef.at[c, i]) for c in range(3)]
            a = i + 1
            e = [at(s.at[c, a]) for c in range(3)]
            e_x = [at(s.at[c, a + 1]) for c in (1, 2)]
            e_y = [at(s.at[c, a], 1) for c in (0, 2)]
            curl = [at(coef.at[3 + c, a]) for c in range(3)]
            b = i + 3
            f = [at(field.at[now, c, b]) for c in range(3)]
            f_x, f_y = at(field.at[now, 0, b - 1]), at(field.at[now, 1, b], -1)
            inverse, inverse_node = [at(diag.at[c, b]) for c in range(3)], at(node.at[b])

            w = curl_back(g_own, g_y[0], z_down(g_own[0], at(gS.at[0, 0]), x), g_x[0],
                          z_down(g_own[1], at(gS.at[1, 0]), x), g_x[1], g_y[1])
            up = (p_x, p_y, z_up(p, at(phiS.at[1]), x))
            u = [s_own[c] + (up[c] - p) for c in range(3)]
            v = [((w[c] + mass[c] * u[c]) - r[c]) - weight * old[c] for c in range(3)]
            flux = fluxes(curl, e, e_y[0], z_up(e[0], at(sS.at[0, 1]), x + 1), e_x[0],
                          z_up(e[1], at(sS.at[1, 1]), x + 1), e_x[1], e_y[1])
            q = ((f_x - f[0]) + (f_y - f[1])) + (z_down(f[2], at(fieldS.at[now, 2, 0]), x + 3) - f[2])
            potential = q * inverse_node
            scaled = [f[c] * inverse[c] for c in range(3)]

            inside = (x >= 4) & (x < 12)
            to = jnp.where(inside, x - 4, 8)
            for c in range(3):
                put(field.at[later, c, i], v[c])
                put(g.at[c, a], flux[c])
                put(s.at[c, b], scaled[c])
            put(phi.at[b], potential)
            sums = list(sums)
            for c in range(3):
                uo, ro, vo = (z[OWN - LO : OWN - LO + 32] for z in (u[c], r[c], v[c]))
                vectors[k, c, to] = vo
                precond[k, c, to] = uo
                for n, prod in ((0, ro * uo), (1, vo * uo)):
                    part = (prod[0:8] + prod[8:16]) + (prod[16:24] + prod[24:32])
                    sums[n] = sums[n] + jnp.where(inside, part, 0.0)
            return tuple(sums)

        zero = jnp.zeros((8, 128), f32)
        sums = lax.fori_loop(0, 18 - 2 * k, row, (zero, zero))
        partial[2 * k] = sums[0]
        partial[2 * k + 1] = sums[1]
        return later, before, now

    lax.fori_loop(0, 4, operator_step, (jnp.int32(0), jnp.int32(1), jnp.int32(2)))

    def look(x, _):
        for c in range(3):
            sink[x, c] = s[c, x + OFF, 16:24] + g[c, x + OFF, 16:24]
        sink[x, 3] = phi[x + OFF, 16:24]
        return 0

    lax.fori_loop(0, 2, look, 0)


def fold(partial, out):
    lane = lax.broadcasted_iota(jnp.int32, (1, 128), 1)
    row = jnp.zeros((1, 128), jnp.float32)
    for d in range(8):
        t = jnp.sum(partial[d], axis=0, keepdims=True)
        for shift in (64, 32, 16):
            t = t + pltpu.roll(t, shift, 1)
        row = jnp.where(lane // 16 == d, t, row)
    out[...] = jnp.broadcast_to(row, out.shape)


def finish(everyone, own, vectors, precond, solution_out, residual_out):
    total = jnp.sum(everyone[...], axis=0, keepdims=True)
    lane = lax.broadcasted_iota(jnp.int32, (1, 128), 1)
    dots = [jnp.broadcast_to(jnp.sum(jnp.where(lane // 16 == d, total, 0.0), axis=1, keepdims=True), (8, 128))
            for d in range(8)]
    size = [1.0] + [2.0 ** (1 - k) for k in range(1, 9)]
    moment = [dots[0], dots[1]]
    for k in range(1, 4):
        moment.append((dots[2 * k] * (2.0 / size[k] ** 2) - moment[0]) * size[2 * k])
        moment.append((dots[2 * k + 1] * (2.0 / (size[k] * size[k + 1])) - moment[1]) * size[2 * k + 1])
    row, earlier = moment, None
    alpha, beta = [row[1] / row[0]], [None]
    for k in range(1, 4):
        following = [None] * 8
        for l in range(k, 8 - k):
            t = row[l + 1] - alpha[k - 1] * row[l] + WEIGHT[l if l < 2 else 2] * row[l - 1]
            if k > 1:
                t = t - beta[k - 1] * earlier[l]
            following[l] = t
        alpha.append(following[k + 1] / following[k] - row[k] / row[k - 1])
        beta.append(following[k] / row[k - 1])
        row, earlier = following, row
    zero = jnp.zeros((8, 128), jnp.float32)
    older, newer = [zero] * 6, [zero + 1.0] + [zero] * 5
    value_older, value = zero, zero + 1.0
    weight = lambda l: WEIGHT[min(l, 2)]
    for k in range(4):
        nxt = []
        for l in range(6):
            t = -alpha[k] * newer[l]
            if l > 0:
                t = t + newer[l - 1]
            if l < 5:
                t = t + weight(l + 1) * newer[l + 1]
            if k > 0:
                t = t - beta[k] * older[l]
            nxt.append(t)
        step = (-1.0 - alpha[k]) * value
        if k > 0:
            step = step - beta[k] * value_older
        older, newer, value_older, value = newer, nxt, value, step
    inverse = 1.0 / value
    e = [newer[l] * inverse for l in range(5)]
    S = [None] * 4
    S[3] = -e[4]
    S[2] = -e[3] - S[3]
    S[1] = -e[2] - S[2] - weight(3) * S[3]
    S[0] = -e[1] - S[1] - weight(2) * S[2]
    e = [v[0:1] for v in e]
    S = [v[0:1] for v in S]

    def combine(x, _):
        for c in range(3):
            residual_out[c, x] = (e[0] * own[c, x] + e[1] * vectors[0, c, x]) + (
                e[2] * vectors[1, c, x] + e[3] * vectors[2, c, x]) + e[4] * vectors[3, c, x]
            solution_out[c, x] = (S[0] * precond[0, c, x] + S[1] * precond[1, c, x]) + (
                S[2] * precond[2, c, x] + S[3] * precond[3, c, x])
        return 0

    lax.fori_loop(0, 8, combine, 0)


def shape(*dims):
    return jax.ShapeDtypeStruct(dims, jnp.float32)


def call(kernel, outs, ins, mib, scratch=(), flops=1000000):
    return pl.pallas_call(
        kernel, out_shape=outs, in_specs=[VMEM] * len(ins), out_specs=jax.tree.map(lambda _: VMEM, outs),
        scratch_shapes=list(scratch), compiler_params=pltpu.CompilerParams(vmem_limit_bytes=int(mib * 2**20)),
        cost_estimate=pl.CostEstimate(flops=flops, bytes_accessed=1 << 20, transcendentals=0))(*ins)


def exchange(low, high, axis):
    n = lax.axis_size(axis)
    up = [(i, (i + 1) % n) for i in range(n)]
    return lax.ppermute(high, axis, up), lax.ppermute(low, axis, [(j, i) for i, j in up])


def body(right, mass, curl):
    face = (shape(3, 8, 32, 128),) + (shape(3, 4, 32, 128),) * 2
    b, *ends = call(load, face, (right,), 8)
    b = (b,) + exchange(*ends, "gx")
    c, *ends = call(load, face, (curl,), 8)
    c = (c,) + exchange(*ends, "gx")
    m, *ends = call(load_mass, face, (mass, c[0]), 8)
    block = b + (m,) + exchange(*ends, "gx") + c
    low, high = call(pack_y, (shape(9, 8, 8, 128),) * 2, block, 8)
    block += exchange(low, high, "gy")
    low, high, field, coef = call(
        pack_z, (shape(9, ROWS, 128),) * 2 + (shape(3, X, Y, 128), shape(6, X, Y, 128)), block, 20)
    sides = (low, high) + exchange(low, high, "gz")

    def held(*dims):
        return pltpu.VMEM(dims + (Y, 128), jnp.float32)

    vectors, precond, partial, _ = call(
        main, (shape(4, 3, 9, 32, 128), shape(4, 3, 9, 32, 128), shape(8, 8, 128), shape(2, 4, 8, 128)), (field, coef) + sides, 40,
        [held(3, 3, X), held(3, X), held(X), held(3, X), held(X), held(3, X),
         held(3, 3, 2), held(6, 2), held(3, 2), held(2), held(3, 2), held(2), held(3, 2)])
    axes = ("gx", "gy", "gz")
    devices = lax.axis_size(axes)
    (rows,) = call(fold, (shape(devices, 128),), (partial,), 4)
    everyone = lax.all_to_all(rows.reshape(devices, 1, 128), axes, 0, 0, tiled=True).reshape(devices, 128)
    return call(finish, (shape(3, 8, 32, 128),) * 2, (everyone, b[0], vectors, precond), 16)


def solution(mesh):
    spec = P(None, "gx", "gy", "gz")
    return jax.shard_map(body, mesh=mesh, in_specs=(spec,) * 3, out_specs=(spec,) * 2, check_vma=False)
```

```python
import jax
import jax.numpy as jnp
from jax import lax
from jax.experimental import pallas as pl
from jax.experimental.pallas import tpu as pltpu
from jax.sharding import PartitionSpec as P


X, Y = 24, 64
OFF, OWN = 4, 16
LO, ROWS = 8, 48
WEIGHT = (0.0, 0.5, 0.25, 0.25, 0.25)
VMEM = pl.BlockSpec(memory_space=pltpu.VMEM)


def load(source, own, low, high):
    def move(c, _):
        for to, x in ((low, 0), (high, 4)):
            value = source[c, x : x + 4]
            own[c, x : x + 4] = value
            to[c] = value
        return 0

    lax.fori_loop(0, 3, move, 0)


def load_mass(source, curl, own, low, high):
    load(source, own, low, high)
    high[1, 0] = source[1, 4] + curl[2, 3]
    high[2, 0] = source[2, 4] + curl[1, 3]


def pack_y(pairs, *refs):
    refs, (low, high) = refs[:-2], refs[-2:]
    n = len(refs) // 3
    sub = lax.broadcasted_iota(jnp.int32, (8, 128), 0)

    def tile(field, c, p, half, y):
        return pairs(refs[field * n : field * n + n], c, p, half, y)

    def pack(c, _):
        for field in range(3):
            for p in range(4):
                a, b = tile(field, c, p, 0, 0), tile(field, c, p, 1, 0)
                low[3 * field + c, p] = jnp.where(sub < 4, a, pltpu.roll(b, 4, 0))
                a, b = tile(field, c, p, 0, 24), tile(field, c, p, 1, 24)
                high[3 * field + c, p] = jnp.where(sub < 4, pltpu.roll(a, 4, 0), b)
        return 0

    lax.fori_loop(0, 3, pack, 0)

    def corrected(i, _):
        c, other = 2 * i, 2 - 2 * i
        for p in range(4):
            a = pltpu.roll(tile(2, other, p, 0, 24), 5, 0)
            b = pltpu.roll(tile(2, other, p, 1, 24), 1, 0)
            high[3 + c, p] = high[3 + c, p] + jnp.where(sub == 0, a, jnp.where(sub == 4, b, 0.0))
        return 0

    lax.fori_loop(0, 2, corrected, 0)


def pack_y_own(*refs):
    pack_y(lambda own, c, p, half, y: own[0][c, p + 4 * half, y : y + 8], *refs)


def pack_y_halo(*refs):
    pack_y(lambda ends, c, p, half, y: ends[half][c, p, y : y + 8], *refs)


def strips(source, base, count, octets, low, high):
    group = lax.broadcasted_iota(jnp.int32, (8, 128), 1) >> 2
    each, x0, start, begin, stride = octets

    def one(i, _):
        comp, o = i // each, i % each
        here = pl.ds(pl.multiple_of(start + 8 * o, 8), 8)
        to = pl.ds(pl.multiple_of(begin + stride * o, 8), 8)
        first, last = (jnp.zeros((8, 128), jnp.float32),) * 2
        for x in range(16):
            t = source[comp, x0 + x, here, :]
            first = jnp.where(group == 2 * x + 1, pltpu.roll(t, 8 * x + 4, 1), first)
            last = jnp.where(group == 2 * x, pltpu.roll(t, (8 * x + 4) % 128, 1), last)
        low[comp + base, to, :] = first
        high[comp + base, to, :] = last
        return 0

    lax.fori_loop(0, count * each, one, 0)


def all_strips(field, coef, octets, low, high):
    strips(field, 0, 3, octets, low, high)
    strips(coef, 3, 6, octets, low, high)
    lane = lax.broadcasted_iota(jnp.int32, (8, 128), 1)
    each, x0, start, begin, stride = octets

    def corrected(i, _):
        which, o = i // each, i % each
        here = pl.ds(pl.multiple_of(start + 8 * o, 8), 8)
        to = pl.ds(pl.multiple_of(begin + stride * o, 8), 8)
        last = jnp.zeros((8, 128), jnp.float32)
        for x in range(16):
            t = coef[4 - which, x0 + x, here, :]
            last = jnp.where(lane == 8 * x, pltpu.roll(t, (8 * x + 5) % 128, 1), last)
        high[3 + which, to, :] = high[3 + which, to, :] + last
        return 0

    lax.fori_loop(0, 2 * each, corrected, 0)


def pack_z_middle(*refs):
    blocks, (low, high, field, coef) = (refs[0:3], refs[3:6], refs[6:9]), refs[9:]

    def assemble(c, _):
        for n, (own, below, above) in enumerate(blocks):
            to = field.at[c] if n == 0 else coef.at[3 * n - 3 + c]
            to[OFF : OFF + 4, OWN : OWN + 32] = below[c]
            to[OFF + 4 : OFF + 12, OWN : OWN + 32] = own[c]
            to[OFF + 12 : OFF + 16, OWN : OWN + 32] = above[c]
        return 0

    lax.fori_loop(0, 3, assemble, 0)
    all_strips(field, coef, (4, OFF, OWN, 8, 8), low, high)


def pack_z_edge(own_low, own_high, halo_low, halo_high, middle_low, middle_high,
                low, high, send_low, send_high, field, coef):
    sub = lax.broadcasted_iota(jnp.int32, (8, 128), 0)

    def assemble(c, _):
        for n in range(3):
            to = field.at[c] if n == 0 else coef.at[3 * n - 3 + c]
            comp = 3 * n + c
            for p in range(4):
                for lows, highs, x0, x1 in ((halo_low, halo_high, p, p + 12), (own_low, own_high, p + 4, p + 8)):
                    lower, upper = lows[comp, p], highs[comp, p]
                    to[x0, 0:8] = jnp.where(sub >= 4, pltpu.roll(lower, 4, 0), 0.0)
                    to[x1, 0:8] = jnp.where(sub >= 4, lower, 0.0)
                    to[x0, 8:16] = jnp.where(sub < 4, upper, 0.0)
                    to[x1, 8:16] = jnp.where(sub < 4, pltpu.roll(upper, 4, 0), 0.0)
        return 0

    lax.fori_loop(0, 3, assemble, 0)
    all_strips(field, coef, (2, 0, 0, 0, 40), low, high)
    for comp in range(9):
        low[comp, 8:40] = middle_low[comp, 8:40]
        high[comp, 8:40] = middle_high[comp, 8:40]
    for n in range(5):
        down, up = low[n], high[n]
        if n < 4:
            down, up = down + pltpu.roll(low[n + 5], 124, 1), up + pltpu.roll(high[n + 5], 4, 1)
        send_low[n] = down
        send_high[n] = up


def at(ref, dy=0):
    return ref[pl.ds(LO + dy, ROWS), :]


def put(ref, value):
    ref[pl.ds(LO, ROWS), :] = value


def diagonals(m, c, cy, cx, cz, mx, my, mz):
    d0 = m[0] + c[1] + cz[1] + c[2] + cy[2]
    d1 = m[1] + c[2] + cx[2] + c[0] + cz[0]
    d2 = m[2] + c[0] + cy[0] + c[1] + cx[1]
    dn = m[0] + mx + m[1] + my + m[2] + mz
    return 1.0 / d0, 1.0 / d1, 1.0 / d2, 1.0 / dn


def invert(field_middle, coef_middle, field_edge, coef_edge, field, coef, diag, node):
    def assemble(c, _):
        coef[c, OFF - 1] = jnp.zeros((Y, 128), jnp.float32)
        for x in range(OFF, OFF + 16):
            coef[c, x, OWN : OWN + 32] = coef_middle[c, x, OWN : OWN + 32]
            coef[c, x, OWN - 8 : OWN] = coef_edge[c, x - OFF, 0:8]
            coef[c, x, OWN + 32 : OWN + 40] = coef_edge[c, x - OFF, 8:16]
        return 0

    def assemble_field(c, _):
        for x in range(OFF, OFF + 16):
            field[c, x, OWN : OWN + 32] = field_middle[c, x, OWN : OWN + 32]
            field[c, x, OWN - 8 : OWN] = field_edge[c, x - OFF, 0:8]
            field[c, x, OWN + 32 : OWN + 40] = field_edge[c, x - OFF, 8:16]
        return 0

    lax.fori_loop(0, 6, assemble, 0)
    lax.fori_loop(0, 3, assemble_field, 0)

    def row(x, _):
        i = x + OFF
        m = [at(coef.at[c, i]) for c in range(3)]
        c_ = [at(coef.at[3 + c, i]) for c in range(3)]
        cy = [at(coef.at[3 + c, i], -1) for c in range(3)]
        cx = [at(coef.at[3 + c, i - 1]) for c in range(3)]
        cz = [pltpu.roll(c_[c], 1, 1) for c in range(2)]
        out = diagonals(m, c_, cy, cx, cz, at(coef.at[0, i - 1]), at(coef.at[1, i], -1), pltpu.roll(m[2], 1, 1))
        for c in range(3):
            put(diag.at[c, i], out[c])
        put(node.at[i], out[3])
        return 0

    lax.fori_loop(0, 16, row, 0)


def main(field_in, coef, diag_in, node_in, zown_low, zown_high, zlow, zhigh, vectors, precond, partial, sink,
         field, diag, node, s, phi, g, fieldS, coefS, diagS, nodeS, sS, phiS, gS):
    f32 = jnp.float32
    lane = lax.broadcasted_iota(jnp.int32, (ROWS, 128), 1)
    first_lane, last_lane = lane == 0, lane == 127

    def z_up(value, strip, x):
        return jnp.where(last_lane, pltpu.roll(strip, (123 - 8 * x) & 127, 1), pltpu.roll(value, 127, 1))

    def z_down(value, strip, x):
        return jnp.where(first_lane, pltpu.roll(strip, (125 - 8 * x) & 127, 1), pltpu.roll(value, 1, 1))

    upper = (lane & 4) != 0
    for comp in range(9):
        lower_part, upper_part = zlow[comp % 5], zhigh[comp % 5]
        if comp >= 5:
            lower_part, upper_part = pltpu.roll(lower_part, 124, 1), pltpu.roll(upper_part, 4, 1)
        for t, value in ((0, jnp.where(upper, zown_low[comp], lower_part)),
                         (1, jnp.where(upper, upper_part, zown_high[comp]))):
            put(fieldS.at[0, comp, t] if comp < 3 else coefS.at[comp - 3, t], value)

    def setup_strip(t, _):
        m = [at(coefS.at[c, t]) for c in range(3)]
        c_ = [at(coefS.at[3 + c, t]) for c in range(3)]
        cy = [at(coefS.at[3 + c, t], -1) for c in range(3)]
        cx = [jnp.where(lane < 8, 0.0, pltpu.roll(v, 8, 1)) for v in c_]
        cz = [jnp.where((lane & 7) == 0, 0.0, pltpu.roll(v, 1, 1)) for v in c_]
        out = diagonals(m, c_, cy, cx, cz, pltpu.roll(m[0], 8, 1), at(coefS.at[1, t], -1), pltpu.roll(m[2], 1, 1))
        for c in range(3):
            put(diagS.at[c, t], out[c])
        put(nodeS.at[t], out[3])
        return 0

    lax.fori_loop(0, 2, setup_strip, 0)

    def setup(x, _):
        i = x + OFF
        for c in range(3):
            put(field.at[0, c, i], at(field_in.at[c, i]))
            put(diag.at[c, i], jnp.where(first_lane, pltpu.roll(at(diagS.at[c, 0]), 124 - 8 * x, 1), at(diag_in.at[c, i])))
        put(node.at[i], jnp.where(first_lane, pltpu.roll(at(nodeS.at[0]), 124 - 8 * x, 1), at(node_in.at[i])))
        return 0

    lax.fori_loop(0, 16, setup, 0)

    def fluxes(coefs, e, e0y, e0z, e1x, e1z, e2x, e2y):
        return (coefs[0] * ((e2y - e[2]) - (e1z - e[1])),
                coefs[1] * ((e0z - e[0]) - (e2x - e[2])),
                coefs[2] * ((e1x - e[1]) - (e0y - e[0])))

    def curl_back(gv, g0y, g0z, g1x, g1z, g2x, g2y):
        return ((g1z - gv[1]) - (g2y - gv[2]), (g2x - gv[2]) - (g0z - gv[0]), (g0y - gv[0]) - (g1x - gv[1]))

    def operator_step(k, turns):
        now, later, before = turns
        weight = jnp.where(k == 0, 0.0, jnp.where(k == 1, 0.5, 0.25))

        def strip_first(t, _):
            r = [at(fieldS.at[now, c, t]) for c in range(3)]
            q = ((pltpu.roll(r[0], 8, 1) - r[0]) + (at(fieldS.at[now, 1, t], -1) - r[1])) + (pltpu.roll(r[2], 1, 1) - r[2])
            put(phiS.at[t], q * at(nodeS.at[t]))
            for c in range(3):
                put(sS.at[c, t], r[c] * at(diagS.at[c, t]))
            return 0

        def strip_second(t, _):
            e = [at(sS.at[c, t]) for c in range(3)]
            out = fluxes([at(coefS.at[3 + c, t]) for c in range(3)], e,
                         at(sS.at[0, t], 1), pltpu.roll(e[0], 127, 1), pltpu.roll(e[1], 120, 1),
                         pltpu.roll(e[1], 127, 1), pltpu.roll(e[2], 120, 1), at(sS.at[2, t], 1))
            for c in range(3):
                put(gS.at[c, t], out[c])
            return 0

        def strip_third(t, _):
            gv = [at(gS.at[c, t]) for c in range(3)]
            w = curl_back(gv, at(gS.at[0, t], -1), pltpu.roll(gv[0], 1, 1), pltpu.roll(gv[1], 8, 1),
                          pltpu.roll(gv[1], 1, 1), pltpu.roll(gv[2], 8, 1), at(gS.at[2, t], -1))
            p = at(phiS.at[t])
            up = (pltpu.roll(p, 120, 1), at(phiS.at[t], 1), pltpu.roll(p, 127, 1))
            for c in range(3):
                u = at(sS.at[c, t]) + (up[c] - p)
                put(fieldS.at[later, c, t], (w[c] + at(coefS.at[c, t]) * u - at(fieldS.at[now, c, t]))
                    - weight * at(fieldS.at[before, c, t]))
            return 0

        for part in (strip_first, strip_second, strip_third):
            lax.fori_loop(0, 2, part, 0)

        def row(n_row, sums):
            i = n_row + k + 1
            x = i - OFF
            g_own = [at(g.at[c, i]) for c in range(3)]
            g_x = [at(g.at[c, i - 1]) for c in (1, 2)]
            g_y = [at(g.at[c, i], -1) for c in (0, 2)]
            p, p_x, p_y = at(phi.at[i]), at(phi.at[i + 1]), at(phi.at[i], 1)
            s_own = [at(s.at[c, i]) for c in range(3)]
            r = [at(field.at[now, c, i]) for c in range(3)]
            old = [at(field.at[before, c, i]) for c in range(3)]
            mass = [at(coef.at[c, i]) for c in range(3)]
            a = i + 1
            e = [at(s.at[c, a]) for c in range(3)]
            e_x = [at(s.at[c, a + 1]) for c in (1, 2)]
            e_y = [at(s.at[c, a], 1) for c in (0, 2)]
            curl = [at(coef.at[3 + c, a]) for c in range(3)]
            b = i + 3
            f = [at(field.at[now, c, b]) for c in range(3)]
            f_x, f_y = at(field.at[now, 0, b - 1]), at(field.at[now, 1, b], -1)
            inverse, inverse_node = [at(diag.at[c, b]) for c in range(3)], at(node.at[b])

            w = curl_back(g_own, g_y[0], z_down(g_own[0], at(gS.at[0, 0]), x), g_x[0],
                          z_down(g_own[1], at(gS.at[1, 0]), x), g_x[1], g_y[1])
            up = (p_x, p_y, z_up(p, at(phiS.at[1]), x))
            u = [s_own[c] + (up[c] - p) for c in range(3)]
            v = [((w[c] + mass[c] * u[c]) - r[c]) - weight * old[c] for c in range(3)]
            flux = fluxes(curl, e, e_y[0], z_up(e[0], at(sS.at[0, 1]), x + 1), e_x[0],
                          z_up(e[1], at(sS.at[1, 1]), x + 1), e_x[1], e_y[1])
            q = ((f_x - f[0]) + (f_y - f[1])) + (z_down(f[2], at(fieldS.at[now, 2, 0]), x + 3) - f[2])
            potential = q * inverse_node
            scaled = [f[c] * inverse[c] for c in range(3)]

            inside = (x >= 4) & (x < 12)
            to = jnp.where(inside, x - 4, 8)
            for c in range(3):
                put(field.at[later, c, i], v[c])
                put(g.at[c, a], flux[c])
                put(s.at[c, b], scaled[c])
            put(phi.at[b], potential)
            sums = list(sums)
            for c in range(3):
                uo, ro, vo = (z[OWN - LO : OWN - LO + 32] for z in (u[c], r[c], v[c]))
                vectors[k, c, to] = vo
                precond[k, c, to] = uo
                for n, prod in ((0, ro * uo), (1, vo * uo)):
                    part = (prod[0:8] + prod[8:16]) + (prod[16:24] + prod[24:32])
                    sums[n] = sums[n] + jnp.where(inside, part, 0.0)
            return tuple(sums)

        zero = jnp.zeros((8, 128), f32)
        sums = lax.fori_loop(0, 18 - 2 * k, row, (zero, zero))
        partial[2 * k] = sums[0]
        partial[2 * k + 1] = sums[1]
        return later, 3 - now - later, now

    lax.fori_loop(0, 4, operator_step, (jnp.int32(0), jnp.int32(1), jnp.int32(0)))

    def look(x, _):
        for c in range(3):
            sink[x, c] = s[c, x + OFF, 16:24] + g[c, x + OFF, 16:24]
        sink[x, 3] = phi[x + OFF, 16:24]
        return 0

    lax.fori_loop(0, 2, look, 0)


def fold(partial, out):
    lane = lax.broadcasted_iota(jnp.int32, (1, 128), 1)
    row = jnp.zeros((1, 128), jnp.float32)
    for d in range(8):
        t = jnp.sum(partial[d], axis=0, keepdims=True)
        for shift in (64, 32, 16):
            t = t + pltpu.roll(t, shift, 1)
        row = jnp.where(lane // 16 == d, t, row)
    out[...] = jnp.broadcast_to(row, out.shape)


def finish(everyone, own, vectors, precond, solution_out, residual_out):
    total = jnp.sum(everyone[...], axis=0, keepdims=True)
    lane = lax.broadcasted_iota(jnp.int32, (1, 128), 1)
    dots = [jnp.broadcast_to(jnp.sum(jnp.where(lane // 16 == d, total, 0.0), axis=1, keepdims=True), (8, 128))
            for d in range(8)]
    size = [1.0] + [2.0 ** (1 - k) for k in range(1, 9)]
    moment = [dots[0], dots[1]]
    for k in range(1, 4):
        moment.append((dots[2 * k] * (2.0 / size[k] ** 2) - moment[0]) * size[2 * k])
        moment.append((dots[2 * k + 1] * (2.0 / (size[k] * size[k + 1])) - moment[1]) * size[2 * k + 1])
    row, earlier = moment, None
    alpha, beta = [row[1] / row[0]], [None]
    for k in range(1, 4):
        following = [None] * 8
        for l in range(k, 8 - k):
            t = row[l + 1] - alpha[k - 1] * row[l] + WEIGHT[l if l < 2 else 2] * row[l - 1]
            if k > 1:
                t = t - beta[k - 1] * earlier[l]
            following[l] = t
        alpha.append(following[k + 1] / following[k] - row[k] / row[k - 1])
        beta.append(following[k] / row[k - 1])
        row, earlier = following, row
    zero = jnp.zeros((8, 128), jnp.float32)
    older, newer = [zero] * 6, [zero + 1.0] + [zero] * 5
    value_older, value = zero, zero + 1.0
    weight = lambda l: WEIGHT[min(l, 2)]
    for k in range(4):
        nxt = []
        for l in range(6):
            t = -alpha[k] * newer[l]
            if l > 0:
                t = t + newer[l - 1]
            if l < 5:
                t = t + weight(l + 1) * newer[l + 1]
            if k > 0:
                t = t - beta[k] * older[l]
            nxt.append(t)
        step = (-1.0 - alpha[k]) * value
        if k > 0:
            step = step - beta[k] * value_older
        older, newer, value_older, value = newer, nxt, value, step
    inverse = 1.0 / value
    e = [newer[l] * inverse for l in range(5)]
    S = [None] * 4
    S[3] = -e[4]
    S[2] = -e[3] - S[3]
    S[1] = -e[2] - S[2] - weight(3) * S[3]
    S[0] = -e[1] - S[1] - weight(2) * S[2]
    e = [v[0:1] for v in e]
    S = [v[0:1] for v in S]

    def combine(x, _):
        for c in range(3):
            residual_out[c, x] = (e[0] * own[c, x] + e[1] * vectors[0, c, x]) + (
                e[2] * vectors[1, c, x] + e[3] * vectors[2, c, x]) + e[4] * vectors[3, c, x]
            solution_out[c, x] = (S[0] * precond[0, c, x] + S[1] * precond[1, c, x]) + (
                S[2] * precond[2, c, x] + S[3] * precond[3, c, x])
        return 0

    lax.fori_loop(0, 8, combine, 0)


def shape(*dims):
    return jax.ShapeDtypeStruct(dims, jnp.float32)


def call(kernel, outs, ins, mib, scratch=(), flops=1000000):
    return pl.pallas_call(
        kernel, out_shape=outs, in_specs=[VMEM] * len(ins), out_specs=jax.tree.map(lambda _: VMEM, outs),
        scratch_shapes=list(scratch),
        compiler_params=pltpu.CompilerParams(vmem_limit_bytes=mib << 20),
        cost_estimate=pl.CostEstimate(flops=flops, bytes_accessed=1 << 20, transcendentals=0))(*ins)


def exchange(low, high, axis):
    n = lax.axis_size(axis)
    up = [(i, (i + 1) % n) for i in range(n)]
    return lax.ppermute(high, axis, up), lax.ppermute(low, axis, [(j, i) for i, j in up])


def body(right, mass, curl):
    face = (shape(3, 8, 32, 128),) + (shape(3, 4, 32, 128),) * 2
    b, *ends = call(load, face, (right,), 8)
    b = (b,) + exchange(*ends, "gx")
    c, *ends = call(load, face, (curl,), 8)
    c = (c,) + exchange(*ends, "gx")
    m, *ends = call(load_mass, face, (mass, c[0]), 8)
    m = (m,) + exchange(*ends, "gx")
    ends = (shape(9, 4, 8, 128),) * 2
    y_own = exchange(*call(pack_y_own, ends, (b[0], m[0], c[0]), 8), "gy")
    y_halo = exchange(*call(pack_y_halo, ends, b[1:] + m[1:] + c[1:], 8), "gy")
    columns = (shape(9, ROWS, 128),) * 2
    extended = (shape(3, X, Y, 128), shape(6, X, Y, 128))
    low, high, *middle = call(pack_z_middle, columns + extended, b + m + c, 8, flops=20000000)
    low, high, *ends, field, coef = call(
        pack_z_edge, columns + (shape(5, ROWS, 128),) * 2 + (shape(3, 16, 16, 128), shape(6, 16, 16, 128)),
        y_own + y_halo + (low, high), 8)
    sides = (low, high) + exchange(*ends, "gz")
    block = call(invert, extended + (shape(3, X, Y, 128), shape(X, Y, 128)), (*middle, field, coef), 8, flops=20000000)

    def held(*dims):
        return pltpu.VMEM(dims + (Y, 128), jnp.float32)

    vectors, precond, partial, _ = call(
        main, (shape(4, 3, 9, 32, 128), shape(4, 3, 9, 32, 128), shape(8, 8, 128), shape(2, 4, 8, 128)),
        tuple(block) + sides, 24,
        [held(3, 3, X), held(3, X), held(X), held(3, X), held(X), held(3, X),
         held(3, 3, 2), held(6, 2), held(3, 2), held(2), held(3, 2), held(2), held(3, 2)])
    axes = ("gx", "gy", "gz")
    devices = lax.axis_size(axes)
    (rows,) = call(fold, (shape(devices, 128),), (partial,), 4)
    everyone = lax.all_to_all(rows.reshape(devices, 1, 128), axes, 0, 0, tiled=True).reshape(devices, 128)
    return call(finish, (shape(3, 8, 32, 128),) * 2, (everyone, b[0], vectors, precond), 16)


def solution(mesh):
    spec = P(None, "gx", "gy", "gz")
    return jax.shard_map(body, mesh=mesh, in_specs=(spec,) * 3, out_specs=(spec,) * 2, check_vma=False)
```

```python
import jax
import jax.numpy as jnp
from jax import lax
from jax.experimental import pallas as pl
from jax.experimental.pallas import tpu as pltpu
from jax.sharding import PartitionSpec as P


X, Y = 24, 56
OFF, OWN = 4, 12
LO, ROWS = 8, 40
WEIGHT = (0.0, 0.5, 0.25, 0.25, 0.25)
VMEM = pl.BlockSpec(memory_space=pltpu.VMEM)


def load(source, own, low, high):
    def move(c, _):
        for to, x in ((low, 0), (high, 4)):
            value = source[c, x : x + 4]
            own[c, x : x + 4] = value
            to[c] = value
        return 0

    lax.fori_loop(0, 3, move, 0)


def load_mass(source, curl, own, low, high):
    load(source, own, low, high)
    high[1, 0] = source[1, 4] + curl[2, 3]
    high[2, 0] = source[2, 4] + curl[1, 3]


def pack_y(pairs, *refs):
    refs, (low, high) = refs[:-2], refs[-2:]
    n = len(refs) // 3
    sub = lax.broadcasted_iota(jnp.int32, (8, 128), 0)

    def tile(field, c, p, half, y):
        return pairs(refs[field * n : field * n + n], c, p, half, y)

    def pack(c, _):
        for field in range(3):
            for p in range(4):
                a, b = tile(field, c, p, 0, 0), tile(field, c, p, 1, 0)
                low[3 * field + c, p] = jnp.where(sub < 4, a, pltpu.roll(b, 4, 0))
                a, b = tile(field, c, p, 0, 24), tile(field, c, p, 1, 24)
                high[3 * field + c, p] = jnp.where(sub < 4, pltpu.roll(a, 4, 0), b)
        return 0

    lax.fori_loop(0, 3, pack, 0)

    def corrected(i, _):
        c, other = 2 * i, 2 - 2 * i
        for p in range(4):
            a = pltpu.roll(tile(2, other, p, 0, 24), 5, 0)
            b = pltpu.roll(tile(2, other, p, 1, 24), 1, 0)
            high[3 + c, p] = high[3 + c, p] + jnp.where(sub == 0, a, jnp.where(sub == 4, b, 0.0))
        return 0

    lax.fori_loop(0, 2, corrected, 0)


def pack_y_own(*refs):
    pack_y(lambda own, c, p, half, y: own[0][c, p + 4 * half, y : y + 8], *refs)


def pack_y_halo(*refs):
    pack_y(lambda ends, c, p, half, y: ends[half][c, p, y : y + 8], *refs)


def strips(source, base, count, octets, low, high):
    group = lax.broadcasted_iota(jnp.int32, (8, 128), 1) >> 2
    each, x0, start, begin, stride = octets

    def one(i, _):
        comp, o = i // each, i % each
        here = pl.ds(pl.multiple_of(start + 8 * o, 8), 8)
        to = pl.ds(pl.multiple_of(begin + stride * o, 8), 8)
        first, last = (jnp.zeros((8, 128), jnp.float32),) * 2
        for x in range(16):
            t = source[comp, x0 + x, here, :]
            first = jnp.where(group == 2 * x + 1, pltpu.roll(t, 8 * x + 4, 1), first)
            last = jnp.where(group == 2 * x, pltpu.roll(t, (8 * x + 4) % 128, 1), last)
        low[comp + base, to, :] = first
        high[comp + base, to, :] = last
        return 0

    lax.fori_loop(0, count * each, one, 0)


def all_strips(field, coef, octets, low, high):
    strips(field, 0, 3, octets, low, high)
    strips(coef, 3, 6, octets, low, high)
    lane = lax.broadcasted_iota(jnp.int32, (8, 128), 1)
    each, x0, start, begin, stride = octets

    def corrected(i, _):
        which, o = i // each, i % each
        here = pl.ds(pl.multiple_of(start + 8 * o, 8), 8)
        to = pl.ds(pl.multiple_of(begin + stride * o, 8), 8)
        last = jnp.zeros((8, 128), jnp.float32)
        for x in range(16):
            t = coef[4 - which, x0 + x, here, :]
            last = jnp.where(lane == 8 * x, pltpu.roll(t, (8 * x + 5) % 128, 1), last)
        high[3 + which, to, :] = high[3 + which, to, :] + last
        return 0

    lax.fori_loop(0, 2 * each, corrected, 0)


def pack_z_middle(*refs):
    blocks, (low, high, field, coef) = (refs[0:3], refs[3:6], refs[6:9]), refs[9:]

    def assemble(c, _):
        for n, (own, below, above) in enumerate(blocks):
            to = field.at[c] if n == 0 else coef.at[3 * n - 3 + c]
            to[OFF : OFF + 4, OWN : OWN + 32] = below[c]
            to[OFF + 4 : OFF + 12, OWN : OWN + 32] = own[c]
            to[OFF + 12 : OFF + 16, OWN : OWN + 32] = above[c]
        return 0

    lax.fori_loop(0, 3, assemble, 0)
    all_strips(field, coef, (3, OFF, 16, 8, 8), low, high)


def pack_z_edge(own_low, own_high, halo_low, halo_high, middle_low, middle_high, middle_field, middle_coef,
                low, high, send_low, send_high, field, coef):
    sub = lax.broadcasted_iota(jnp.int32, (8, 128), 0)

    def assemble(c, _):
        for n in range(3):
            to = field.at[c] if n == 0 else coef.at[3 * n - 3 + c]
            source = middle_field.at[c] if n == 0 else middle_coef.at[3 * n - 3 + c]
            comp = 3 * n + c
            for p in range(4):
                for lows, highs, x0, x1 in ((halo_low, halo_high, p, p + 12), (own_low, own_high, p + 4, p + 8)):
                    lower, upper = lows[comp, p], highs[comp, p]
                    to[x0, 0:8] = jnp.where(sub < 4, lower, source[OFF + x0, 8:16])
                    to[x1, 0:8] = jnp.where(sub < 4, pltpu.roll(lower, 4, 0), source[OFF + x1, 8:16])
                    to[x0, 8:16] = jnp.where(sub < 4, source[OFF + x0, 40:48], pltpu.roll(upper, 4, 0))
                    to[x1, 8:16] = jnp.where(sub < 4, source[OFF + x1, 40:48], upper)
        return 0

    lax.fori_loop(0, 3, assemble, 0)
    all_strips(field, coef, (2, 0, 0, 0, 32), low, high)
    for comp in range(9):
        low[comp, 8:32] = middle_low[comp, 8:32]
        high[comp, 8:32] = middle_high[comp, 8:32]
    for n in range(5):
        down, up = low[n], high[n]
        if n < 4:
            down, up = down + pltpu.roll(low[n + 5], 124, 1), up + pltpu.roll(high[n + 5], 4, 1)
        send_low[n] = down
        send_high[n] = up


def at(ref, dy=0):
    return ref[pl.ds(LO + dy, ROWS), :]


def put(ref, value):
    ref[pl.ds(LO, ROWS), :] = value


def diagonals(m, c, cy, cx, cz, mx, my, mz):
    d0 = m[0] + c[1] + cz[1] + c[2] + cy[2]
    d1 = m[1] + c[2] + cx[2] + c[0] + cz[0]
    d2 = m[2] + c[0] + cy[0] + c[1] + cx[1]
    dn = m[0] + mx + m[1] + my + m[2] + mz
    return 1.0 / d0, 1.0 / d1, 1.0 / d2, 1.0 / dn


def invert(field_middle, coef_middle, field_edge, coef_edge, field, coef, diag, node):
    def assemble(c, _):
        coef[c, OFF - 1] = jnp.zeros((Y, 128), jnp.float32)
        for x in range(OFF, OFF + 16):
            coef[c, x, 0:8] = jnp.zeros((8, 128), jnp.float32)
            coef[c, x, 16:40] = coef_middle[c, x, 16:40]
            coef[c, x, 8:16] = coef_edge[c, x - OFF, 0:8]
            coef[c, x, 40:48] = coef_edge[c, x - OFF, 8:16]
        return 0

    def assemble_field(c, _):
        for x in range(OFF, OFF + 16):
            field[c, x, 16:40] = field_middle[c, x, 16:40]
            field[c, x, 8:16] = field_edge[c, x - OFF, 0:8]
            field[c, x, 40:48] = field_edge[c, x - OFF, 8:16]
        return 0

    lax.fori_loop(0, 6, assemble, 0)
    lax.fori_loop(0, 3, assemble_field, 0)

    def row(x, _):
        i = x + OFF
        m = [at(coef.at[c, i]) for c in range(3)]
        c_ = [at(coef.at[3 + c, i]) for c in range(3)]
        cy = [at(coef.at[3 + c, i], -1) for c in range(3)]
        cx = [at(coef.at[3 + c, i - 1]) for c in range(3)]
        cz = [pltpu.roll(c_[c], 1, 1) for c in range(2)]
        out = diagonals(m, c_, cy, cx, cz, at(coef.at[0, i - 1]), at(coef.at[1, i], -1), pltpu.roll(m[2], 1, 1))
        for c in range(3):
            put(diag.at[c, i], out[c])
        put(node.at[i], out[3])
        return 0

    lax.fori_loop(0, 16, row, 0)


def main(field_in, coef, diag_in, node_in, zown_low, zown_high, zlow, zhigh, field, precond, partial, sink,
         diag, node, s, phi, g, fieldS, coefS, diagS, nodeS, sS, phiS, gS):
    f32 = jnp.float32
    lane = lax.broadcasted_iota(jnp.int32, (ROWS, 128), 1)
    first_lane, last_lane = lane == 0, lane == 127
    below_half = lax.broadcasted_iota(jnp.int32, (8, 128), 0) < 4

    def z_up(value, strip, x):
        return jnp.where(last_lane, pltpu.roll(strip, (123 - 8 * x) & 127, 1), pltpu.roll(value, 127, 1))

    def z_down(value, strip, x):
        return jnp.where(first_lane, pltpu.roll(strip, (125 - 8 * x) & 127, 1), pltpu.roll(value, 1, 1))

    upper = (lane & 4) != 0
    for comp in range(9):
        lower_part, upper_part = zlow[comp % 5], zhigh[comp % 5]
        if comp >= 5:
            lower_part, upper_part = pltpu.roll(lower_part, 124, 1), pltpu.roll(upper_part, 4, 1)
        for t, value in ((0, jnp.where(upper, zown_low[comp], lower_part)),
                         (1, jnp.where(upper, upper_part, zown_high[comp]))):
            put(fieldS.at[0, comp, t] if comp < 3 else coefS.at[comp - 3, t], value)
            if comp >= 3:
                coefS[comp - 3, t, 0:8] = jnp.zeros((8, 128), f32)

    def setup_strip(t, _):
        m = [at(coefS.at[c, t]) for c in range(3)]
        c_ = [at(coefS.at[3 + c, t]) for c in range(3)]
        cy = [at(coefS.at[3 + c, t], -1) for c in range(3)]
        cx = [jnp.where(lane < 8, 0.0, pltpu.roll(v, 8, 1)) for v in c_]
        cz = [jnp.where((lane & 7) == 0, 0.0, pltpu.roll(v, 1, 1)) for v in c_]
        out = diagonals(m, c_, cy, cx, cz, pltpu.roll(m[0], 8, 1), at(coefS.at[1, t], -1), pltpu.roll(m[2], 1, 1))
        for c in range(3):
            put(diagS.at[c, t], out[c])
        put(nodeS.at[t], out[3])
        return 0

    lax.fori_loop(0, 2, setup_strip, 0)

    def setup(x, _):
        i = x + OFF
        for c in range(3):
            put(field.at[0, c, i], at(field_in.at[c, i]))
            put(diag.at[c, i], jnp.where(first_lane, pltpu.roll(at(diagS.at[c, 0]), 124 - 8 * x, 1), at(diag_in.at[c, i])))
        put(node.at[i], jnp.where(first_lane, pltpu.roll(at(nodeS.at[0]), 124 - 8 * x, 1), at(node_in.at[i])))
        return 0

    lax.fori_loop(0, 16, setup, 0)

    def fluxes(coefs, e, e0y, e0z, e1x, e1z, e2x, e2y):
        return (coefs[0] * ((e2y - e[2]) - (e1z - e[1])),
                coefs[1] * ((e0z - e[0]) - (e2x - e[2])),
                coefs[2] * ((e1x - e[1]) - (e0y - e[0])))

    def curl_back(gv, g0y, g0z, g1x, g1z, g2x, g2y):
        return ((g1z - gv[1]) - (g2y - gv[2]), (g2x - gv[2]) - (g0z - gv[0]), (g0y - gv[0]) - (g1x - gv[1]))

    def operator_step(k, _):
        now, later, before = k, k + 1, jnp.maximum(k - 1, 0)
        weight = jnp.where(k == 0, 0.0, jnp.where(k == 1, 0.5, 0.25))

        def strip_first(t, _):
            r = [at(fieldS.at[now, c, t]) for c in range(3)]
            q = ((pltpu.roll(r[0], 8, 1) - r[0]) + (at(fieldS.at[now, 1, t], -1) - r[1])) + (pltpu.roll(r[2], 1, 1) - r[2])
            put(phiS.at[t], q * at(nodeS.at[t]))
            for c in range(3):
                put(sS.at[c, t], r[c] * at(diagS.at[c, t]))
            return 0

        def strip_second(t, _):
            e = [at(sS.at[c, t]) for c in range(3)]
            out = fluxes([at(coefS.at[3 + c, t]) for c in range(3)], e,
                         at(sS.at[0, t], 1), pltpu.roll(e[0], 127, 1), pltpu.roll(e[1], 120, 1),
                         pltpu.roll(e[1], 127, 1), pltpu.roll(e[2], 120, 1), at(sS.at[2, t], 1))
            for c in range(3):
                put(gS.at[c, t], out[c])
            return 0

        def strip_third(t, _):
            gv = [at(gS.at[c, t]) for c in range(3)]
            w = curl_back(gv, at(gS.at[0, t], -1), pltpu.roll(gv[0], 1, 1), pltpu.roll(gv[1], 8, 1),
                          pltpu.roll(gv[1], 1, 1), pltpu.roll(gv[2], 8, 1), at(gS.at[2, t], -1))
            p = at(phiS.at[t])
            up = (pltpu.roll(p, 120, 1), at(phiS.at[t], 1), pltpu.roll(p, 127, 1))
            for c in range(3):
                u = at(sS.at[c, t]) + (up[c] - p)
                put(fieldS.at[later, c, t], (w[c] + at(coefS.at[c, t]) * u - at(fieldS.at[now, c, t]))
                    - weight * at(fieldS.at[before, c, t]))
            return 0

        for part in (strip_first, strip_second, strip_third):
            lax.fori_loop(0, 2, part, 0)

        def row(n_row, sums):
            i = n_row + k + 1
            x = i - OFF
            g_own = [at(g.at[c, i]) for c in range(3)]
            g_x = [at(g.at[c, i - 1]) for c in (1, 2)]
            g_y = [at(g.at[c, i], -1) for c in (0, 2)]
            p, p_x, p_y = at(phi.at[i]), at(phi.at[i + 1]), at(phi.at[i], 1)
            s_own = [at(s.at[c, i]) for c in range(3)]
            r = [at(field.at[now, c, i]) for c in range(3)]
            old = [at(field.at[before, c, i]) for c in range(3)]
            mass = [at(coef.at[c, i]) for c in range(3)]
            a = i + 1
            e = [at(s.at[c, a]) for c in range(3)]
            e_x = [at(s.at[c, a + 1]) for c in (1, 2)]
            e_y = [at(s.at[c, a], 1) for c in (0, 2)]
            curl = [at(coef.at[3 + c, a]) for c in range(3)]
            b = i + 3
            f = [at(field.at[now, c, b]) for c in range(3)]
            f_x, f_y = at(field.at[now, 0, b - 1]), at(field.at[now, 1, b], -1)
            inverse, inverse_node = [at(diag.at[c, b]) for c in range(3)], at(node.at[b])

            w = curl_back(g_own, g_y[0], z_down(g_own[0], at(gS.at[0, 0]), x), g_x[0],
                          z_down(g_own[1], at(gS.at[1, 0]), x), g_x[1], g_y[1])
            up = (p_x, p_y, z_up(p, at(phiS.at[1]), x))
            u = [s_own[c] + (up[c] - p) for c in range(3)]
            v = [((w[c] + mass[c] * u[c]) - r[c]) - weight * old[c] for c in range(3)]
            flux = fluxes(curl, e, e_y[0], z_up(e[0], at(sS.at[0, 1]), x + 1), e_x[0],
                          z_up(e[1], at(sS.at[1, 1]), x + 1), e_x[1], e_y[1])
            q = ((f_x - f[0]) + (f_y - f[1])) + (z_down(f[2], at(fieldS.at[now, 2, 0]), x + 3) - f[2])
            potential = q * inverse_node
            scaled = [f[c] * inverse[c] for c in range(3)]

            inside = (x >= 4) & (x < 12)
            to = jnp.where(inside, x - 4, 8)
            for c in range(3):
                put(field.at[later, c, i], v[c])
                put(g.at[c, a], flux[c])
                put(s.at[c, b], scaled[c])
            put(phi.at[b], potential)
            sums = list(sums)
            for c in range(3):
                precond[k, c, to] = u[c]
                for n, prod in ((0, r[c] * u[c]), (1, v[c] * u[c])):
                    ends = jnp.where(below_half, prod[32:40], prod[0:8])
                    part = ((prod[8:16] + prod[16:24]) + prod[24:32]) + ends
                    sums[n] = sums[n] + jnp.where(inside, part, 0.0)
            return tuple(sums)

        zero = jnp.zeros((8, 128), f32)
        sums = lax.fori_loop(0, 18 - 2 * k, row, (zero, zero))
        partial[2 * k] = sums[0]
        partial[2 * k + 1] = sums[1]
        return 0

    lax.fori_loop(0, 4, operator_step, 0)

    def look(x, _):
        for c in range(3):
            sink[x, c] = s[c, x + OFF, 16:24] + g[c, x + OFF, 16:24]
        sink[x, 3] = phi[x + OFF, 16:24]
        return 0

    lax.fori_loop(0, 2, look, 0)


def fold(partial, out):
    lane = lax.broadcasted_iota(jnp.int32, (1, 128), 1)
    row = jnp.zeros((1, 128), jnp.float32)
    for d in range(8):
        t = jnp.sum(partial[d], axis=0, keepdims=True)
        for shift in (64, 32, 16):
            t = t + pltpu.roll(t, shift, 1)
        row = jnp.where(lane // 16 == d, t, row)
    out[...] = jnp.broadcast_to(row, out.shape)


def finish(everyone, field, precond, solution_out, residual_out):
    total = jnp.sum(everyone[...], axis=0, keepdims=True)
    lane = lax.broadcasted_iota(jnp.int32, (1, 128), 1)
    dots = [jnp.broadcast_to(jnp.sum(jnp.where(lane // 16 == d, total, 0.0), axis=1, keepdims=True), (8, 128))
            for d in range(8)]
    size = [1.0] + [2.0 ** (1 - k) for k in range(1, 9)]
    moment = [dots[0], dots[1]]
    for k in range(1, 4):
        moment.append((dots[2 * k] * (2.0 / size[k] ** 2) - moment[0]) * size[2 * k])
        moment.append((dots[2 * k + 1] * (2.0 / (size[k] * size[k + 1])) - moment[1]) * size[2 * k + 1])
    row, earlier = moment, None
    alpha, beta = [row[1] / row[0]], [None]
    for k in range(1, 4):
        following = [None] * 8
        for l in range(k, 8 - k):
            t = row[l + 1] - alpha[k - 1] * row[l] + WEIGHT[l if l < 2 else 2] * row[l - 1]
            if k > 1:
                t = t - beta[k - 1] * earlier[l]
            following[l] = t
        alpha.append(following[k + 1] / following[k] - row[k] / row[k - 1])
        beta.append(following[k] / row[k - 1])
        row, earlier = following, row
    zero = jnp.zeros((8, 128), jnp.float32)
    older, newer = [zero] * 6, [zero + 1.0] + [zero] * 5
    value_older, value = zero, zero + 1.0
    weight = lambda l: WEIGHT[min(l, 2)]
    for k in range(4):
        nxt = []
        for l in range(6):
            t = -alpha[k] * newer[l]
            if l > 0:
                t = t + newer[l - 1]
            if l < 5:
                t = t + weight(l + 1) * newer[l + 1]
            if k > 0:
                t = t - beta[k] * older[l]
            nxt.append(t)
        step = (-1.0 - alpha[k]) * value
        if k > 0:
            step = step - beta[k] * value_older
        older, newer, value_older, value = newer, nxt, value, step
    inverse = 1.0 / value
    e = [newer[l] * inverse for l in range(5)]
    S = [None] * 4
    S[3] = -e[4]
    S[2] = -e[3] - S[3]
    S[1] = -e[2] - S[2] - weight(3) * S[3]
    S[0] = -e[1] - S[1] - weight(2) * S[2]
    e = [v[0:1] for v in e]
    S = [v[0:1] for v in S]

    def combine(x, _):
        rows, first = pl.ds(OWN, 32), pl.ds(OWN - LO, 32)
        for c in range(3):
            v = [field[k, c, x + OFF + 4, rows, :] for k in range(5)]
            u = [precond[k, c, x, first, :] for k in range(4)]
            residual_out[c, x] = (e[0] * v[0] + e[1] * v[1]) + (e[2] * v[2] + e[3] * v[3]) + e[4] * v[4]
            solution_out[c, x] = (S[0] * u[0] + S[1] * u[1]) + (S[2] * u[2] + S[3] * u[3])
        return 0

    lax.fori_loop(0, 8, combine, 0)


def shape(*dims):
    return jax.ShapeDtypeStruct(dims, jnp.float32)


def call(kernel, outs, ins, mib, scratch=(), flops=1000000):
    return pl.pallas_call(
        kernel, out_shape=outs, in_specs=[VMEM] * len(ins), out_specs=jax.tree.map(lambda _: VMEM, outs),
        scratch_shapes=list(scratch),
        compiler_params=pltpu.CompilerParams(vmem_limit_bytes=mib << 20),
        cost_estimate=pl.CostEstimate(flops=flops, bytes_accessed=1 << 20, transcendentals=0))(*ins)


def exchange(low, high, axis):
    n = lax.axis_size(axis)
    up = [(i, (i + 1) % n) for i in range(n)]
    return lax.ppermute(high, axis, up), lax.ppermute(low, axis, [(j, i) for i, j in up])


def body(right, mass, curl):
    face = (shape(3, 8, 32, 128),) + (shape(3, 4, 32, 128),) * 2
    b, *ends = call(load, face, (right,), 8)
    b = (b,) + exchange(*ends, "gx")
    c, *ends = call(load, face, (curl,), 8)
    c = (c,) + exchange(*ends, "gx")
    m, *ends = call(load_mass, face, (mass, c[0]), 8)
    m = (m,) + exchange(*ends, "gx")
    ends = (shape(9, 4, 8, 128),) * 2
    y_own = exchange(*call(pack_y_own, ends, (b[0], m[0], c[0]), 8), "gy")
    y_halo = exchange(*call(pack_y_halo, ends, b[1:] + m[1:] + c[1:], 8), "gy")
    columns = (shape(9, ROWS, 128),) * 2
    extended = (shape(3, X, Y, 128), shape(6, X, Y, 128))
    low, high, *middle = call(pack_z_middle, columns + extended, b + m + c, 8, flops=20000000)
    low, high, *ends, field, coef = call(
        pack_z_edge, columns + (shape(5, ROWS, 128),) * 2 + (shape(3, 16, 16, 128), shape(6, 16, 16, 128)),
        y_own + y_halo + (low, high, *middle), 8)
    sides = (low, high) + exchange(*ends, "gz")
    block = call(invert, extended + (shape(3, X, Y, 128), shape(X, Y, 128)), (*middle, field, coef), 8, flops=20000000)

    def held(*dims):
        return pltpu.VMEM(dims + (Y, 128), jnp.float32)

    vectors, precond, partial, _ = call(
        main, (shape(5, 3, X, Y, 128), shape(4, 3, 9, ROWS, 128), shape(8, 8, 128), shape(2, 4, 8, 128)),
        tuple(block) + sides, 20,
        [held(3, X), held(X), held(3, X), held(X), held(3, X),
         held(5, 3, 2), held(6, 2), held(3, 2), held(2), held(3, 2), held(2), held(3, 2)])
    axes = ("gx", "gy", "gz")
    devices = lax.axis_size(axes)
    (rows,) = call(fold, (shape(devices, 128),), (partial,), 4)
    everyone = lax.all_to_all(rows.reshape(devices, 1, 128), axes, 0, 0, tiled=True).reshape(devices, 128)
    return call(finish, (shape(3, 8, 32, 128),) * 2, (everyone, vectors, precond), 16)


def solution(mesh):
    spec = P(None, "gx", "gy", "gz")
    return jax.shard_map(body, mesh=mesh, in_specs=(spec,) * 3, out_specs=(spec,) * 2, check_vma=False)
```

```python
import jax
import jax.numpy as jnp
from jax import lax
from jax.experimental import pallas as pl
from jax.experimental.pallas import tpu as pltpu
from jax.sharding import PartitionSpec as P


X, Y = 24, 56
OFF, OWN = 4, 12
LO, ROWS = 8, 40
WEIGHT = (0.0, 0.5, 0.25, 0.25, 0.25)
VMEM = pl.BlockSpec(memory_space=pltpu.VMEM)


def load(source, own, low, high):
    def move(c, _):
        for to, x in ((low, 0), (high, 4)):
            value = source[c, x : x + 4]
            own[c, x : x + 4] = value
            to[c] = value
        return 0

    lax.fori_loop(0, 3, move, 0)


def load_mass(source, curl, own, low, high):
    load(source, own, low, high)
    high[1, 0] = source[1, 4] + curl[2, 3]
    high[2, 0] = source[2, 4] + curl[1, 3]


def pack_y(pairs, *refs):
    refs, (low, high) = refs[:-2], refs[-2:]
    n = len(refs) // 3
    sub = lax.broadcasted_iota(jnp.int32, (8, 128), 0)

    def tile(field, c, p, half, y):
        return pairs(refs[field * n : field * n + n], c, p, half, y)

    def pack(c, _):
        for field in range(3):
            for p in range(4):
                a, b = tile(field, c, p, 0, 0), tile(field, c, p, 1, 0)
                low[3 * field + c, p] = jnp.where(sub < 4, a, pltpu.roll(b, 4, 0))
                a, b = tile(field, c, p, 0, 24), tile(field, c, p, 1, 24)
                high[3 * field + c, p] = jnp.where(sub < 4, pltpu.roll(a, 4, 0), b)
        return 0

    lax.fori_loop(0, 3, pack, 0)

    def corrected(i, _):
        c, other = 2 * i, 2 - 2 * i
        for p in range(4):
            a = pltpu.roll(tile(2, other, p, 0, 24), 5, 0)
            b = pltpu.roll(tile(2, other, p, 1, 24), 1, 0)
            high[3 + c, p] = high[3 + c, p] + jnp.where(sub == 0, a, jnp.where(sub == 4, b, 0.0))
        return 0

    lax.fori_loop(0, 2, corrected, 0)


def pack_y_own(*refs):
    pack_y(lambda own, c, p, half, y: own[0][c, p + 4 * half, y : y + 8], *refs)


def pack_y_halo(after, *refs):
    pack_y(lambda ends, c, p, half, y: ends[half][c, p, y : y + 8], *refs)


def strips(source, base, count, octets, low, high, xs, before):
    group = lax.broadcasted_iota(jnp.int32, (8, 128), 1) >> 2
    each, x0, start, begin, stride = octets

    def one(i, _):
        comp, o = i // each, i % each
        here = pl.ds(pl.multiple_of(start + 8 * o, 8), 8)
        to = pl.ds(pl.multiple_of(begin + stride * o, 8), 8)
        first, last = (jnp.zeros((8, 128), jnp.float32),) * 2
        if before:
            first, last = before[0][comp + base, to, :], before[1][comp + base, to, :]
        for x in xs:
            t = source[comp, x0 + x, here, :]
            first = jnp.where(group == 2 * x + 1, pltpu.roll(t, 8 * x + 4, 1), first)
            last = jnp.where(group == 2 * x, pltpu.roll(t, (8 * x + 4) % 128, 1), last)
        low[comp + base, to, :] = first
        high[comp + base, to, :] = last
        return 0

    lax.fori_loop(0, count * each, one, 0)


def all_strips(field, coef, octets, low, high, xs=range(16), before=None):
    strips(field, 0, 3, octets, low, high, xs, before)
    strips(coef, 3, 6, octets, low, high, xs, before)
    lane = lax.broadcasted_iota(jnp.int32, (8, 128), 1)
    each, x0, start, begin, stride = octets

    def corrected(i, _):
        which, o = i // each, i % each
        here = pl.ds(pl.multiple_of(start + 8 * o, 8), 8)
        to = pl.ds(pl.multiple_of(begin + stride * o, 8), 8)
        last = jnp.zeros((8, 128), jnp.float32)
        for x in xs:
            t = coef[4 - which, x0 + x, here, :]
            last = jnp.where(lane == 8 * x, pltpu.roll(t, (8 * x + 5) % 128, 1), last)
        high[3 + which, to, :] = high[3 + which, to, :] + last
        return 0

    lax.fori_loop(0, 2 * each, corrected, 0)


def pack_z_own(right, mass, curl, low, high, field, coef):
    def assemble(c, _):
        for to, source in ((field.at[c], right), (coef.at[c], mass), (coef.at[3 + c], curl)):
            to[:, 4:36] = source[c]
        return 0

    lax.fori_loop(0, 3, assemble, 0)
    all_strips(field, coef, (3, -4, 8, 8, 8), low, high, range(4, 12))


def pack_z_middle(*refs):
    blocks = refs[0:2], refs[2:4], refs[4:6]
    own_low, own_high, own_field, own_coef, low, high, field, coef = refs[6:]

    def assemble(c, _):
        for n, (below, above) in enumerate(blocks):
            to = field.at[c] if n == 0 else coef.at[3 * n - 3 + c]
            own = own_field.at[c] if n == 0 else own_coef.at[3 * n - 3 + c]
            to[OFF : OFF + 4, OWN : OWN + 32] = below[c]
            to[OFF + 4 : OFF + 12, LO : LO + ROWS] = own[...]
            to[OFF + 12 : OFF + 16, OWN : OWN + 32] = above[c]
        return 0

    lax.fori_loop(0, 3, assemble, 0)
    ends = (0, 1, 2, 3, 12, 13, 14, 15)
    all_strips(field, coef, (3, OFF, 16, 8, 8), low, high, ends, (own_low, own_high))


def pack_z_edge(own_low, own_high, halo_low, halo_high, middle_low, middle_high, middle_field, middle_coef,
                low, high, send_low, send_high, field, coef):
    sub = lax.broadcasted_iota(jnp.int32, (8, 128), 0)

    def assemble(c, _):
        for n in range(3):
            to = field.at[c] if n == 0 else coef.at[3 * n - 3 + c]
            source = middle_field.at[c] if n == 0 else middle_coef.at[3 * n - 3 + c]
            comp = 3 * n + c
            for p in range(4):
                for lows, highs, x0, x1 in ((halo_low, halo_high, p, p + 12), (own_low, own_high, p + 4, p + 8)):
                    lower, upper = lows[comp, p], highs[comp, p]
                    to[x0, 0:8] = jnp.where(sub < 4, lower, source[OFF + x0, 8:16])
                    to[x1, 0:8] = jnp.where(sub < 4, pltpu.roll(lower, 4, 0), source[OFF + x1, 8:16])
                    to[x0, 8:16] = jnp.where(sub < 4, source[OFF + x0, 40:48], pltpu.roll(upper, 4, 0))
                    to[x1, 8:16] = jnp.where(sub < 4, source[OFF + x1, 40:48], upper)
        return 0

    lax.fori_loop(0, 3, assemble, 0)
    all_strips(field, coef, (2, 0, 0, 0, 32), low, high)
    for comp in range(9):
        low[comp, 8:32] = middle_low[comp, 8:32]
        high[comp, 8:32] = middle_high[comp, 8:32]
    for n in range(5):
        down, up = low[n], high[n]
        if n < 4:
            down, up = down + pltpu.roll(low[n + 5], 124, 1), up + pltpu.roll(high[n + 5], 4, 1)
        send_low[n] = down
        send_high[n] = up


def at(ref, dy=0):
    return ref[pl.ds(LO + dy, ROWS), :]


def put(ref, value):
    ref[pl.ds(LO, ROWS), :] = value


def diagonals(m, c, cy, cx, cz, mx, my, mz):
    d0 = m[0] + c[1] + cz[1] + c[2] + cy[2]
    d1 = m[1] + c[2] + cx[2] + c[0] + cz[0]
    d2 = m[2] + c[0] + cy[0] + c[1] + cx[1]
    dn = m[0] + mx + m[1] + my + m[2] + mz
    return 1.0 / d0, 1.0 / d1, 1.0 / d2, 1.0 / dn


def invert(field_middle, coef_middle, field_edge, coef_edge, field, coef, diag, node):
    def assemble(c, _):
        coef[c, OFF - 1] = jnp.zeros((Y, 128), jnp.float32)
        for x in range(OFF, OFF + 16):
            coef[c, x, 0:8] = jnp.zeros((8, 128), jnp.float32)
            coef[c, x, 16:40] = coef_middle[c, x, 16:40]
            coef[c, x, 8:16] = coef_edge[c, x - OFF, 0:8]
            coef[c, x, 40:48] = coef_edge[c, x - OFF, 8:16]
        return 0

    def assemble_field(c, _):
        for x in range(OFF, OFF + 16):
            field[c, x, 16:40] = field_middle[c, x, 16:40]
            field[c, x, 8:16] = field_edge[c, x - OFF, 0:8]
            field[c, x, 40:48] = field_edge[c, x - OFF, 8:16]
        return 0

    lax.fori_loop(0, 6, assemble, 0)
    lax.fori_loop(0, 3, assemble_field, 0)

    def row(x, _):
        i = x + OFF
        m = [at(coef.at[c, i]) for c in range(3)]
        c_ = [at(coef.at[3 + c, i]) for c in range(3)]
        cy = [at(coef.at[3 + c, i], -1) for c in range(3)]
        cx = [at(coef.at[3 + c, i - 1]) for c in range(3)]
        cz = [pltpu.roll(c_[c], 1, 1) for c in range(2)]
        out = diagonals(m, c_, cy, cx, cz, at(coef.at[0, i - 1]), at(coef.at[1, i], -1), pltpu.roll(m[2], 1, 1))
        for c in range(3):
            put(diag.at[c, i], out[c])
        put(node.at[i], out[3])
        return 0

    lax.fori_loop(0, 16, row, 0)


def main(field_in, coef, diag_in, node_in, zown_low, zown_high, zlow, zhigh, field, precond, partial, sink,
         diag, node, s, phi, g, fieldS, coefS, diagS, nodeS, sS, phiS, gS, dots):
    f32 = jnp.float32
    lane = lax.broadcasted_iota(jnp.int32, (ROWS, 128), 1)
    first_lane, last_lane = lane == 0, lane == 127
    below_half = lax.broadcasted_iota(jnp.int32, (8, 128), 0) < 4

    def z_up(value, strip, x):
        return jnp.where(last_lane, pltpu.roll(strip, (123 - 8 * x) & 127, 1), pltpu.roll(value, 127, 1))

    def z_down(value, strip, x):
        return jnp.where(first_lane, pltpu.roll(strip, (125 - 8 * x) & 127, 1), pltpu.roll(value, 1, 1))

    upper = (lane & 4) != 0
    for comp in range(9):
        lower_part, upper_part = zlow[comp % 5], zhigh[comp % 5]
        if comp >= 5:
            lower_part, upper_part = pltpu.roll(lower_part, 124, 1), pltpu.roll(upper_part, 4, 1)
        for t, value in ((0, jnp.where(upper, zown_low[comp], lower_part)),
                         (1, jnp.where(upper, upper_part, zown_high[comp]))):
            put(fieldS.at[0, comp, t] if comp < 3 else coefS.at[comp - 3, t], value)
            if comp >= 3:
                coefS[comp - 3, t, 0:8] = jnp.zeros((8, 128), f32)

    def setup_strip(t, _):
        m = [at(coefS.at[c, t]) for c in range(3)]
        c_ = [at(coefS.at[3 + c, t]) for c in range(3)]
        cy = [at(coefS.at[3 + c, t], -1) for c in range(3)]
        cx = [jnp.where(lane < 8, 0.0, pltpu.roll(v, 8, 1)) for v in c_]
        cz = [jnp.where((lane & 7) == 0, 0.0, pltpu.roll(v, 1, 1)) for v in c_]
        out = diagonals(m, c_, cy, cx, cz, pltpu.roll(m[0], 8, 1), at(coefS.at[1, t], -1), pltpu.roll(m[2], 1, 1))
        for c in range(3):
            put(diagS.at[c, t], out[c])
        put(nodeS.at[t], out[3])
        return 0

    lax.fori_loop(0, 2, setup_strip, 0)

    def setup(x, _):
        i = x + OFF
        for c in range(3):
            put(field.at[0, c, i], at(field_in.at[c, i]))
            put(diag.at[c, i], jnp.where(first_lane, pltpu.roll(at(diagS.at[c, 0]), 124 - 8 * x, 1), at(diag_in.at[c, i])))
        put(node.at[i], jnp.where(first_lane, pltpu.roll(at(nodeS.at[0]), 124 - 8 * x, 1), at(node_in.at[i])))
        return 0

    lax.fori_loop(0, 16, setup, 0)

    def fluxes(coefs, e, e0y, e0z, e1x, e1z, e2x, e2y):
        return (coefs[0] * ((e2y - e[2]) - (e1z - e[1])),
                coefs[1] * ((e0z - e[0]) - (e2x - e[2])),
                coefs[2] * ((e1x - e[1]) - (e0y - e[0])))

    def curl_back(gv, g0y, g0z, g1x, g1z, g2x, g2y):
        return ((g1z - gv[1]) - (g2y - gv[2]), (g2x - gv[2]) - (g0z - gv[0]), (g0y - gv[0]) - (g1x - gv[1]))

    def operator_step(k, _):
        now, later, before = k, k + 1, jnp.maximum(k - 1, 0)
        weight = jnp.where(k == 0, 0.0, jnp.where(k == 1, 0.5, 0.25))

        def strip_first(t, _):
            r = [at(fieldS.at[now, c, t]) for c in range(3)]
            q = ((pltpu.roll(r[0], 8, 1) - r[0]) + (at(fieldS.at[now, 1, t], -1) - r[1])) + (pltpu.roll(r[2], 1, 1) - r[2])
            put(phiS.at[t], q * at(nodeS.at[t]))
            for c in range(3):
                put(sS.at[c, t], r[c] * at(diagS.at[c, t]))
            return 0

        def strip_second(t, _):
            e = [at(sS.at[c, t]) for c in range(3)]
            out = fluxes([at(coefS.at[3 + c, t]) for c in range(3)], e,
                         at(sS.at[0, t], 1), pltpu.roll(e[0], 127, 1), pltpu.roll(e[1], 120, 1),
                         pltpu.roll(e[1], 127, 1), pltpu.roll(e[2], 120, 1), at(sS.at[2, t], 1))
            for c in range(3):
                put(gS.at[c, t], out[c])
            return 0

        def strip_third(t, _):
            gv = [at(gS.at[c, t]) for c in range(3)]
            w = curl_back(gv, at(gS.at[0, t], -1), pltpu.roll(gv[0], 1, 1), pltpu.roll(gv[1], 8, 1),
                          pltpu.roll(gv[1], 1, 1), pltpu.roll(gv[2], 8, 1), at(gS.at[2, t], -1))
            p = at(phiS.at[t])
            up = (pltpu.roll(p, 120, 1), at(phiS.at[t], 1), pltpu.roll(p, 127, 1))
            for c in range(3):
                u = at(sS.at[c, t]) + (up[c] - p)
                put(fieldS.at[later, c, t], (w[c] + at(coefS.at[c, t]) * u - at(fieldS.at[now, c, t]))
                    - weight * at(fieldS.at[before, c, t]))
            return 0

        for part in (strip_first, strip_second, strip_third):
            lax.fori_loop(0, 2, part, 0)

        def scale(n_row, _):
            x = n_row + k
            b = x + OFF
            f = [at(field.at[now, c, b]) for c in range(3)]
            q = ((at(field.at[now, 0, b - 1]) - f[0]) + (at(field.at[now, 1, b], -1) - f[1])) + (
                z_down(f[2], at(fieldS.at[now, 2, 0]), x) - f[2])
            for c in range(3):
                put(s.at[c, b], f[c] * at(diag.at[c, b]))
            put(phi.at[b], q * at(node.at[b]))
            return 0

        lax.fori_loop(0, 2, scale, 0)

        def row(n_row, sums):
            i = n_row + k + 3
            x = i - OFF
            g_own = [at(g.at[c, i]) for c in range(3)]
            g_x = [at(g.at[c, i - 1]) for c in (1, 2)]
            g_y = [at(g.at[c, i], -1) for c in (0, 2)]
            p, p_x, p_y = at(phi.at[i]), at(phi.at[i + 1]), at(phi.at[i], 1)
            s_own = [at(s.at[c, i]) for c in range(3)]
            r = [at(field.at[now, c, i]) for c in range(3)]
            old = [at(field.at[before, c, i]) for c in range(3)]
            mass = [at(coef.at[c, i]) for c in range(3)]
            a = i + 1
            e = [at(s.at[c, a]) for c in range(3)]
            e_x = [at(s.at[c, a + 1]) for c in (1, 2)]
            e_y = [at(s.at[c, a], 1) for c in (0, 2)]
            curl = [at(coef.at[3 + c, a]) for c in range(3)]
            b = i + 3
            f = [at(field.at[now, c, b]) for c in range(3)]
            f_x, f_y = at(field.at[now, 0, b - 1]), at(field.at[now, 1, b], -1)
            inverse, inverse_node = [at(diag.at[c, b]) for c in range(3)], at(node.at[b])

            w = curl_back(g_own, g_y[0], z_down(g_own[0], at(gS.at[0, 0]), x), g_x[0],
                          z_down(g_own[1], at(gS.at[1, 0]), x), g_x[1], g_y[1])
            up = (p_x, p_y, z_up(p, at(phiS.at[1]), x))
            u = [s_own[c] + (up[c] - p) for c in range(3)]
            v = [((w[c] + mass[c] * u[c]) - r[c]) - weight * old[c] for c in range(3)]
            flux = fluxes(curl, e, e_y[0], z_up(e[0], at(sS.at[0, 1]), x + 1), e_x[0],
                          z_up(e[1], at(sS.at[1, 1]), x + 1), e_x[1], e_y[1])
            q = ((f_x - f[0]) + (f_y - f[1])) + (z_down(f[2], at(fieldS.at[now, 2, 0]), x + 3) - f[2])
            potential = q * inverse_node
            scaled = [f[c] * inverse[c] for c in range(3)]

            inside = (x >= 4) & (x < 12)
            to = jnp.where(inside, x - 4, 8)
            for c in range(3):
                put(field.at[later, c, i], v[c])
                put(g.at[c, a], flux[c])
                put(s.at[c, b], scaled[c])
            put(phi.at[b], potential)
            sums = list(sums)
            for c in range(3):
                precond[k, c, to] = u[c]
                for n, prod in ((0, r[c] * u[c]), (1, v[c] * u[c])):
                    ends = jnp.where(below_half, prod[32:40], prod[0:8])
                    part = ((prod[8:16] + prod[16:24]) + prod[24:32]) + ends
                    sums[n] = sums[n] + jnp.where(inside, part, 0.0)
            return tuple(sums)

        zero = jnp.zeros((8, 128), f32)
        sums = lax.fori_loop(0, 16 - 2 * k, row, (zero, zero))
        dots[2 * k] = sums[0]
        dots[2 * k + 1] = sums[1]
        return 0

    lax.fori_loop(0, 4, operator_step, 0)

    row_lane = lax.broadcasted_iota(jnp.int32, (1, 128), 1) // 16
    parts = [jnp.sum(dots[d], axis=0, keepdims=True) for d in range(8)]
    for shift in (64, 32, 16):
        parts = [t + pltpu.roll(t, shift, 1) for t in parts]
    moments = parts[0]
    for d in range(1, 8):
        moments = jnp.where(row_lane == d, parts[d], moments)
    partial[...] = jnp.broadcast_to(moments, partial.shape)

    def look(x, _):
        for c in range(3):
            sink[x, c] = s[c, x + OFF, 16:24] + g[c, x + OFF, 16:24]
        sink[x, 3] = phi[x + OFF, 16:24]
        return 0

    lax.fori_loop(0, 2, look, 0)


def finish(everyone, field, precond, solution_out, residual_out):
    total = jnp.sum(everyone[...], axis=0, keepdims=True)
    lane = lax.broadcasted_iota(jnp.int32, (1, 128), 1)
    dots = [jnp.broadcast_to(jnp.sum(jnp.where(lane // 16 == d, total, 0.0), axis=1, keepdims=True), (8, 128))
            for d in range(8)]
    size = [1.0] + [2.0 ** (1 - k) for k in range(1, 9)]
    moment = [dots[0], dots[1]]
    for k in range(1, 4):
        moment.append((dots[2 * k] * (2.0 / size[k] ** 2) - moment[0]) * size[2 * k])
        moment.append((dots[2 * k + 1] * (2.0 / (size[k] * size[k + 1])) - moment[1]) * size[2 * k + 1])
    row, earlier = moment, None
    alpha, beta = [row[1] / row[0]], [None]
    for k in range(1, 4):
        following = [None] * 8
        for l in range(k, 8 - k):
            t = row[l + 1] - alpha[k - 1] * row[l] + WEIGHT[l if l < 2 else 2] * row[l - 1]
            if k > 1:
                t = t - beta[k - 1] * earlier[l]
            following[l] = t
        alpha.append(following[k + 1] / following[k] - row[k] / row[k - 1])
        beta.append(following[k] / row[k - 1])
        row, earlier = following, row
    zero = jnp.zeros((8, 128), jnp.float32)
    older, newer = [zero] * 6, [zero + 1.0] + [zero] * 5
    value_older, value = zero, zero + 1.0
    weight = lambda l: WEIGHT[min(l, 2)]
    for k in range(4):
        nxt = []
        for l in range(6):
            t = -alpha[k] * newer[l]
            if l > 0:
                t = t + newer[l - 1]
            if l < 5:
                t = t + weight(l + 1) * newer[l + 1]
            if k > 0:
                t = t - beta[k] * older[l]
            nxt.append(t)
        step = (-1.0 - alpha[k]) * value
        if k > 0:
            step = step - beta[k] * value_older
        older, newer, value_older, value = newer, nxt, value, step
    inverse = 1.0 / value
    e = [newer[l] * inverse for l in range(5)]
    S = [None] * 4
    S[3] = -e[4]
    S[2] = -e[3] - S[3]
    S[1] = -e[2] - S[2] - weight(3) * S[3]
    S[0] = -e[1] - S[1] - weight(2) * S[2]
    e = [v[0:1] for v in e]
    S = [v[0:1] for v in S]

    def combine(x, _):
        rows, first = pl.ds(OWN, 32), pl.ds(OWN - LO, 32)
        for c in range(3):
            v = [field[k, c, x + OFF + 4, rows, :] for k in range(5)]
            u = [precond[k, c, x, first, :] for k in range(4)]
            residual_out[c, x] = (e[0] * v[0] + e[1] * v[1]) + (e[2] * v[2] + e[3] * v[3]) + e[4] * v[4]
            solution_out[c, x] = (S[0] * u[0] + S[1] * u[1]) + (S[2] * u[2] + S[3] * u[3])
        return 0

    lax.fori_loop(0, 8, combine, 0)


def shape(*dims):
    return jax.ShapeDtypeStruct(dims, jnp.float32)


def call(kernel, outs, ins, mib, scratch=(), flops=1000000):
    return pl.pallas_call(
        kernel, out_shape=outs, in_specs=[VMEM] * len(ins), out_specs=jax.tree.map(lambda _: VMEM, outs),
        scratch_shapes=list(scratch),
        compiler_params=pltpu.CompilerParams(vmem_limit_bytes=mib << 20),
        cost_estimate=pl.CostEstimate(flops=flops, bytes_accessed=1 << 20, transcendentals=0))(*ins)


def exchange(low, high, axis):
    n = lax.axis_size(axis)
    up = [(i, (i + 1) % n) for i in range(n)]
    return lax.ppermute(high, axis, up), lax.ppermute(low, axis, [(j, i) for i, j in up])


def body(right, mass, curl):
    face = (shape(3, 8, 32, 128),) + (shape(3, 4, 32, 128),) * 2
    b, *ends = call(load, face, (right,), 8)
    b = (b,) + exchange(*ends, "gx")
    c, *ends = call(load, face, (curl,), 8)
    c = (c,) + exchange(*ends, "gx")
    m, *ends = call(load_mass, face, (mass, c[0]), 8)
    m = (m,) + exchange(*ends, "gx")
    ends = (shape(9, 4, 8, 128),) * 2
    y_own = exchange(*call(pack_y_own, ends, (b[0], m[0], c[0]), 8), "gy")
    columns = (shape(9, ROWS, 128),) * 2
    extended = (shape(3, X, Y, 128), shape(6, X, Y, 128))
    own = call(pack_z_own, columns + (shape(3, 8, ROWS, 128), shape(6, 8, ROWS, 128)), (b[0], m[0], c[0]), 8, flops=20000000)
    y_halo = exchange(*call(pack_y_halo, ends, (own[0],) + b[1:] + m[1:] + c[1:], 8), "gy")
    low, high, *middle = call(pack_z_middle, columns + extended, b[1:] + m[1:] + c[1:] + tuple(own), 8, flops=20000000)
    low, high, *ends, field, coef = call(
        pack_z_edge, columns + (shape(5, ROWS, 128),) * 2 + (shape(3, 16, 16, 128), shape(6, 16, 16, 128)),
        y_own + y_halo + (low, high, *middle), 8)
    sides = (low, high) + exchange(*ends, "gz")
    block = call(invert, extended + (shape(3, X, Y, 128), shape(X, Y, 128)), (*middle, field, coef), 8, flops=20000000)

    def held(*dims):
        return pltpu.VMEM(dims + (Y, 128), jnp.float32)

    axes = ("gx", "gy", "gz")
    devices = lax.axis_size(axes)
    vectors, precond, rows, _ = call(
        main, (shape(5, 3, X, Y, 128), shape(4, 3, 9, ROWS, 128), shape(devices, 128), shape(2, 4, 8, 128)),
        tuple(block) + sides, 20,
        [held(3, X), held(X), held(3, X), held(X), held(3, X),
         held(5, 3, 2), held(6, 2), held(3, 2), held(2), held(3, 2), held(2), held(3, 2), pltpu.VMEM((8, 8, 128), jnp.float32)])
    everyone = lax.all_to_all(rows.reshape(devices, 1, 128), axes, 0, 0, tiled=True).reshape(devices, 128)
    return call(finish, (shape(3, 8, 32, 128),) * 2, (everyone, vectors, precond), 16)


def solution(mesh):
    spec = P(None, "gx", "gy", "gz")
    return jax.shard_map(body, mesh=mesh, in_specs=(spec,) * 3, out_specs=(spec,) * 2, check_vma=False)
```

```python
import jax
import jax.numpy as jnp
from jax import lax
from jax.experimental import pallas as pl
from jax.experimental.pallas import tpu as pltpu
from jax.sharding import PartitionSpec as P


X, Y = 24, 56
OFF, OWN = 4, 12
LO, ROWS = 8, 40
WEIGHT = (0.0, 0.5, 0.25, 0.25, 0.25)
VMEM = pl.BlockSpec(memory_space=pltpu.VMEM)


def load(source, own, low, high):
    def move(c, _):
        for to, x in ((low, 0), (high, 4)):
            value = source[c, x : x + 4]
            own[c, x : x + 4] = value
            to[c] = value
        return 0

    lax.fori_loop(0, 3, move, 0)


def load_mass(source, curl, own, low, high):
    load(source, own, low, high)
    high[1, 0] = source[1, 4] + curl[2, 3]
    high[2, 0] = source[2, 4] + curl[1, 3]


def pack_y(pairs, *refs):
    refs, (low, high) = refs[:-2], refs[-2:]
    n = len(refs) // 3
    sub = lax.broadcasted_iota(jnp.int32, (8, 128), 0)

    def tile(field, c, p, half, y):
        return pairs(refs[field * n : field * n + n], c, p, half, y)

    def pack(c, _):
        for field in range(3):
            for p in range(4):
                a, b = tile(field, c, p, 0, 0), tile(field, c, p, 1, 0)
                low[3 * field + c, p] = jnp.where(sub < 4, a, pltpu.roll(b, 4, 0))
                a, b = tile(field, c, p, 0, 24), tile(field, c, p, 1, 24)
                high[3 * field + c, p] = jnp.where(sub < 4, pltpu.roll(a, 4, 0), b)
        return 0

    lax.fori_loop(0, 3, pack, 0)

    def corrected(i, _):
        c, other = 2 * i, 2 - 2 * i
        for p in range(4):
            a = pltpu.roll(tile(2, other, p, 0, 24), 5, 0)
            b = pltpu.roll(tile(2, other, p, 1, 24), 1, 0)
            high[3 + c, p] = high[3 + c, p] + jnp.where(sub == 0, a, jnp.where(sub == 4, b, 0.0))
        return 0

    lax.fori_loop(0, 2, corrected, 0)


def pack_y_own(*refs):
    pack_y(lambda own, c, p, half, y: own[0][c, p + 4 * half, y : y + 8], *refs)


def pack_y_halo(after, *refs):
    pack_y(lambda ends, c, p, half, y: ends[half][c, p, y : y + 8], *refs)


def strips(source, base, count, octets, low, high, xs, before):
    group = lax.broadcasted_iota(jnp.int32, (8, 128), 1) >> 2
    each, x0, start, begin, stride = octets

    def one(i, _):
        comp, o = i // each, i % each
        here = pl.ds(pl.multiple_of(start + 8 * o, 8), 8)
        to = pl.ds(pl.multiple_of(begin + stride * o, 8), 8)
        first, last = (jnp.zeros((8, 128), jnp.float32),) * 2
        if before:
            first, last = before[0][comp + base, to, :], before[1][comp + base, to, :]
        for x in xs:
            t = source[comp, x0 + x, here, :]
            first = jnp.where(group == 2 * x + 1, pltpu.roll(t, 8 * x + 4, 1), first)
            last = jnp.where(group == 2 * x, pltpu.roll(t, (8 * x + 4) % 128, 1), last)
        low[comp + base, to, :] = first
        high[comp + base, to, :] = last
        return 0

    lax.fori_loop(0, count * each, one, 0)


def all_strips(field, coef, octets, low, high, xs=range(16), before=None):
    strips(field, 0, 3, octets, low, high, xs, before)
    strips(coef, 3, 6, octets, low, high, xs, before)
    lane = lax.broadcasted_iota(jnp.int32, (8, 128), 1)
    each, x0, start, begin, stride = octets

    def corrected(i, _):
        which, o = i // each, i % each
        here = pl.ds(pl.multiple_of(start + 8 * o, 8), 8)
        to = pl.ds(pl.multiple_of(begin + stride * o, 8), 8)
        last = jnp.zeros((8, 128), jnp.float32)
        for x in xs:
            t = coef[4 - which, x0 + x, here, :]
            last = jnp.where(lane == 8 * x, pltpu.roll(t, (8 * x + 5) % 128, 1), last)
        high[3 + which, to, :] = high[3 + which, to, :] + last
        return 0

    lax.fori_loop(0, 2 * each, corrected, 0)


def pack_z_own(right, mass, curl, low, high, field, coef):
    def assemble(c, _):
        for to, source in ((field.at[c], right), (coef.at[c], mass), (coef.at[3 + c], curl)):
            to[:, 4:36] = source[c]
        return 0

    lax.fori_loop(0, 3, assemble, 0)
    all_strips(field, coef, (3, -4, 8, 8, 8), low, high, range(4, 12))


def pack_z_middle(*refs):
    blocks = refs[0:2], refs[2:4], refs[4:6]
    own_low, own_high, own_field, own_coef, low, high, field, coef = refs[6:]

    def assemble(c, _):
        for n, (below, above) in enumerate(blocks):
            to = field.at[c] if n == 0 else coef.at[3 * n - 3 + c]
            own = own_field.at[c] if n == 0 else own_coef.at[3 * n - 3 + c]
            to[OFF : OFF + 4, OWN : OWN + 32] = below[c]
            to[OFF + 4 : OFF + 12, LO : LO + ROWS] = own[...]
            to[OFF + 12 : OFF + 16, OWN : OWN + 32] = above[c]
        return 0

    lax.fori_loop(0, 3, assemble, 0)
    ends = (0, 1, 2, 3, 12, 13, 14, 15)
    all_strips(field, coef, (3, OFF, 16, 8, 8), low, high, ends, (own_low, own_high))


def pack_z_edge(own_low, own_high, halo_low, halo_high, middle_low, middle_high, middle_field, middle_coef,
                low, high, send_low, send_high, field, coef):
    sub = lax.broadcasted_iota(jnp.int32, (8, 128), 0)

    def assemble(c, _):
        for n in range(3):
            to = field.at[c] if n == 0 else coef.at[3 * n - 3 + c]
            source = middle_field.at[c] if n == 0 else middle_coef.at[3 * n - 3 + c]
            comp = 3 * n + c
            for p in range(4):
                for lows, highs, x0, x1 in ((halo_low, halo_high, p, p + 12), (own_low, own_high, p + 4, p + 8)):
                    lower, upper = lows[comp, p], highs[comp, p]
                    to[x0, 0:8] = jnp.where(sub < 4, lower, source[OFF + x0, 8:16])
                    to[x1, 0:8] = jnp.where(sub < 4, pltpu.roll(lower, 4, 0), source[OFF + x1, 8:16])
                    to[x0, 8:16] = jnp.where(sub < 4, source[OFF + x0, 40:48], pltpu.roll(upper, 4, 0))
                    to[x1, 8:16] = jnp.where(sub < 4, source[OFF + x1, 40:48], upper)
        return 0

    lax.fori_loop(0, 3, assemble, 0)
    all_strips(field, coef, (2, 0, 0, 0, 32), low, high)
    for comp in range(9):
        low[comp, 8:32] = middle_low[comp, 8:32]
        high[comp, 8:32] = middle_high[comp, 8:32]
    for n in range(5):
        down, up = low[n], high[n]
        if n < 4:
            down, up = down + pltpu.roll(low[n + 5], 124, 1), up + pltpu.roll(high[n + 5], 4, 1)
        send_low[n] = down
        send_high[n] = up


def at(ref, dy=0):
    return ref[pl.ds(LO + dy, ROWS), :]


def put(ref, value):
    ref[pl.ds(LO, ROWS), :] = value


def diagonals(m, c, cy, cx, cz, mx, my, mz):
    d0 = m[0] + c[1] + cz[1] + c[2] + cy[2]
    d1 = m[1] + c[2] + cx[2] + c[0] + cz[0]
    d2 = m[2] + c[0] + cy[0] + c[1] + cx[1]
    dn = m[0] + mx + m[1] + my + m[2] + mz
    return 1.0 / d0, 1.0 / d1, 1.0 / d2, 1.0 / dn


def invert(field_middle, coef_middle, field_edge, coef_edge, field, coef, diag, node):
    def assemble(c, _):
        coef[c, OFF - 1] = jnp.zeros((Y, 128), jnp.float32)
        for x in range(OFF, OFF + 16):
            coef[c, x, 0:8] = jnp.zeros((8, 128), jnp.float32)
            coef[c, x, 16:40] = coef_middle[c, x, 16:40]
            coef[c, x, 8:16] = coef_edge[c, x - OFF, 0:8]
            coef[c, x, 40:48] = coef_edge[c, x - OFF, 8:16]
        return 0

    def assemble_field(c, _):
        for x in range(OFF, OFF + 16):
            field[c, x, 16:40] = field_middle[c, x, 16:40]
            field[c, x, 8:16] = field_edge[c, x - OFF, 0:8]
            field[c, x, 40:48] = field_edge[c, x - OFF, 8:16]
        return 0

    lax.fori_loop(0, 6, assemble, 0)
    lax.fori_loop(0, 3, assemble_field, 0)

    def row(x, _):
        i = x + OFF
        m = [at(coef.at[c, i]) for c in range(3)]
        c_ = [at(coef.at[3 + c, i]) for c in range(3)]
        cy = [at(coef.at[3 + c, i], -1) for c in range(3)]
        cx = [at(coef.at[3 + c, i - 1]) for c in range(3)]
        cz = [pltpu.roll(c_[c], 1, 1) for c in range(2)]
        out = diagonals(m, c_, cy, cx, cz, at(coef.at[0, i - 1]), at(coef.at[1, i], -1), pltpu.roll(m[2], 1, 1))
        for c in range(3):
            put(diag.at[c, i], out[c])
        put(node.at[i], out[3])
        return 0

    lax.fori_loop(0, 16, row, 0)


def main(field_in, coef, diag_in, node_in, zown_low, zown_high, zlow, zhigh, field, precond, partial, sink,
         diag, node, s, phi, g, fieldS, coefS, diagS, nodeS, sS, phiS, gS, dots):
    f32 = jnp.float32
    lane = lax.broadcasted_iota(jnp.int32, (ROWS, 128), 1)
    first_lane, last_lane = lane == 0, lane == 127
    below_half = lax.broadcasted_iota(jnp.int32, (8, 128), 0) < 4

    def z_up(value, strip, x):
        return jnp.where(last_lane, pltpu.roll(strip, (123 - 8 * x) & 127, 1), pltpu.roll(value, 127, 1))

    def z_down(value, strip, x):
        return jnp.where(first_lane, pltpu.roll(strip, (125 - 8 * x) & 127, 1), pltpu.roll(value, 1, 1))

    upper = (lane & 4) != 0
    for comp in range(9):
        lower_part, upper_part = zlow[comp % 5], zhigh[comp % 5]
        if comp >= 5:
            lower_part, upper_part = pltpu.roll(lower_part, 124, 1), pltpu.roll(upper_part, 4, 1)
        for t, value in ((0, jnp.where(upper, zown_low[comp], lower_part)),
                         (1, jnp.where(upper, upper_part, zown_high[comp]))):
            put(fieldS.at[0, comp, t] if comp < 3 else coefS.at[comp - 3, t], value)
            if comp >= 3:
                coefS[comp - 3, t, 0:8] = jnp.zeros((8, 128), f32)

    def setup_strip(t, _):
        m = [at(coefS.at[c, t]) for c in range(3)]
        c_ = [at(coefS.at[3 + c, t]) for c in range(3)]
        cy = [at(coefS.at[3 + c, t], -1) for c in range(3)]
        cx = [jnp.where(lane < 8, 0.0, pltpu.roll(v, 8, 1)) for v in c_]
        cz = [jnp.where((lane & 7) == 0, 0.0, pltpu.roll(v, 1, 1)) for v in c_]
        out = diagonals(m, c_, cy, cx, cz, pltpu.roll(m[0], 8, 1), at(coefS.at[1, t], -1), pltpu.roll(m[2], 1, 1))
        for c in range(3):
            put(diagS.at[c, t], out[c])
        put(nodeS.at[t], out[3])
        return 0

    lax.fori_loop(0, 2, setup_strip, 0)

    def setup(x, _):
        i = x + OFF
        for c in range(3):
            put(field.at[0, c, i], at(field_in.at[c, i]))
            put(diag.at[c, i], jnp.where(first_lane, pltpu.roll(at(diagS.at[c, 0]), 124 - 8 * x, 1), at(diag_in.at[c, i])))
        put(node.at[i], jnp.where(first_lane, pltpu.roll(at(nodeS.at[0]), 124 - 8 * x, 1), at(node_in.at[i])))
        return 0

    lax.fori_loop(0, 16, setup, 0)

    def fluxes(coefs, e, e0y, e0z, e1x, e1z, e2x, e2y):
        return (coefs[0] * ((e2y - e[2]) - (e1z - e[1])),
                coefs[1] * ((e0z - e[0]) - (e2x - e[2])),
                coefs[2] * ((e1x - e[1]) - (e0y - e[0])))

    def curl_back(gv, g0y, g0z, g1x, g1z, g2x, g2y):
        return ((g1z - gv[1]) - (g2y - gv[2]), (g2x - gv[2]) - (g0z - gv[0]), (g0y - gv[0]) - (g1x - gv[1]))

    def operator_step(k, _):
        now, later, before = k, k + 1, jnp.maximum(k - 1, 0)
        weight = jnp.where(k == 0, 0.0, jnp.where(k == 1, 0.5, 0.25))

        def strip_first(t, _):
            r = [at(fieldS.at[now, c, t]) for c in range(3)]
            q = ((pltpu.roll(r[0], 8, 1) - r[0]) + (at(fieldS.at[now, 1, t], -1) - r[1])) + (pltpu.roll(r[2], 1, 1) - r[2])
            put(phiS.at[t], q * at(nodeS.at[t]))
            for c in range(3):
                put(sS.at[c, t], r[c] * at(diagS.at[c, t]))
            return 0

        def strip_second(t, _):
            e = [at(sS.at[c, t]) for c in range(3)]
            out = fluxes([at(coefS.at[3 + c, t]) for c in range(3)], e,
                         at(sS.at[0, t], 1), pltpu.roll(e[0], 127, 1), pltpu.roll(e[1], 120, 1),
                         pltpu.roll(e[1], 127, 1), pltpu.roll(e[2], 120, 1), at(sS.at[2, t], 1))
            for c in range(3):
                put(gS.at[c, t], out[c])
            return 0

        def strip_third(t, _):
            gv = [at(gS.at[c, t]) for c in range(3)]
            w = curl_back(gv, at(gS.at[0, t], -1), pltpu.roll(gv[0], 1, 1), pltpu.roll(gv[1], 8, 1),
                          pltpu.roll(gv[1], 1, 1), pltpu.roll(gv[2], 8, 1), at(gS.at[2, t], -1))
            p = at(phiS.at[t])
            up = (pltpu.roll(p, 120, 1), at(phiS.at[t], 1), pltpu.roll(p, 127, 1))
            for c in range(3):
                u = at(sS.at[c, t]) + (up[c] - p)
                put(fieldS.at[later, c, t], (w[c] + at(coefS.at[c, t]) * u - at(fieldS.at[now, c, t]))
                    - weight * at(fieldS.at[before, c, t]))
            return 0

        for part in (strip_first, strip_second, strip_third):
            lax.fori_loop(0, 2, part, 0)

        def scale(n_row, _):
            x = n_row + k
            b = x + OFF
            f = [at(field.at[now, c, b]) for c in range(3)]
            q = ((at(field.at[now, 0, b - 1]) - f[0]) + (at(field.at[now, 1, b], -1) - f[1])) + (
                z_down(f[2], at(fieldS.at[now, 2, 0]), x) - f[2])
            for c in range(3):
                put(s.at[c, b], f[c] * at(diag.at[c, b]))
            put(phi.at[b], q * at(node.at[b]))
            return 0

        lax.fori_loop(0, 2, scale, 0)

        def read(x):
            i = x + OFF
            g_own = [at(g.at[c, i]) for c in range(3)]
            g_x = [at(g.at[c, i - 1]) for c in (1, 2)]
            g_y = [at(g.at[c, i], -1) for c in (0, 2)]
            p, p_x, p_y = at(phi.at[i]), at(phi.at[i + 1]), at(phi.at[i], 1)
            s_own = [at(s.at[c, i]) for c in range(3)]
            r = [at(field.at[now, c, i]) for c in range(3)]
            old = [at(field.at[before, c, i]) for c in range(3)]
            mass = [at(coef.at[c, i]) for c in range(3)]
            a = i + 2
            e = [at(s.at[c, a]) for c in range(3)]
            e_x = [at(s.at[c, a + 1]) for c in (1, 2)]
            e_y = [at(s.at[c, a], 1) for c in (0, 2)]
            curl = [at(coef.at[3 + c, a]) for c in range(3)]
            b = i + 5
            f = [at(field.at[now, c, b]) for c in range(3)]
            f_x, f_y = at(field.at[now, 0, b - 1]), at(field.at[now, 1, b], -1)
            inverse, inverse_node = [at(diag.at[c, b]) for c in range(3)], at(node.at[b])
            strip = (at(gS.at[0, 0]), at(gS.at[1, 0]), at(phiS.at[1]), at(sS.at[0, 1]), at(sS.at[1, 1]),
                     at(fieldS.at[now, 2, 0]))
            return (g_own, g_x, g_y, p, p_x, p_y, s_own, r, old, mass, e, e_x, e_y, curl, f, f_x, f_y, inverse,
                    inverse_node, strip)

        def work(x, values):
            (g_own, g_x, g_y, p, p_x, p_y, s_own, r, old, mass, e, e_x, e_y, curl, f, f_x, f_y, inverse,
             inverse_node, strip) = values
            w = curl_back(g_own, g_y[0], z_down(g_own[0], strip[0], x), g_x[0],
                          z_down(g_own[1], strip[1], x), g_x[1], g_y[1])
            up = (p_x, p_y, z_up(p, strip[2], x))
            u = [s_own[c] + (up[c] - p) for c in range(3)]
            v = [((w[c] + mass[c] * u[c]) - r[c]) - weight * old[c] for c in range(3)]
            flux = fluxes(curl, e, e_y[0], z_up(e[0], strip[3], x + 2), e_x[0],
                          z_up(e[1], strip[4], x + 2), e_x[1], e_y[1])
            q = ((f_x - f[0]) + (f_y - f[1])) + (z_down(f[2], strip[5], x + 5) - f[2])
            return r, u, v, flux, q * inverse_node, [f[c] * inverse[c] for c in range(3)]

        def write(x, results, sums):
            r, u, v, flux, potential, scaled = results
            i = x + OFF
            inside = (x >= 4) & (x < 12)
            to = jnp.where(inside, x - 4, 8)
            for c in range(3):
                put(field.at[later, c, i], v[c])
                put(g.at[c, i + 2], flux[c])
                put(s.at[c, i + 5], scaled[c])
            put(phi.at[i + 5], potential)
            sums = list(sums)
            for c in range(3):
                precond[k, c, to] = u[c]
                for n, prod in ((0, r[c] * u[c]), (1, v[c] * u[c])):
                    ends = jnp.where(below_half, prod[32:40], prod[0:8])
                    part = ((prod[8:16] + prod[16:24]) + prod[24:32]) + ends
                    sums[n] = sums[n] + jnp.where(inside, part, 0.0)
            return tuple(sums)

        def rows(n, sums):
            x = 2 * n + k - 3
            first, second = read(x), read(x + 1)
            first, second = work(x, first), work(x + 1, second)
            return write(x + 1, second, write(x, first, sums))

        zero = jnp.zeros((8, 128), f32)
        sums = lax.fori_loop(0, 9 - k, rows, (zero, zero))
        dots[2 * k] = sums[0]
        dots[2 * k + 1] = sums[1]
        return 0

    lax.fori_loop(0, 4, operator_step, 0)

    row_lane = lax.broadcasted_iota(jnp.int32, (1, 128), 1) // 16
    parts = [jnp.sum(dots[d], axis=0, keepdims=True) for d in range(8)]
    for shift in (64, 32, 16):
        parts = [t + pltpu.roll(t, shift, 1) for t in parts]
    moments = parts[0]
    for d in range(1, 8):
        moments = jnp.where(row_lane == d, parts[d], moments)
    partial[...] = jnp.broadcast_to(moments, partial.shape)

    def look(x, _):
        for c in range(3):
            sink[x, c] = s[c, x + OFF, 16:24] + g[c, x + OFF, 16:24]
        sink[x, 3] = phi[x + OFF, 16:24]
        return 0

    lax.fori_loop(0, 2, look, 0)


def finish(everyone, field, precond, solution_out, residual_out):
    total = jnp.sum(everyone[...], axis=0, keepdims=True)
    lane = lax.broadcasted_iota(jnp.int32, (1, 128), 1)
    dots = [jnp.broadcast_to(jnp.sum(jnp.where(lane // 16 == d, total, 0.0), axis=1, keepdims=True), (8, 128))
            for d in range(8)]
    size = [1.0] + [2.0 ** (1 - k) for k in range(1, 9)]
    moment = [dots[0], dots[1]]
    for k in range(1, 4):
        moment.append((dots[2 * k] * (2.0 / size[k] ** 2) - moment[0]) * size[2 * k])
        moment.append((dots[2 * k + 1] * (2.0 / (size[k] * size[k + 1])) - moment[1]) * size[2 * k + 1])
    row, earlier = moment, None
    alpha, beta = [row[1] / row[0]], [None]
    for k in range(1, 4):
        following = [None] * 8
        for l in range(k, 8 - k):
            t = row[l + 1] - alpha[k - 1] * row[l] + WEIGHT[l if l < 2 else 2] * row[l - 1]
            if k > 1:
                t = t - beta[k - 1] * earlier[l]
            following[l] = t
        alpha.append(following[k + 1] / following[k] - row[k] / row[k - 1])
        beta.append(following[k] / row[k - 1])
        row, earlier = following, row
    zero = jnp.zeros((8, 128), jnp.float32)
    older, newer = [zero] * 6, [zero + 1.0] + [zero] * 5
    value_older, value = zero, zero + 1.0
    weight = lambda l: WEIGHT[min(l, 2)]
    for k in range(4):
        nxt = []
        for l in range(6):
            t = -alpha[k] * newer[l]
            if l > 0:
                t = t + newer[l - 1]
            if l < 5:
                t = t + weight(l + 1) * newer[l + 1]
            if k > 0:
                t = t - beta[k] * older[l]
            nxt.append(t)
        step = (-1.0 - alpha[k]) * value
        if k > 0:
            step = step - beta[k] * value_older
        older, newer, value_older, value = newer, nxt, value, step
    inverse = 1.0 / value
    e = [newer[l] * inverse for l in range(5)]
    S = [None] * 4
    S[3] = -e[4]
    S[2] = -e[3] - S[3]
    S[1] = -e[2] - S[2] - weight(3) * S[3]
    S[0] = -e[1] - S[1] - weight(2) * S[2]
    e = [v[0:1] for v in e]
    S = [v[0:1] for v in S]

    def combine(x, _):
        rows, first = pl.ds(OWN, 32), pl.ds(OWN - LO, 32)
        for c in range(3):
            v = [field[k, c, x + OFF + 4, rows, :] for k in range(5)]
            u = [precond[k, c, x, first, :] for k in range(4)]
            residual_out[c, x] = (e[0] * v[0] + e[1] * v[1]) + (e[2] * v[2] + e[3] * v[3]) + e[4] * v[4]
            solution_out[c, x] = (S[0] * u[0] + S[1] * u[1]) + (S[2] * u[2] + S[3] * u[3])
        return 0

    lax.fori_loop(0, 8, combine, 0)


def shape(*dims):
    return jax.ShapeDtypeStruct(dims, jnp.float32)


def call(kernel, outs, ins, mib, scratch=(), flops=1000000):
    return pl.pallas_call(
        kernel, out_shape=outs, in_specs=[VMEM] * len(ins), out_specs=jax.tree.map(lambda _: VMEM, outs),
        scratch_shapes=list(scratch),
        compiler_params=pltpu.CompilerParams(vmem_limit_bytes=mib << 20),
        cost_estimate=pl.CostEstimate(flops=flops, bytes_accessed=1 << 20, transcendentals=0))(*ins)


def exchange(low, high, axis):
    n = lax.axis_size(axis)
    up = [(i, (i + 1) % n) for i in range(n)]
    return lax.ppermute(high, axis, up), lax.ppermute(low, axis, [(j, i) for i, j in up])


def body(right, mass, curl):
    face = (shape(3, 8, 32, 128),) + (shape(3, 4, 32, 128),) * 2
    b, *ends = call(load, face, (right,), 8)
    b = (b,) + exchange(*ends, "gx")
    c, *ends = call(load, face, (curl,), 8)
    c = (c,) + exchange(*ends, "gx")
    m, *ends = call(load_mass, face, (mass, c[0]), 8)
    m = (m,) + exchange(*ends, "gx")
    ends = (shape(9, 4, 8, 128),) * 2
    y_own = exchange(*call(pack_y_own, ends, (b[0], m[0], c[0]), 8), "gy")
    columns = (shape(9, ROWS, 128),) * 2
    extended = (shape(3, X, Y, 128), shape(6, X, Y, 128))
    own = call(pack_z_own, columns + (shape(3, 8, ROWS, 128), shape(6, 8, ROWS, 128)), (b[0], m[0], c[0]), 8, flops=20000000)
    y_halo = exchange(*call(pack_y_halo, ends, (own[0],) + b[1:] + m[1:] + c[1:], 8), "gy")
    low, high, *middle = call(pack_z_middle, columns + extended, b[1:] + m[1:] + c[1:] + tuple(own), 8, flops=20000000)
    low, high, *ends, field, coef = call(
        pack_z_edge, columns + (shape(5, ROWS, 128),) * 2 + (shape(3, 16, 16, 128), shape(6, 16, 16, 128)),
        y_own + y_halo + (low, high, *middle), 8)
    sides = (low, high) + exchange(*ends, "gz")
    block = call(invert, extended + (shape(3, X, Y, 128), shape(X, Y, 128)), (*middle, field, coef), 8, flops=20000000)

    def held(*dims):
        return pltpu.VMEM(dims + (Y, 128), jnp.float32)

    axes = ("gx", "gy", "gz")
    devices = lax.axis_size(axes)
    vectors, precond, rows, _ = call(
        main, (shape(5, 3, X, Y, 128), shape(4, 3, 9, ROWS, 128), shape(devices, 128), shape(2, 4, 8, 128)),
        tuple(block) + sides, 20,
        [held(3, X), held(X), held(3, X), held(X), held(3, X),
         held(5, 3, 2), held(6, 2), held(3, 2), held(2), held(3, 2), held(2), held(3, 2), pltpu.VMEM((8, 8, 128), jnp.float32)])
    everyone = lax.all_to_all(rows.reshape(devices, 1, 128), axes, 0, 0, tiled=True).reshape(devices, 128)
    return call(finish, (shape(3, 8, 32, 128),) * 2, (everyone, vectors, precond), 16)


def solution(mesh):
    spec = P(None, "gx", "gy", "gz")
    return jax.shard_map(body, mesh=mesh, in_specs=(spec,) * 3, out_specs=(spec,) * 2, check_vma=False)
```

```python
import jax
import jax.numpy as jnp
from jax import lax
from jax.experimental import pallas as pl
from jax.experimental.pallas import tpu as pltpu
from jax.sharding import PartitionSpec as P


X, Y = 24, 56
OFF, OWN = 4, 12
LO, ROWS = 8, 40
WEIGHT = (0.0, 0.5, 0.25, 0.25, 0.25)
VMEM = pl.BlockSpec(memory_space=pltpu.VMEM)


def load(source, own, low, high):
    def move(c, _):
        for to, x in ((low, 0), (high, 4)):
            value = source[c, x : x + 4]
            own[c, x : x + 4] = value
            to[c] = value
        return 0

    lax.fori_loop(0, 3, move, 0)


def load_mass(source, curl, own, low, high):
    load(source, own, low, high)
    high[1, 0] = source[1, 4] + curl[2, 3]
    high[2, 0] = source[2, 4] + curl[1, 3]


def pack_y(pairs, *refs):
    refs, (low, high) = refs[:-2], refs[-2:]
    n = len(refs) // 3
    sub = lax.broadcasted_iota(jnp.int32, (8, 128), 0)

    def tile(field, c, p, half, y):
        return pairs(refs[field * n : field * n + n], c, p, half, y)

    def pack(c, _):
        for field in range(3):
            for p in range(4):
                a, b = tile(field, c, p, 0, 0), tile(field, c, p, 1, 0)
                low[3 * field + c, p] = jnp.where(sub < 4, a, pltpu.roll(b, 4, 0))
                a, b = tile(field, c, p, 0, 24), tile(field, c, p, 1, 24)
                high[3 * field + c, p] = jnp.where(sub < 4, pltpu.roll(a, 4, 0), b)
        return 0

    lax.fori_loop(0, 3, pack, 0)

    def corrected(i, _):
        c, other = 2 * i, 2 - 2 * i
        for p in range(4):
            a = pltpu.roll(tile(2, other, p, 0, 24), 5, 0)
            b = pltpu.roll(tile(2, other, p, 1, 24), 1, 0)
            high[3 + c, p] = high[3 + c, p] + jnp.where(sub == 0, a, jnp.where(sub == 4, b, 0.0))
        return 0

    lax.fori_loop(0, 2, corrected, 0)


def pack_y_own(*refs):
    pack_y(lambda own, c, p, half, y: own[0][c, p + 4 * half, y : y + 8], *refs)


def pack_y_halo(after, *refs):
    pack_y(lambda ends, c, p, half, y: ends[half][c, p, y : y + 8], *refs)


def all_strips(field, coef, octets, low, high, xs=range(16), before=None):
    group = lax.broadcasted_iota(jnp.int32, (8, 128), 1) >> 2
    each, x0, start, begin, stride = octets

    def three(i, _):
        c, o = i // each, i % each
        here = pl.ds(pl.multiple_of(start + 8 * o, 8), 8)
        to = pl.ds(pl.multiple_of(begin + stride * o, 8), 8)
        done = []
        for source, comp, dest in ((field, c, c), (coef, c, 3 + c), (coef, 3 + c, 6 + c)):
            first, last = (jnp.zeros((8, 128), jnp.float32),) * 2
            if before:
                first, last = before[0][dest, to, :], before[1][dest, to, :]
            for x in xs:
                t = source[comp, x0 + x, here, :]
                first = jnp.where(group == 2 * x + 1, pltpu.roll(t, 8 * x + 4, 1), first)
                last = jnp.where(group == 2 * x, pltpu.roll(t, (8 * x + 4) % 128, 1), last)
            done.append((dest, first, last))
        for dest, first, last in done:
            low[dest, to, :] = first
            high[dest, to, :] = last
        return 0

    lax.fori_loop(0, 3 * each, three, 0)
    lane = lax.broadcasted_iota(jnp.int32, (8, 128), 1)

    def corrected(i, _):
        which, o = i // each, i % each
        here = pl.ds(pl.multiple_of(start + 8 * o, 8), 8)
        to = pl.ds(pl.multiple_of(begin + stride * o, 8), 8)
        last = jnp.zeros((8, 128), jnp.float32)
        for x in xs:
            t = coef[4 - which, x0 + x, here, :]
            last = jnp.where(lane == 8 * x, pltpu.roll(t, (8 * x + 5) % 128, 1), last)
        high[3 + which, to, :] = high[3 + which, to, :] + last
        return 0

    lax.fori_loop(0, 2 * each, corrected, 0)


def pack_z_own(right, mass, curl, low, high, field, coef):
    def assemble(c, _):
        for to, source in ((field.at[c], right), (coef.at[c], mass), (coef.at[3 + c], curl)):
            to[:, 4:36] = source[c]
        return 0

    lax.fori_loop(0, 3, assemble, 0)
    all_strips(field, coef, (3, -4, 8, 8, 8), low, high, range(4, 12))


def pack_z_middle(*refs):
    blocks = refs[0:2], refs[2:4], refs[4:6]
    own_low, own_high, own_field, own_coef, low, high, field, coef = refs[6:]

    def assemble(c, _):
        for n, (below, above) in enumerate(blocks):
            to = field.at[c] if n == 0 else coef.at[3 * n - 3 + c]
            own = own_field.at[c] if n == 0 else own_coef.at[3 * n - 3 + c]
            to[OFF : OFF + 4, OWN : OWN + 32] = below[c]
            to[OFF + 4 : OFF + 12, LO : LO + ROWS] = own[...]
            to[OFF + 12 : OFF + 16, OWN : OWN + 32] = above[c]
        return 0

    lax.fori_loop(0, 3, assemble, 0)
    ends = (0, 1, 2, 3, 12, 13, 14, 15)
    all_strips(field, coef, (3, OFF, 16, 8, 8), low, high, ends, (own_low, own_high))


def pack_z_edge(own_low, own_high, halo_low, halo_high, middle_low, middle_high, middle_field, middle_coef,
                low, high, send_low, send_high, field, coef):
    sub = lax.broadcasted_iota(jnp.int32, (8, 128), 0)

    def assemble(c, _):
        for n in range(3):
            to = field.at[c] if n == 0 else coef.at[3 * n - 3 + c]
            source = middle_field.at[c] if n == 0 else middle_coef.at[3 * n - 3 + c]
            comp = 3 * n + c
            for p in range(4):
                for lows, highs, x0, x1 in ((halo_low, halo_high, p, p + 12), (own_low, own_high, p + 4, p + 8)):
                    lower, upper = lows[comp, p], highs[comp, p]
                    to[x0, 0:8] = jnp.where(sub < 4, lower, source[OFF + x0, 8:16])
                    to[x1, 0:8] = jnp.where(sub < 4, pltpu.roll(lower, 4, 0), source[OFF + x1, 8:16])
                    to[x0, 8:16] = jnp.where(sub < 4, source[OFF + x0, 40:48], pltpu.roll(upper, 4, 0))
                    to[x1, 8:16] = jnp.where(sub < 4, source[OFF + x1, 40:48], upper)
        return 0

    lax.fori_loop(0, 3, assemble, 0)
    all_strips(field, coef, (2, 0, 0, 0, 32), low, high)
    for comp in range(9):
        low[comp, 8:32] = middle_low[comp, 8:32]
        high[comp, 8:32] = middle_high[comp, 8:32]
    for n in range(5):
        down, up = low[n], high[n]
        if n < 4:
            down, up = down + pltpu.roll(low[n + 5], 124, 1), up + pltpu.roll(high[n + 5], 4, 1)
        send_low[n] = down
        send_high[n] = up


def at(ref, dy=0):
    return ref[pl.ds(LO + dy, ROWS), :]


def put(ref, value):
    ref[pl.ds(LO, ROWS), :] = value


def diagonals(m, c, cy, cx, cz, mx, my, mz):
    d0 = m[0] + c[1] + cz[1] + c[2] + cy[2]
    d1 = m[1] + c[2] + cx[2] + c[0] + cz[0]
    d2 = m[2] + c[0] + cy[0] + c[1] + cx[1]
    dn = m[0] + mx + m[1] + my + m[2] + mz
    return 1.0 / d0, 1.0 / d1, 1.0 / d2, 1.0 / dn


def invert(field_middle, coef_middle, field_edge, coef_edge, field, coef, diag, node):
    def assemble(c, _):
        coef[c, OFF - 1] = jnp.zeros((Y, 128), jnp.float32)
        for x in range(OFF, OFF + 16):
            coef[c, x, 0:8] = jnp.zeros((8, 128), jnp.float32)
            coef[c, x, 16:40] = coef_middle[c, x, 16:40]
            coef[c, x, 8:16] = coef_edge[c, x - OFF, 0:8]
            coef[c, x, 40:48] = coef_edge[c, x - OFF, 8:16]
        return 0

    def assemble_field(c, _):
        for x in range(OFF, OFF + 16):
            field[c, x, 16:40] = field_middle[c, x, 16:40]
            field[c, x, 8:16] = field_edge[c, x - OFF, 0:8]
            field[c, x, 40:48] = field_edge[c, x - OFF, 8:16]
        return 0

    lax.fori_loop(0, 6, assemble, 0)
    lax.fori_loop(0, 3, assemble_field, 0)

    def row(x, _):
        i = x + OFF
        m = [at(coef.at[c, i]) for c in range(3)]
        c_ = [at(coef.at[3 + c, i]) for c in range(3)]
        cy = [at(coef.at[3 + c, i], -1) for c in range(3)]
        cx = [at(coef.at[3 + c, i - 1]) for c in range(3)]
        cz = [pltpu.roll(c_[c], 1, 1) for c in range(2)]
        out = diagonals(m, c_, cy, cx, cz, at(coef.at[0, i - 1]), at(coef.at[1, i], -1), pltpu.roll(m[2], 1, 1))
        for c in range(3):
            put(diag.at[c, i], out[c])
        put(node.at[i], out[3])
        return 0

    lax.fori_loop(0, 16, row, 0)


def main(field_in, coef, diag_in, node_in, zown_low, zown_high, zlow, zhigh, field, precond, partial, sink,
         diag, node, s, phi, g, fieldS, coefS, diagS, nodeS, sS, phiS, gS, dots):
    f32 = jnp.float32
    lane = lax.broadcasted_iota(jnp.int32, (ROWS, 128), 1)
    first_lane, last_lane = lane == 0, lane == 127
    below_half = lax.broadcasted_iota(jnp.int32, (8, 128), 0) < 4

    def z_up(value, strip, x):
        return jnp.where(last_lane, pltpu.roll(strip, (123 - 8 * x) & 127, 1), pltpu.roll(value, 127, 1))

    def z_down(value, strip, x):
        return jnp.where(first_lane, pltpu.roll(strip, (125 - 8 * x) & 127, 1), pltpu.roll(value, 1, 1))

    upper = (lane & 4) != 0
    for comp in range(9):
        lower_part, upper_part = zlow[comp % 5], zhigh[comp % 5]
        if comp >= 5:
            lower_part, upper_part = pltpu.roll(lower_part, 124, 1), pltpu.roll(upper_part, 4, 1)
        for t, value in ((0, jnp.where(upper, zown_low[comp], lower_part)),
                         (1, jnp.where(upper, upper_part, zown_high[comp]))):
            put(fieldS.at[0, comp, t] if comp < 3 else coefS.at[comp - 3, t], value)
            if comp >= 3:
                coefS[comp - 3, t, 0:8] = jnp.zeros((8, 128), f32)

    def setup_strip(t, _):
        m = [at(coefS.at[c, t]) for c in range(3)]
        c_ = [at(coefS.at[3 + c, t]) for c in range(3)]
        cy = [at(coefS.at[3 + c, t], -1) for c in range(3)]
        cx = [jnp.where(lane < 8, 0.0, pltpu.roll(v, 8, 1)) for v in c_]
        cz = [jnp.where((lane & 7) == 0, 0.0, pltpu.roll(v, 1, 1)) for v in c_]
        out = diagonals(m, c_, cy, cx, cz, pltpu.roll(m[0], 8, 1), at(coefS.at[1, t], -1), pltpu.roll(m[2], 1, 1))
        for c in range(3):
            put(diagS.at[c, t], out[c])
        put(nodeS.at[t], out[3])
        return 0

    lax.fori_loop(0, 2, setup_strip, 0)

    def setup(n, _):
        ready = []
        for x in (2 * n, 2 * n + 1):
            i = x + OFF
            ready.append((i, [at(field_in.at[c, i]) for c in range(3)], [
                jnp.where(first_lane, pltpu.roll(at(diagS.at[c, 0]), 124 - 8 * x, 1), at(diag_in.at[c, i]))
                for c in range(3)], jnp.where(first_lane, pltpu.roll(at(nodeS.at[0]), 124 - 8 * x, 1), at(node_in.at[i]))))
        for i, fields, diags, nodes in ready:
            for c in range(3):
                put(field.at[0, c, i], fields[c])
                put(diag.at[c, i], diags[c])
            put(node.at[i], nodes)
        return 0

    lax.fori_loop(0, 8, setup, 0)

    def fluxes(coefs, e, e0y, e0z, e1x, e1z, e2x, e2y):
        return (coefs[0] * ((e2y - e[2]) - (e1z - e[1])),
                coefs[1] * ((e0z - e[0]) - (e2x - e[2])),
                coefs[2] * ((e1x - e[1]) - (e0y - e[0])))

    def curl_back(gv, g0y, g0z, g1x, g1z, g2x, g2y):
        return ((g1z - gv[1]) - (g2y - gv[2]), (g2x - gv[2]) - (g0z - gv[0]), (g0y - gv[0]) - (g1x - gv[1]))

    def operator_step(k, _):
        now, later, before = k, k + 1, jnp.maximum(k - 1, 0)
        weight = jnp.where(k == 0, 0.0, jnp.where(k == 1, 0.5, 0.25))

        def strip_first(t, _):
            r = [at(fieldS.at[now, c, t]) for c in range(3)]
            q = ((pltpu.roll(r[0], 8, 1) - r[0]) + (at(fieldS.at[now, 1, t], -1) - r[1])) + (pltpu.roll(r[2], 1, 1) - r[2])
            put(phiS.at[t], q * at(nodeS.at[t]))
            for c in range(3):
                put(sS.at[c, t], r[c] * at(diagS.at[c, t]))
            return 0

        def strip_second(t, _):
            e = [at(sS.at[c, t]) for c in range(3)]
            out = fluxes([at(coefS.at[3 + c, t]) for c in range(3)], e,
                         at(sS.at[0, t], 1), pltpu.roll(e[0], 127, 1), pltpu.roll(e[1], 120, 1),
                         pltpu.roll(e[1], 127, 1), pltpu.roll(e[2], 120, 1), at(sS.at[2, t], 1))
            for c in range(3):
                put(gS.at[c, t], out[c])
            return 0

        def strip_third(t, _):
            gv = [at(gS.at[c, t]) for c in range(3)]
            w = curl_back(gv, at(gS.at[0, t], -1), pltpu.roll(gv[0], 1, 1), pltpu.roll(gv[1], 8, 1),
                          pltpu.roll(gv[1], 1, 1), pltpu.roll(gv[2], 8, 1), at(gS.at[2, t], -1))
            p = at(phiS.at[t])
            up = (pltpu.roll(p, 120, 1), at(phiS.at[t], 1), pltpu.roll(p, 127, 1))
            for c in range(3):
                u = at(sS.at[c, t]) + (up[c] - p)
                put(fieldS.at[later, c, t], (w[c] + at(coefS.at[c, t]) * u - at(fieldS.at[now, c, t]))
                    - weight * at(fieldS.at[before, c, t]))
            return 0

        for part in (strip_first, strip_second, strip_third):
            for t in range(2):
                part(t, 0)

        def scale(n_row, _):
            x = n_row + k
            b = x + OFF
            f = [at(field.at[now, c, b]) for c in range(3)]
            q = ((at(field.at[now, 0, b - 1]) - f[0]) + (at(field.at[now, 1, b], -1) - f[1])) + (
                z_down(f[2], at(fieldS.at[now, 2, 0]), x) - f[2])
            for c in range(3):
                put(s.at[c, b], f[c] * at(diag.at[c, b]))
            put(phi.at[b], q * at(node.at[b]))
            return 0

        lax.fori_loop(0, 2, scale, 0)

        def read(x):
            i = x + OFF
            g_own = [at(g.at[c, i]) for c in range(3)]
            g_x = [at(g.at[c, i - 1]) for c in (1, 2)]
            g_y = [at(g.at[c, i], -1) for c in (0, 2)]
            p, p_x, p_y = at(phi.at[i]), at(phi.at[i + 1]), at(phi.at[i], 1)
            s_own = [at(s.at[c, i]) for c in range(3)]
            r = [at(field.at[now, c, i]) for c in range(3)]
            old = [at(field.at[before, c, i]) for c in range(3)]
            mass = [at(coef.at[c, i]) for c in range(3)]
            a = i + 2
            e = [at(s.at[c, a]) for c in range(3)]
            e_x = [at(s.at[c, a + 1]) for c in (1, 2)]
            e_y = [at(s.at[c, a], 1) for c in (0, 2)]
            curl = [at(coef.at[3 + c, a]) for c in range(3)]
            b = i + 5
            f = [at(field.at[now, c, b]) for c in range(3)]
            f_x, f_y = at(field.at[now, 0, b - 1]), at(field.at[now, 1, b], -1)
            inverse, inverse_node = [at(diag.at[c, b]) for c in range(3)], at(node.at[b])
            strip = (at(gS.at[0, 0]), at(gS.at[1, 0]), at(phiS.at[1]), at(sS.at[0, 1]), at(sS.at[1, 1]),
                     at(fieldS.at[now, 2, 0]))
            return (g_own, g_x, g_y, p, p_x, p_y, s_own, r, old, mass, e, e_x, e_y, curl, f, f_x, f_y, inverse,
                    inverse_node, strip)

        def work(x, values):
            (g_own, g_x, g_y, p, p_x, p_y, s_own, r, old, mass, e, e_x, e_y, curl, f, f_x, f_y, inverse,
             inverse_node, strip) = values
            w = curl_back(g_own, g_y[0], z_down(g_own[0], strip[0], x), g_x[0],
                          z_down(g_own[1], strip[1], x), g_x[1], g_y[1])
            up = (p_x, p_y, z_up(p, strip[2], x))
            u = [s_own[c] + (up[c] - p) for c in range(3)]
            v = [((w[c] + mass[c] * u[c]) - r[c]) - weight * old[c] for c in range(3)]
            flux = fluxes(curl, e, e_y[0], z_up(e[0], strip[3], x + 2), e_x[0],
                          z_up(e[1], strip[4], x + 2), e_x[1], e_y[1])
            q = ((f_x - f[0]) + (f_y - f[1])) + (z_down(f[2], strip[5], x + 5) - f[2])
            return r, u, v, flux, q * inverse_node, [f[c] * inverse[c] for c in range(3)]

        def write(x, results, sums):
            r, u, v, flux, potential, scaled = results
            i = x + OFF
            inside = (x >= 4) & (x < 12)
            to = jnp.where(inside, x - 4, 8)
            for c in range(3):
                put(field.at[later, c, i], v[c])
                put(g.at[c, i + 2], flux[c])
                put(s.at[c, i + 5], scaled[c])
            put(phi.at[i + 5], potential)
            sums = list(sums)
            for c in range(3):
                precond[k, c, to] = u[c]
                for n, prod in ((0, r[c] * u[c]), (1, v[c] * u[c])):
                    ends = jnp.where(below_half, prod[32:40], prod[0:8])
                    part = ((prod[8:16] + prod[16:24]) + prod[24:32]) + ends
                    sums[n] = sums[n] + jnp.where(inside, part, 0.0)
            return tuple(sums)

        def rows(n, sums):
            x = 2 * n + k - 3
            first, second = read(x), read(x + 1)
            first, second = work(x, first), work(x + 1, second)
            return write(x + 1, second, write(x, first, sums))

        zero = jnp.zeros((8, 128), f32)
        sums = lax.fori_loop(0, 9 - k, rows, (zero, zero))
        dots[2 * k] = sums[0]
        dots[2 * k + 1] = sums[1]
        return 0

    lax.fori_loop(0, 4, operator_step, 0)

    row_lane = lax.broadcasted_iota(jnp.int32, (1, 128), 1) // 16
    parts = [jnp.sum(dots[d], axis=0, keepdims=True) for d in range(8)]
    for shift in (64, 32, 16):
        parts = [t + pltpu.roll(t, shift, 1) for t in parts]
    moments = parts[0]
    for d in range(1, 8):
        moments = jnp.where(row_lane == d, parts[d], moments)
    partial[...] = jnp.broadcast_to(moments, partial.shape)

    def look(x, _):
        for c in range(3):
            sink[x, c] = s[c, x + OFF, 16:24] + g[c, x + OFF, 16:24]
        sink[x, 3] = phi[x + OFF, 16:24]
        return 0

    lax.fori_loop(0, 2, look, 0)


def finish(everyone, field, precond, solution_out, residual_out):
    total = jnp.sum(everyone[...], axis=0, keepdims=True)
    lane = lax.broadcasted_iota(jnp.int32, (1, 128), 1)
    dots = [jnp.broadcast_to(jnp.sum(jnp.where(lane // 16 == d, total, 0.0), axis=1, keepdims=True), (8, 128))
            for d in range(8)]
    size = [1.0] + [2.0 ** (1 - k) for k in range(1, 9)]
    moment = [dots[0], dots[1]]
    for k in range(1, 4):
        moment.append((dots[2 * k] * (2.0 / size[k] ** 2) - moment[0]) * size[2 * k])
        moment.append((dots[2 * k + 1] * (2.0 / (size[k] * size[k + 1])) - moment[1]) * size[2 * k + 1])
    row, earlier = moment, None
    alpha, beta = [row[1] / row[0]], [None]
    for k in range(1, 4):
        following = [None] * 8
        for l in range(k, 8 - k):
            t = row[l + 1] - alpha[k - 1] * row[l] + WEIGHT[l if l < 2 else 2] * row[l - 1]
            if k > 1:
                t = t - beta[k - 1] * earlier[l]
            following[l] = t
        alpha.append(following[k + 1] / following[k] - row[k] / row[k - 1])
        beta.append(following[k] / row[k - 1])
        row, earlier = following, row
    zero = jnp.zeros((8, 128), jnp.float32)
    older, newer = [zero] * 6, [zero + 1.0] + [zero] * 5
    value_older, value = zero, zero + 1.0
    weight = lambda l: WEIGHT[min(l, 2)]
    for k in range(4):
        nxt = []
        for l in range(6):
            t = -alpha[k] * newer[l]
            if l > 0:
                t = t + newer[l - 1]
            if l < 5:
                t = t + weight(l + 1) * newer[l + 1]
            if k > 0:
                t = t - beta[k] * older[l]
            nxt.append(t)
        step = (-1.0 - alpha[k]) * value
        if k > 0:
            step = step - beta[k] * value_older
        older, newer, value_older, value = newer, nxt, value, step
    inverse = 1.0 / value
    e = [newer[l] * inverse for l in range(5)]
    S = [None] * 4
    S[3] = -e[4]
    S[2] = -e[3] - S[3]
    S[1] = -e[2] - S[2] - weight(3) * S[3]
    S[0] = -e[1] - S[1] - weight(2) * S[2]
    e = [v[0:1] for v in e]
    S = [v[0:1] for v in S]

    def combine(x, _):
        rows, first = pl.ds(OWN, 32), pl.ds(OWN - LO, 32)
        for c in range(3):
            v = [field[k, c, x + OFF + 4, rows, :] for k in range(5)]
            u = [precond[k, c, x, first, :] for k in range(4)]
            residual_out[c, x] = (e[0] * v[0] + e[1] * v[1]) + (e[2] * v[2] + e[3] * v[3]) + e[4] * v[4]
            solution_out[c, x] = (S[0] * u[0] + S[1] * u[1]) + (S[2] * u[2] + S[3] * u[3])
        return 0

    lax.fori_loop(0, 8, combine, 0)


def shape(*dims):
    return jax.ShapeDtypeStruct(dims, jnp.float32)


def call(kernel, outs, ins, mib, scratch=(), flops=1000000):
    return pl.pallas_call(
        kernel, out_shape=outs, in_specs=[VMEM] * len(ins), out_specs=jax.tree.map(lambda _: VMEM, outs),
        scratch_shapes=list(scratch),
        compiler_params=pltpu.CompilerParams(vmem_limit_bytes=mib << 20),
        cost_estimate=pl.CostEstimate(flops=flops, bytes_accessed=1 << 20, transcendentals=0))(*ins)


def exchange(low, high, axis):
    n = lax.axis_size(axis)
    up = [(i, (i + 1) % n) for i in range(n)]
    return lax.ppermute(high, axis, up), lax.ppermute(low, axis, [(j, i) for i, j in up])


def body(right, mass, curl):
    face = (shape(3, 8, 32, 128),) + (shape(3, 4, 32, 128),) * 2
    b, *ends = call(load, face, (right,), 8)
    b = (b,) + exchange(*ends, "gx")
    c, *ends = call(load, face, (curl,), 8)
    c = (c,) + exchange(*ends, "gx")
    m, *ends = call(load_mass, face, (mass, c[0]), 8)
    m = (m,) + exchange(*ends, "gx")
    ends = (shape(9, 4, 8, 128),) * 2
    y_own = exchange(*call(pack_y_own, ends, (b[0], m[0], c[0]), 8), "gy")
    columns = (shape(9, ROWS, 128),) * 2
    extended = (shape(3, X, Y, 128), shape(6, X, Y, 128))
    own = call(pack_z_own, columns + (shape(3, 8, ROWS, 128), shape(6, 8, ROWS, 128)), (b[0], m[0], c[0]), 8, flops=20000000)
    y_halo = exchange(*call(pack_y_halo, ends, (own[0],) + b[1:] + m[1:] + c[1:], 8), "gy")
    low, high, *middle = call(pack_z_middle, columns + extended, b[1:] + m[1:] + c[1:] + tuple(own), 8, flops=20000000)
    low, high, *ends, field, coef = call(
        pack_z_edge, columns + (shape(5, ROWS, 128),) * 2 + (shape(3, 16, 16, 128), shape(6, 16, 16, 128)),
        y_own + y_halo + (low, high, *middle), 8)
    sides = (low, high) + exchange(*ends, "gz")
    block = call(invert, extended + (shape(3, X, Y, 128), shape(X, Y, 128)), (*middle, field, coef), 8, flops=20000000)

    def held(*dims):
        return pltpu.VMEM(dims + (Y, 128), jnp.float32)

    axes = ("gx", "gy", "gz")
    devices = lax.axis_size(axes)
    vectors, precond, rows, _ = call(
        main, (shape(5, 3, X, Y, 128), shape(4, 3, 9, ROWS, 128), shape(devices, 128), shape(2, 4, 8, 128)),
        tuple(block) + sides, 20,
        [held(3, X), held(X), held(3, X), held(X), held(3, X),
         held(5, 3, 2), held(6, 2), held(3, 2), held(2), held(3, 2), held(2), held(3, 2), pltpu.VMEM((8, 8, 128), jnp.float32)])
    everyone = lax.all_to_all(rows.reshape(devices, 1, 128), axes, 0, 0, tiled=True).reshape(devices, 128)
    return call(finish, (shape(3, 8, 32, 128),) * 2, (everyone, vectors, precond), 16)


def solution(mesh):
    spec = P(None, "gx", "gy", "gz")
    return jax.shard_map(body, mesh=mesh, in_specs=(spec,) * 3, out_specs=(spec,) * 2, check_vma=False)
```

```python
import jax
import jax.numpy as jnp
from jax import lax
from jax.experimental import pallas as pl
from jax.experimental.pallas import tpu as pltpu
from jax.sharding import PartitionSpec as P


X, Y = 24, 56
OFF, OWN = 4, 12
LO, ROWS = 8, 40
WEIGHT = (0.0, 0.5, 0.25, 0.25, 0.25)
VMEM = pl.BlockSpec(memory_space=pltpu.VMEM)


def load(source, own, low, high):
    def move(c, _):
        for to, x in ((low, 0), (high, 4)):
            value = source[c, x : x + 4]
            own[c, x : x + 4] = value
            to[c] = value
        return 0

    lax.fori_loop(0, 3, move, 0)


def load_mass(source, curl, own, low, high):
    load(source, own, low, high)
    high[1, 0] = source[1, 4] + curl[2, 3]
    high[2, 0] = source[2, 4] + curl[1, 3]


def pack_y(pairs, *refs):
    refs, (low, high) = refs[:-2], refs[-2:]
    n = len(refs) // 3
    sub = lax.broadcasted_iota(jnp.int32, (8, 128), 0)

    def tile(field, c, p, half, y):
        return pairs(refs[field * n : field * n + n], c, p, half, y)

    def pack(c, _):
        for field in range(3):
            for p in range(4):
                a, b = tile(field, c, p, 0, 0), tile(field, c, p, 1, 0)
                low[3 * field + c, p] = jnp.where(sub < 4, a, pltpu.roll(b, 4, 0))
                a, b = tile(field, c, p, 0, 24), tile(field, c, p, 1, 24)
                high[3 * field + c, p] = jnp.where(sub < 4, pltpu.roll(a, 4, 0), b)
        return 0

    lax.fori_loop(0, 3, pack, 0)

    def corrected(i, _):
        c, other = 2 * i, 2 - 2 * i
        for p in range(4):
            a = pltpu.roll(tile(2, other, p, 0, 24), 5, 0)
            b = pltpu.roll(tile(2, other, p, 1, 24), 1, 0)
            high[3 + c, p] = high[3 + c, p] + jnp.where(sub == 0, a, jnp.where(sub == 4, b, 0.0))
        return 0

    lax.fori_loop(0, 2, corrected, 0)


def pack_y_own(*refs):
    pack_y(lambda own, c, p, half, y: own[0][c, p + 4 * half, y : y + 8], *refs)


def pack_y_halo(after, *refs):
    pack_y(lambda ends, c, p, half, y: ends[half][c, p, y : y + 8], *refs)


def all_strips(field, coef, octets, low, high, xs=range(16), before=None):
    group = lax.broadcasted_iota(jnp.int32, (8, 128), 1) >> 2
    each, x0, start, begin, stride = octets

    def three(i, _):
        c, o = i // each, i % each
        here = pl.ds(pl.multiple_of(start + 8 * o, 8), 8)
        to = pl.ds(pl.multiple_of(begin + stride * o, 8), 8)
        done = []
        for source, comp, dest in ((field, c, c), (coef, c, 3 + c), (coef, 3 + c, 6 + c)):
            first, last = (jnp.zeros((8, 128), jnp.float32),) * 2
            if before:
                first, last = before[0][dest, to, :], before[1][dest, to, :]
            for x in xs:
                t = source[comp, x0 + x, here, :]
                first = jnp.where(group == 2 * x + 1, pltpu.roll(t, 8 * x + 4, 1), first)
                last = jnp.where(group == 2 * x, pltpu.roll(t, (8 * x + 4) % 128, 1), last)
            done.append((dest, first, last))
        for dest, first, last in done:
            low[dest, to, :] = first
            high[dest, to, :] = last
        return 0

    lax.fori_loop(0, 3 * each, three, 0)
    lane = lax.broadcasted_iota(jnp.int32, (8, 128), 1)

    def corrected(o, _):
        here = pl.ds(pl.multiple_of(start + 8 * o, 8), 8)
        to = pl.ds(pl.multiple_of(begin + stride * o, 8), 8)
        lasts = []
        for which in range(2):
            last = jnp.zeros((8, 128), jnp.float32)
            for x in xs:
                t = coef[4 - which, x0 + x, here, :]
                last = jnp.where(lane == 8 * x, pltpu.roll(t, (8 * x + 5) % 128, 1), last)
            lasts.append(high[3 + which, to, :] + last)
        for which in range(2):
            high[3 + which, to, :] = lasts[which]
        return 0

    lax.fori_loop(0, each, corrected, 0)


def pack_z_own(right, mass, curl, low, high, field, coef):
    def assemble(c, _):
        for to, source in ((field.at[c], right), (coef.at[c], mass), (coef.at[3 + c], curl)):
            to[:, 4:36] = source[c]
        return 0

    lax.fori_loop(0, 3, assemble, 0)
    all_strips(field, coef, (3, -4, 8, 8, 8), low, high, range(4, 12))


def pack_z_middle(*refs):
    blocks = refs[0:2], refs[2:4], refs[4:6]
    own_low, own_high, own_field, own_coef, low, high, field, coef = refs[6:]

    def assemble(c, _):
        for n, (below, above) in enumerate(blocks):
            to = field.at[c] if n == 0 else coef.at[3 * n - 3 + c]
            own = own_field.at[c] if n == 0 else own_coef.at[3 * n - 3 + c]
            to[OFF : OFF + 4, OWN : OWN + 32] = below[c]
            to[OFF + 4 : OFF + 12, LO : LO + ROWS] = own[...]
            to[OFF + 12 : OFF + 16, OWN : OWN + 32] = above[c]
        return 0

    lax.fori_loop(0, 3, assemble, 0)
    ends = (0, 1, 2, 3, 12, 13, 14, 15)
    all_strips(field, coef, (3, OFF, 16, 8, 8), low, high, ends, (own_low, own_high))


def pack_z_edge(own_low, own_high, halo_low, halo_high, middle_low, middle_high, middle_field, middle_coef,
                low, high, send_low, send_high, field, coef):
    sub = lax.broadcasted_iota(jnp.int32, (8, 128), 0)

    def assemble(c, _):
        for n in range(3):
            to = field.at[c] if n == 0 else coef.at[3 * n - 3 + c]
            source = middle_field.at[c] if n == 0 else middle_coef.at[3 * n - 3 + c]
            comp = 3 * n + c
            for p in range(4):
                for lows, highs, x0, x1 in ((halo_low, halo_high, p, p + 12), (own_low, own_high, p + 4, p + 8)):
                    lower, upper = lows[comp, p], highs[comp, p]
                    to[x0, 0:8] = jnp.where(sub < 4, lower, source[OFF + x0, 8:16])
                    to[x1, 0:8] = jnp.where(sub < 4, pltpu.roll(lower, 4, 0), source[OFF + x1, 8:16])
                    to[x0, 8:16] = jnp.where(sub < 4, source[OFF + x0, 40:48], pltpu.roll(upper, 4, 0))
                    to[x1, 8:16] = jnp.where(sub < 4, source[OFF + x1, 40:48], upper)
        return 0

    lax.fori_loop(0, 3, assemble, 0)
    all_strips(field, coef, (2, 0, 0, 0, 32), low, high)
    for comp in range(9):
        low[comp, 8:32] = middle_low[comp, 8:32]
        high[comp, 8:32] = middle_high[comp, 8:32]
    for n in range(5):
        down, up = low[n], high[n]
        if n < 4:
            down, up = down + pltpu.roll(low[n + 5], 124, 1), up + pltpu.roll(high[n + 5], 4, 1)
        send_low[n] = down
        send_high[n] = up


def at(ref, dy=0):
    return ref[pl.ds(LO + dy, ROWS), :]


def put(ref, value):
    ref[pl.ds(LO, ROWS), :] = value


def diagonals(m, c, cy, cx, cz, mx, my, mz):
    d0 = m[0] + c[1] + cz[1] + c[2] + cy[2]
    d1 = m[1] + c[2] + cx[2] + c[0] + cz[0]
    d2 = m[2] + c[0] + cy[0] + c[1] + cx[1]
    dn = m[0] + mx + m[1] + my + m[2] + mz
    return 1.0 / d0, 1.0 / d1, 1.0 / d2, 1.0 / dn


def invert(field_middle, coef_middle, field_edge, coef_edge, field, coef, diag, node):
    def assemble(c, _):
        coef[c, OFF - 1] = jnp.zeros((Y, 128), jnp.float32)
        for x in range(OFF, OFF + 16):
            coef[c, x, 0:8] = jnp.zeros((8, 128), jnp.float32)
            coef[c, x, 16:40] = coef_middle[c, x, 16:40]
            coef[c, x, 8:16] = coef_edge[c, x - OFF, 0:8]
            coef[c, x, 40:48] = coef_edge[c, x - OFF, 8:16]
        return 0

    def assemble_field(c, _):
        for x in range(OFF, OFF + 16):
            field[c, x, 16:40] = field_middle[c, x, 16:40]
            field[c, x, 8:16] = field_edge[c, x - OFF, 0:8]
            field[c, x, 40:48] = field_edge[c, x - OFF, 8:16]
        return 0

    lax.fori_loop(0, 6, assemble, 0)
    lax.fori_loop(0, 3, assemble_field, 0)

    def row(x, _):
        i = x + OFF
        m = [at(coef.at[c, i]) for c in range(3)]
        c_ = [at(coef.at[3 + c, i]) for c in range(3)]
        cy = [at(coef.at[3 + c, i], -1) for c in range(3)]
        cx = [at(coef.at[3 + c, i - 1]) for c in range(3)]
        cz = [pltpu.roll(c_[c], 1, 1) for c in range(2)]
        out = diagonals(m, c_, cy, cx, cz, at(coef.at[0, i - 1]), at(coef.at[1, i], -1), pltpu.roll(m[2], 1, 1))
        for c in range(3):
            put(diag.at[c, i], out[c])
        put(node.at[i], out[3])
        return 0

    lax.fori_loop(0, 16, row, 0)


def main(field_in, coef, diag_in, node_in, zown_low, zown_high, zlow, zhigh, field, precond, partial, sink,
         diag, node, s, phi, g, fieldS, coefS, diagS, nodeS, sS, phiS, gS, dots):
    f32 = jnp.float32
    lane = lax.broadcasted_iota(jnp.int32, (ROWS, 128), 1)
    first_lane, last_lane = lane == 0, lane == 127
    below_half = lax.broadcasted_iota(jnp.int32, (8, 128), 0) < 4

    def z_up(value, strip, x):
        return jnp.where(last_lane, pltpu.roll(strip, (123 - 8 * x) & 127, 1), pltpu.roll(value, 127, 1))

    def z_down(value, strip, x):
        return jnp.where(first_lane, pltpu.roll(strip, (125 - 8 * x) & 127, 1), pltpu.roll(value, 1, 1))

    upper = (lane & 4) != 0
    for comp in range(9):
        lower_part, upper_part = zlow[comp % 5], zhigh[comp % 5]
        if comp >= 5:
            lower_part, upper_part = pltpu.roll(lower_part, 124, 1), pltpu.roll(upper_part, 4, 1)
        for t, value in ((0, jnp.where(upper, zown_low[comp], lower_part)),
                         (1, jnp.where(upper, upper_part, zown_high[comp]))):
            put(fieldS.at[0, comp, t] if comp < 3 else coefS.at[comp - 3, t], value)
            if comp >= 3:
                coefS[comp - 3, t, 0:8] = jnp.zeros((8, 128), f32)

    def setup_strip(t, _):
        m = [at(coefS.at[c, t]) for c in range(3)]
        c_ = [at(coefS.at[3 + c, t]) for c in range(3)]
        cy = [at(coefS.at[3 + c, t], -1) for c in range(3)]
        cx = [jnp.where(lane < 8, 0.0, pltpu.roll(v, 8, 1)) for v in c_]
        cz = [jnp.where((lane & 7) == 0, 0.0, pltpu.roll(v, 1, 1)) for v in c_]
        out = diagonals(m, c_, cy, cx, cz, pltpu.roll(m[0], 8, 1), at(coefS.at[1, t], -1), pltpu.roll(m[2], 1, 1))
        for c in range(3):
            put(diagS.at[c, t], out[c])
        put(nodeS.at[t], out[3])
        return 0

    lax.fori_loop(0, 2, setup_strip, 0)

    def setup(n, _):
        ready = []
        for x in (2 * n, 2 * n + 1):
            i = x + OFF
            ready.append((i, [at(field_in.at[c, i]) for c in range(3)], [
                jnp.where(first_lane, pltpu.roll(at(diagS.at[c, 0]), 124 - 8 * x, 1), at(diag_in.at[c, i]))
                for c in range(3)], jnp.where(first_lane, pltpu.roll(at(nodeS.at[0]), 124 - 8 * x, 1), at(node_in.at[i]))))
        for i, fields, diags, nodes in ready:
            for c in range(3):
                put(field.at[0, c, i], fields[c])
                put(diag.at[c, i], diags[c])
            put(node.at[i], nodes)
        return 0

    lax.fori_loop(0, 8, setup, 0)

    def fluxes(coefs, e, e0y, e0z, e1x, e1z, e2x, e2y):
        return (coefs[0] * ((e2y - e[2]) - (e1z - e[1])),
                coefs[1] * ((e0z - e[0]) - (e2x - e[2])),
                coefs[2] * ((e1x - e[1]) - (e0y - e[0])))

    def curl_back(gv, g0y, g0z, g1x, g1z, g2x, g2y):
        return ((g1z - gv[1]) - (g2y - gv[2]), (g2x - gv[2]) - (g0z - gv[0]), (g0y - gv[0]) - (g1x - gv[1]))

    def operator_step(k, _):
        now, later, before = k, k + 1, jnp.maximum(k - 1, 0)
        weight = jnp.where(k == 0, 0.0, jnp.where(k == 1, 0.5, 0.25))

        def strip_first(t, _):
            r = [at(fieldS.at[now, c, t]) for c in range(3)]
            q = ((pltpu.roll(r[0], 8, 1) - r[0]) + (at(fieldS.at[now, 1, t], -1) - r[1])) + (pltpu.roll(r[2], 1, 1) - r[2])
            put(phiS.at[t], q * at(nodeS.at[t]))
            for c in range(3):
                put(sS.at[c, t], r[c] * at(diagS.at[c, t]))
            return 0

        def strip_second(t, _):
            e = [at(sS.at[c, t]) for c in range(3)]
            out = fluxes([at(coefS.at[3 + c, t]) for c in range(3)], e,
                         at(sS.at[0, t], 1), pltpu.roll(e[0], 127, 1), pltpu.roll(e[1], 120, 1),
                         pltpu.roll(e[1], 127, 1), pltpu.roll(e[2], 120, 1), at(sS.at[2, t], 1))
            for c in range(3):
                put(gS.at[c, t], out[c])
            return 0

        def strip_third(t, _):
            gv = [at(gS.at[c, t]) for c in range(3)]
            w = curl_back(gv, at(gS.at[0, t], -1), pltpu.roll(gv[0], 1, 1), pltpu.roll(gv[1], 8, 1),
                          pltpu.roll(gv[1], 1, 1), pltpu.roll(gv[2], 8, 1), at(gS.at[2, t], -1))
            p = at(phiS.at[t])
            up = (pltpu.roll(p, 120, 1), at(phiS.at[t], 1), pltpu.roll(p, 127, 1))
            for c in range(3):
                u = at(sS.at[c, t]) + (up[c] - p)
                put(fieldS.at[later, c, t], (w[c] + at(coefS.at[c, t]) * u - at(fieldS.at[now, c, t]))
                    - weight * at(fieldS.at[before, c, t]))
            return 0

        for part in (strip_first, strip_second, strip_third):
            for t in range(2):
                part(t, 0)

        ready = []
        for n_row in range(2):
            x = n_row + k
            b = x + OFF
            f = [at(field.at[now, c, b]) for c in range(3)]
            q = ((at(field.at[now, 0, b - 1]) - f[0]) + (at(field.at[now, 1, b], -1) - f[1])) + (
                z_down(f[2], at(fieldS.at[now, 2, 0]), x) - f[2])
            ready.append((b, [f[c] * at(diag.at[c, b]) for c in range(3)], q * at(node.at[b])))
        for b, scaled, potential in ready:
            for c in range(3):
                put(s.at[c, b], scaled[c])
            put(phi.at[b], potential)

        def read(x):
            i = x + OFF
            g_own = [at(g.at[c, i]) for c in range(3)]
            g_x = [at(g.at[c, i - 1]) for c in (1, 2)]
            g_y = [at(g.at[c, i], -1) for c in (0, 2)]
            p, p_x, p_y = at(phi.at[i]), at(phi.at[i + 1]), at(phi.at[i], 1)
            s_own = [at(s.at[c, i]) for c in range(3)]
            r = [at(field.at[now, c, i]) for c in range(3)]
            old = [at(field.at[before, c, i]) for c in range(3)]
            mass = [at(coef.at[c, i]) for c in range(3)]
            a = i + 2
            e = [at(s.at[c, a]) for c in range(3)]
            e_x = [at(s.at[c, a + 1]) for c in (1, 2)]
            e_y = [at(s.at[c, a], 1) for c in (0, 2)]
            curl = [at(coef.at[3 + c, a]) for c in range(3)]
            b = i + 5
            f = [at(field.at[now, c, b]) for c in range(3)]
            f_x, f_y = at(field.at[now, 0, b - 1]), at(field.at[now, 1, b], -1)
            inverse, inverse_node = [at(diag.at[c, b]) for c in range(3)], at(node.at[b])
            strip = (at(gS.at[0, 0]), at(gS.at[1, 0]), at(phiS.at[1]), at(sS.at[0, 1]), at(sS.at[1, 1]),
                     at(fieldS.at[now, 2, 0]))
            return (g_own, g_x, g_y, p, p_x, p_y, s_own, r, old, mass, e, e_x, e_y, curl, f, f_x, f_y, inverse,
                    inverse_node, strip)

        def work(x, values):
            (g_own, g_x, g_y, p, p_x, p_y, s_own, r, old, mass, e, e_x, e_y, curl, f, f_x, f_y, inverse,
             inverse_node, strip) = values
            w = curl_back(g_own, g_y[0], z_down(g_own[0], strip[0], x), g_x[0],
                          z_down(g_own[1], strip[1], x), g_x[1], g_y[1])
            up = (p_x, p_y, z_up(p, strip[2], x))
            u = [s_own[c] + (up[c] - p) for c in range(3)]
            v = [((w[c] + mass[c] * u[c]) - r[c]) - weight * old[c] for c in range(3)]
            flux = fluxes(curl, e, e_y[0], z_up(e[0], strip[3], x + 2), e_x[0],
                          z_up(e[1], strip[4], x + 2), e_x[1], e_y[1])
            q = ((f_x - f[0]) + (f_y - f[1])) + (z_down(f[2], strip[5], x + 5) - f[2])
            return r, u, v, flux, q * inverse_node, [f[c] * inverse[c] for c in range(3)]

        def write(x, results, sums):
            r, u, v, flux, potential, scaled = results
            i = x + OFF
            inside = (x >= 4) & (x < 12)
            to = jnp.where(inside, x - 4, 8)
            for c in range(3):
                put(field.at[later, c, i], v[c])
                put(g.at[c, i + 2], flux[c])
                put(s.at[c, i + 5], scaled[c])
            put(phi.at[i + 5], potential)
            sums = list(sums)
            for c in range(3):
                precond[k, c, to] = u[c]
                for n, prod in ((0, r[c] * u[c]), (1, v[c] * u[c])):
                    ends = jnp.where(below_half, prod[32:40], prod[0:8])
                    part = ((prod[8:16] + prod[16:24]) + prod[24:32]) + ends
                    sums[n] = sums[n] + jnp.where(inside, part, 0.0)
            return tuple(sums)

        def rows(n, sums):
            x = 2 * n + k - 3
            first, second = read(x), read(x + 1)
            first, second = work(x, first), work(x + 1, second)
            return write(x + 1, second, write(x, first, sums))

        zero = jnp.zeros((8, 128), f32)
        sums = lax.fori_loop(0, 9 - k, rows, (zero, zero))
        dots[2 * k] = sums[0]
        dots[2 * k + 1] = sums[1]
        return 0

    lax.fori_loop(0, 4, operator_step, 0)

    row_lane = lax.broadcasted_iota(jnp.int32, (1, 128), 1) // 16
    parts = [jnp.sum(dots[d], axis=0, keepdims=True) for d in range(8)]
    for shift in (64, 32, 16):
        parts = [t + pltpu.roll(t, shift, 1) for t in parts]
    moments = parts[0]
    for d in range(1, 8):
        moments = jnp.where(row_lane == d, parts[d], moments)
    partial[...] = jnp.broadcast_to(moments, partial.shape)

    def look(x, _):
        for c in range(3):
            sink[x, c] = s[c, x + OFF, 16:24] + g[c, x + OFF, 16:24]
        sink[x, 3] = phi[x + OFF, 16:24]
        return 0

    lax.fori_loop(0, 2, look, 0)


def finish(everyone, field, precond, solution_out, residual_out):
    total = jnp.sum(everyone[...], axis=0, keepdims=True)
    lane = lax.broadcasted_iota(jnp.int32, (1, 128), 1)
    dots = [jnp.broadcast_to(jnp.sum(jnp.where(lane // 16 == d, total, 0.0), axis=1, keepdims=True), (8, 128))
            for d in range(8)]
    size = [1.0] + [2.0 ** (1 - k) for k in range(1, 9)]
    moment = [dots[0], dots[1]]
    for k in range(1, 4):
        moment.append((dots[2 * k] * (2.0 / size[k] ** 2) - moment[0]) * size[2 * k])
        moment.append((dots[2 * k + 1] * (2.0 / (size[k] * size[k + 1])) - moment[1]) * size[2 * k + 1])
    row, earlier = moment, None
    alpha, beta = [row[1] / row[0]], [None]
    for k in range(1, 4):
        following = [None] * 8
        for l in range(k, 8 - k):
            t = row[l + 1] - alpha[k - 1] * row[l] + WEIGHT[l if l < 2 else 2] * row[l - 1]
            if k > 1:
                t = t - beta[k - 1] * earlier[l]
            following[l] = t
        alpha.append(following[k + 1] / following[k] - row[k] / row[k - 1])
        beta.append(following[k] / row[k - 1])
        row, earlier = following, row
    zero = jnp.zeros((8, 128), jnp.float32)
    older, newer = [zero] * 6, [zero + 1.0] + [zero] * 5
    value_older, value = zero, zero + 1.0
    weight = lambda l: WEIGHT[min(l, 2)]
    for k in range(4):
        nxt = []
        for l in range(6):
            t = -alpha[k] * newer[l]
            if l > 0:
                t = t + newer[l - 1]
            if l < 5:
                t = t + weight(l + 1) * newer[l + 1]
            if k > 0:
                t = t - beta[k] * older[l]
            nxt.append(t)
        step = (-1.0 - alpha[k]) * value
        if k > 0:
            step = step - beta[k] * value_older
        older, newer, value_older, value = newer, nxt, value, step
    inverse = 1.0 / value
    e = [newer[l] * inverse for l in range(5)]
    S = [None] * 4
    S[3] = -e[4]
    S[2] = -e[3] - S[3]
    S[1] = -e[2] - S[2] - weight(3) * S[3]
    S[0] = -e[1] - S[1] - weight(2) * S[2]
    e = [v[0:1] for v in e]
    S = [v[0:1] for v in S]

    def combine(x, _):
        rows, first = pl.ds(OWN, 32), pl.ds(OWN - LO, 32)
        for c in range(3):
            v = [field[k, c, x + OFF + 4, rows, :] for k in range(5)]
            u = [precond[k, c, x, first, :] for k in range(4)]
            residual_out[c, x] = (e[0] * v[0] + e[1] * v[1]) + (e[2] * v[2] + e[3] * v[3]) + e[4] * v[4]
            solution_out[c, x] = (S[0] * u[0] + S[1] * u[1]) + (S[2] * u[2] + S[3] * u[3])
        return 0

    lax.fori_loop(0, 8, combine, 0)


def shape(*dims):
    return jax.ShapeDtypeStruct(dims, jnp.float32)


def call(kernel, outs, ins, mib, scratch=(), flops=1000000):
    return pl.pallas_call(
        kernel, out_shape=outs, in_specs=[VMEM] * len(ins), out_specs=jax.tree.map(lambda _: VMEM, outs),
        scratch_shapes=list(scratch),
        compiler_params=pltpu.CompilerParams(vmem_limit_bytes=mib << 20),
        cost_estimate=pl.CostEstimate(flops=flops, bytes_accessed=1 << 20, transcendentals=0))(*ins)


def exchange(low, high, axis):
    n = lax.axis_size(axis)
    up = [(i, (i + 1) % n) for i in range(n)]
    return lax.ppermute(high, axis, up), lax.ppermute(low, axis, [(j, i) for i, j in up])


def body(right, mass, curl):
    face = (shape(3, 8, 32, 128),) + (shape(3, 4, 32, 128),) * 2
    b, *ends = call(load, face, (right,), 8)
    b = (b,) + exchange(*ends, "gx")
    c, *ends = call(load, face, (curl,), 8)
    c = (c,) + exchange(*ends, "gx")
    m, *ends = call(load_mass, face, (mass, c[0]), 8)
    m = (m,) + exchange(*ends, "gx")
    ends = (shape(9, 4, 8, 128),) * 2
    y_own = exchange(*call(pack_y_own, ends, (b[0], m[0], c[0]), 8), "gy")
    columns = (shape(9, ROWS, 128),) * 2
    extended = (shape(3, X, Y, 128), shape(6, X, Y, 128))
    own = call(pack_z_own, columns + (shape(3, 8, ROWS, 128), shape(6, 8, ROWS, 128)), (b[0], m[0], c[0]), 8, flops=20000000)
    y_halo = exchange(*call(pack_y_halo, ends, (own[0],) + b[1:] + m[1:] + c[1:], 8), "gy")
    low, high, *middle = call(pack_z_middle, columns + extended, b[1:] + m[1:] + c[1:] + tuple(own), 8, flops=20000000)
    low, high, *ends, field, coef = call(
        pack_z_edge, columns + (shape(5, ROWS, 128),) * 2 + (shape(3, 16, 16, 128), shape(6, 16, 16, 128)),
        y_own + y_halo + (low, high, *middle), 8)
    sides = (low, high) + exchange(*ends, "gz")
    block = call(invert, extended + (shape(3, X, Y, 128), shape(X, Y, 128)), (*middle, field, coef), 8, flops=20000000)

    def held(*dims):
        return pltpu.VMEM(dims + (Y, 128), jnp.float32)

    axes = ("gx", "gy", "gz")
    devices = lax.axis_size(axes)
    vectors, precond, rows, _ = call(
        main, (shape(5, 3, X, Y, 128), shape(4, 3, 9, ROWS, 128), shape(devices, 128), shape(2, 4, 8, 128)),
        tuple(block) + sides, 20,
        [held(3, X), held(X), held(3, X), held(X), held(3, X),
         held(5, 3, 2), held(6, 2), held(3, 2), held(2), held(3, 2), held(2), held(3, 2), pltpu.VMEM((8, 8, 128), jnp.float32)])
    everyone = lax.all_to_all(rows.reshape(devices, 1, 128), axes, 0, 0, tiled=True).reshape(devices, 128)
    return call(finish, (shape(3, 8, 32, 128),) * 2, (everyone, vectors, precond), 16)


def solution(mesh):
    spec = P(None, "gx", "gy", "gz")
    return jax.shard_map(body, mesh=mesh, in_specs=(spec,) * 3, out_specs=(spec,) * 2, check_vma=False)
```

```python
import jax
import jax.numpy as jnp
from jax import lax
from jax.experimental import pallas as pl
from jax.experimental.pallas import tpu as pltpu
from jax.sharding import PartitionSpec as P


X, Y = 24, 56
OFF, OWN = 4, 12
LO, ROWS = 8, 40
WEIGHT = (0.0, 0.5, 0.25, 0.25, 0.25)
VMEM = pl.BlockSpec(memory_space=pltpu.VMEM)


def load(source, own, low, high):
    def move(c, _):
        for to, x in ((low, 0), (high, 4)):
            value = source[c, x : x + 4]
            own[c, x : x + 4] = value
            to[c] = value
        return 0

    lax.fori_loop(0, 3, move, 0)


def load_mass(source, curl, own, low, high):
    load(source, own, low, high)
    high[1, 0] = source[1, 4] + curl[2, 3]
    high[2, 0] = source[2, 4] + curl[1, 3]


def pack_y(pairs, *refs):
    refs, (low, high) = refs[:-2], refs[-2:]
    n = len(refs) // 3
    sub = lax.broadcasted_iota(jnp.int32, (8, 128), 0)

    def tile(field, c, p, half, y):
        return pairs(refs[field * n : field * n + n], c, p, half, y)

    def pack(c, _):
        for field in range(3):
            for p in range(4):
                a, b = tile(field, c, p, 0, 0), tile(field, c, p, 1, 0)
                low[3 * field + c, p] = jnp.where(sub < 4, a, pltpu.roll(b, 4, 0))
                a, b = tile(field, c, p, 0, 24), tile(field, c, p, 1, 24)
                high[3 * field + c, p] = jnp.where(sub < 4, pltpu.roll(a, 4, 0), b)
        return 0

    lax.fori_loop(0, 3, pack, 0)

    def corrected(i, _):
        c, other = 2 * i, 2 - 2 * i
        for p in range(4):
            a = pltpu.roll(tile(2, other, p, 0, 24), 5, 0)
            b = pltpu.roll(tile(2, other, p, 1, 24), 1, 0)
            high[3 + c, p] = high[3 + c, p] + jnp.where(sub == 0, a, jnp.where(sub == 4, b, 0.0))
        return 0

    lax.fori_loop(0, 2, corrected, 0)


def pack_y_own(*refs):
    pack_y(lambda own, c, p, half, y: own[0][c, p + 4 * half, y : y + 8], *refs)


def pack_y_halo(after, *refs):
    pack_y(lambda ends, c, p, half, y: ends[half][c, p, y : y + 8], *refs)


def all_strips(field, coef, octets, low, high, xs=range(16), before=None):
    group = lax.broadcasted_iota(jnp.int32, (8, 128), 1) >> 2
    each, x0, start, begin, stride = octets

    def three(i, _):
        c, o = i // each, i % each
        here = pl.ds(pl.multiple_of(start + 8 * o, 8), 8)
        to = pl.ds(pl.multiple_of(begin + stride * o, 8), 8)
        done = []
        for source, comp, dest in ((field, c, c), (coef, c, 3 + c), (coef, 3 + c, 6 + c)):
            first, last = (jnp.zeros((8, 128), jnp.float32),) * 2
            if before:
                first, last = before[0][dest, to, :], before[1][dest, to, :]
            for x in xs:
                t = source[comp, x0 + x, here, :]
                first = jnp.where(group == 2 * x + 1, pltpu.roll(t, 8 * x + 4, 1), first)
                last = jnp.where(group == 2 * x, pltpu.roll(t, (8 * x + 4) % 128, 1), last)
            done.append((dest, first, last))
        for dest, first, last in done:
            low[dest, to, :] = first
            high[dest, to, :] = last
        return 0

    lax.fori_loop(0, 3 * each, three, 0)
    lane = lax.broadcasted_iota(jnp.int32, (8, 128), 1)

    def corrected(o, _):
        here = pl.ds(pl.multiple_of(start + 8 * o, 8), 8)
        to = pl.ds(pl.multiple_of(begin + stride * o, 8), 8)
        lasts = []
        for which in range(2):
            last = jnp.zeros((8, 128), jnp.float32)
            for x in xs:
                t = coef[4 - which, x0 + x, here, :]
                last = jnp.where(lane == 8 * x, pltpu.roll(t, (8 * x + 5) % 128, 1), last)
            lasts.append(high[3 + which, to, :] + last)
        for which in range(2):
            high[3 + which, to, :] = lasts[which]
        return 0

    lax.fori_loop(0, each, corrected, 0)


def pack_z_own(right, mass, curl, low, high, field, coef):
    def assemble(c, _):
        for to, source in ((field.at[c], right), (coef.at[c], mass), (coef.at[3 + c], curl)):
            to[:, 4:36] = source[c]
        return 0

    lax.fori_loop(0, 3, assemble, 0)
    all_strips(field, coef, (3, -4, 8, 8, 8), low, high, range(4, 12))


def pack_z_middle(*refs):
    blocks = refs[0:2], refs[2:4], refs[4:6]
    own_low, own_high, own_field, own_coef, low, high, field, coef = refs[6:]

    def assemble(c, _):
        for n, (below, above) in enumerate(blocks):
            to = field.at[c] if n == 0 else coef.at[3 * n - 3 + c]
            own = own_field.at[c] if n == 0 else own_coef.at[3 * n - 3 + c]
            to[OFF : OFF + 4, OWN : OWN + 32] = below[c]
            to[OFF + 4 : OFF + 12, LO : LO + ROWS] = own[...]
            to[OFF + 12 : OFF + 16, OWN : OWN + 32] = above[c]
        return 0

    lax.fori_loop(0, 3, assemble, 0)
    ends = (0, 1, 2, 3, 12, 13, 14, 15)
    all_strips(field, coef, (3, OFF, 16, 8, 8), low, high, ends, (own_low, own_high))


def pack_z_edge(own_low, own_high, halo_low, halo_high, middle_low, middle_high, middle_field, middle_coef,
                low, high, send_low, send_high, field, coef):
    sub = lax.broadcasted_iota(jnp.int32, (8, 128), 0)

    def assemble(c, _):
        for n in range(3):
            to = field.at[c] if n == 0 else coef.at[3 * n - 3 + c]
            source = middle_field.at[c] if n == 0 else middle_coef.at[3 * n - 3 + c]
            comp = 3 * n + c
            for p in range(4):
                for lows, highs, x0, x1 in ((halo_low, halo_high, p, p + 12), (own_low, own_high, p + 4, p + 8)):
                    lower, upper = lows[comp, p], highs[comp, p]
                    to[x0, 0:8] = jnp.where(sub < 4, lower, source[OFF + x0, 8:16])
                    to[x1, 0:8] = jnp.where(sub < 4, pltpu.roll(lower, 4, 0), source[OFF + x1, 8:16])
                    to[x0, 8:16] = jnp.where(sub < 4, source[OFF + x0, 40:48], pltpu.roll(upper, 4, 0))
                    to[x1, 8:16] = jnp.where(sub < 4, source[OFF + x1, 40:48], upper)
        return 0

    lax.fori_loop(0, 3, assemble, 0)
    all_strips(field, coef, (2, 0, 0, 0, 32), low, high)
    for comp in range(9):
        low[comp, 8:32] = middle_low[comp, 8:32]
        high[comp, 8:32] = middle_high[comp, 8:32]
    for n in range(5):
        down, up = low[n], high[n]
        if n < 4:
            down, up = down + pltpu.roll(low[n + 5], 124, 1), up + pltpu.roll(high[n + 5], 4, 1)
        send_low[n] = down
        send_high[n] = up


def at(ref, dy=0):
    return ref[pl.ds(LO + dy, ROWS), :]


def put(ref, value):
    ref[pl.ds(LO, ROWS), :] = value


def diagonals(m, c, cy, cx, cz, mx, my, mz):
    d0 = m[0] + c[1] + cz[1] + c[2] + cy[2]
    d1 = m[1] + c[2] + cx[2] + c[0] + cz[0]
    d2 = m[2] + c[0] + cy[0] + c[1] + cx[1]
    dn = m[0] + mx + m[1] + my + m[2] + mz
    return 1.0 / d0, 1.0 / d1, 1.0 / d2, 1.0 / dn


def invert(field_middle, coef_middle, field_edge, coef_edge, field, coef, diag, node):
    def assemble(c, _):
        coef[c, OFF - 1] = jnp.zeros((Y, 128), jnp.float32)
        for x in range(OFF, OFF + 16):
            coef[c, x, 0:8] = jnp.zeros((8, 128), jnp.float32)
            coef[c, x, 16:40] = coef_middle[c, x, 16:40]
            coef[c, x, 8:16] = coef_edge[c, x - OFF, 0:8]
            coef[c, x, 40:48] = coef_edge[c, x - OFF, 8:16]
        return 0

    def assemble_field(c, _):
        for x in range(OFF, OFF + 16):
            field[c, x, 16:40] = field_middle[c, x, 16:40]
            field[c, x, 8:16] = field_edge[c, x - OFF, 0:8]
            field[c, x, 40:48] = field_edge[c, x - OFF, 8:16]
        return 0

    lax.fori_loop(0, 6, assemble, 0)
    lax.fori_loop(0, 3, assemble_field, 0)

    def row(x, _):
        i = x + OFF
        m = [at(coef.at[c, i]) for c in range(3)]
        c_ = [at(coef.at[3 + c, i]) for c in range(3)]
        cy = [at(coef.at[3 + c, i], -1) for c in range(3)]
        cx = [at(coef.at[3 + c, i - 1]) for c in range(3)]
        cz = [pltpu.roll(c_[c], 1, 1) for c in range(2)]
        out = diagonals(m, c_, cy, cx, cz, at(coef.at[0, i - 1]), at(coef.at[1, i], -1), pltpu.roll(m[2], 1, 1))
        for c in range(3):
            put(diag.at[c, i], out[c])
        put(node.at[i], out[3])
        return 0

    lax.fori_loop(0, 16, row, 0)


def main(field_in, coef, diag_in, node_in, zown_low, zown_high, zlow, zhigh, field, precond, partial, sink,
         diag, node, s, phi, g, fieldS, coefS, diagS, nodeS, sS, phiS, gS, dots):
    f32 = jnp.float32
    lane = lax.broadcasted_iota(jnp.int32, (ROWS, 128), 1)
    first_lane, last_lane = lane == 0, lane == 127
    below_half = lax.broadcasted_iota(jnp.int32, (8, 128), 0) < 4

    def z_up(value, strip, x):
        return jnp.where(last_lane, pltpu.roll(strip, (123 - 8 * x) & 127, 1), pltpu.roll(value, 127, 1))

    def z_down(value, strip, x):
        return jnp.where(first_lane, pltpu.roll(strip, (125 - 8 * x) & 127, 1), pltpu.roll(value, 1, 1))

    upper = (lane & 4) != 0
    for comp in range(9):
        lower_part, upper_part = zlow[comp % 5], zhigh[comp % 5]
        if comp >= 5:
            lower_part, upper_part = pltpu.roll(lower_part, 124, 1), pltpu.roll(upper_part, 4, 1)
        for t, value in ((0, jnp.where(upper, zown_low[comp], lower_part)),
                         (1, jnp.where(upper, upper_part, zown_high[comp]))):
            put(fieldS.at[0, comp, t] if comp < 3 else coefS.at[comp - 3, t], value)
            if comp >= 3:
                coefS[comp - 3, t, 0:8] = jnp.zeros((8, 128), f32)

    def setup_strip(t, _):
        m = [at(coefS.at[c, t]) for c in range(3)]
        c_ = [at(coefS.at[3 + c, t]) for c in range(3)]
        cy = [at(coefS.at[3 + c, t], -1) for c in range(3)]
        cx = [jnp.where(lane < 8, 0.0, pltpu.roll(v, 8, 1)) for v in c_]
        cz = [jnp.where((lane & 7) == 0, 0.0, pltpu.roll(v, 1, 1)) for v in c_]
        out = diagonals(m, c_, cy, cx, cz, pltpu.roll(m[0], 8, 1), at(coefS.at[1, t], -1), pltpu.roll(m[2], 1, 1))
        for c in range(3):
            put(diagS.at[c, t], out[c])
        put(nodeS.at[t], out[3])
        return 0

    for t in range(2):
        setup_strip(t, 0)

    def setup(n, _):
        ready = []
        for x in (4 * n, 4 * n + 1, 4 * n + 2, 4 * n + 3):
            i = x + OFF
            ready.append((i, [at(field_in.at[c, i]) for c in range(3)], [
                jnp.where(first_lane, pltpu.roll(at(diagS.at[c, 0]), 124 - 8 * x, 1), at(diag_in.at[c, i]))
                for c in range(3)], jnp.where(first_lane, pltpu.roll(at(nodeS.at[0]), 124 - 8 * x, 1), at(node_in.at[i]))))
        for i, fields, diags, nodes in ready:
            for c in range(3):
                put(field.at[0, c, i], fields[c])
                put(diag.at[c, i], diags[c])
            put(node.at[i], nodes)
        return 0

    lax.fori_loop(0, 4, setup, 0)

    def fluxes(coefs, e, e0y, e0z, e1x, e1z, e2x, e2y):
        return (coefs[0] * ((e2y - e[2]) - (e1z - e[1])),
                coefs[1] * ((e0z - e[0]) - (e2x - e[2])),
                coefs[2] * ((e1x - e[1]) - (e0y - e[0])))

    def curl_back(gv, g0y, g0z, g1x, g1z, g2x, g2y):
        return ((g1z - gv[1]) - (g2y - gv[2]), (g2x - gv[2]) - (g0z - gv[0]), (g0y - gv[0]) - (g1x - gv[1]))

    def operator_step(k, _):
        now, later, before = k, k + 1, jnp.maximum(k - 1, 0)
        weight = jnp.where(k == 0, 0.0, jnp.where(k == 1, 0.5, 0.25))

        def strip_first(t, _):
            r = [at(fieldS.at[now, c, t]) for c in range(3)]
            q = ((pltpu.roll(r[0], 8, 1) - r[0]) + (at(fieldS.at[now, 1, t], -1) - r[1])) + (pltpu.roll(r[2], 1, 1) - r[2])
            put(phiS.at[t], q * at(nodeS.at[t]))
            for c in range(3):
                put(sS.at[c, t], r[c] * at(diagS.at[c, t]))
            return 0

        def strip_second(t, _):
            e = [at(sS.at[c, t]) for c in range(3)]
            out = fluxes([at(coefS.at[3 + c, t]) for c in range(3)], e,
                         at(sS.at[0, t], 1), pltpu.roll(e[0], 127, 1), pltpu.roll(e[1], 120, 1),
                         pltpu.roll(e[1], 127, 1), pltpu.roll(e[2], 120, 1), at(sS.at[2, t], 1))
            for c in range(3):
                put(gS.at[c, t], out[c])
            return 0

        def strip_third(t, _):
            gv = [at(gS.at[c, t]) for c in range(3)]
            w = curl_back(gv, at(gS.at[0, t], -1), pltpu.roll(gv[0], 1, 1), pltpu.roll(gv[1], 8, 1),
                          pltpu.roll(gv[1], 1, 1), pltpu.roll(gv[2], 8, 1), at(gS.at[2, t], -1))
            p = at(phiS.at[t])
            up = (pltpu.roll(p, 120, 1), at(phiS.at[t], 1), pltpu.roll(p, 127, 1))
            for c in range(3):
                u = at(sS.at[c, t]) + (up[c] - p)
                put(fieldS.at[later, c, t], (w[c] + at(coefS.at[c, t]) * u - at(fieldS.at[now, c, t]))
                    - weight * at(fieldS.at[before, c, t]))
            return 0

        for part in (strip_first, strip_second, strip_third):
            for t in range(2):
                part(t, 0)

        ready = []
        for n_row in range(2):
            x = n_row + k
            b = x + OFF
            f = [at(field.at[now, c, b]) for c in range(3)]
            q = ((at(field.at[now, 0, b - 1]) - f[0]) + (at(field.at[now, 1, b], -1) - f[1])) + (
                z_down(f[2], at(fieldS.at[now, 2, 0]), x) - f[2])
            ready.append((b, [f[c] * at(diag.at[c, b]) for c in range(3)], q * at(node.at[b])))
        for b, scaled, potential in ready:
            for c in range(3):
                put(s.at[c, b], scaled[c])
            put(phi.at[b], potential)

        def read(x):
            i = x + OFF
            g_own = [at(g.at[c, i]) for c in range(3)]
            g_x = [at(g.at[c, i - 1]) for c in (1, 2)]
            g_y = [at(g.at[c, i], -1) for c in (0, 2)]
            p, p_x, p_y = at(phi.at[i]), at(phi.at[i + 1]), at(phi.at[i], 1)
            s_own = [at(s.at[c, i]) for c in range(3)]
            r = [at(field.at[now, c, i]) for c in range(3)]
            old = [at(field.at[before, c, i]) for c in range(3)]
            mass = [at(coef.at[c, i]) for c in range(3)]
            a = i + 2
            e = [at(s.at[c, a]) for c in range(3)]
            e_x = [at(s.at[c, a + 1]) for c in (1, 2)]
            e_y = [at(s.at[c, a], 1) for c in (0, 2)]
            curl = [at(coef.at[3 + c, a]) for c in range(3)]
            b = i + 5
            f = [at(field.at[now, c, b]) for c in range(3)]
            f_x, f_y = at(field.at[now, 0, b - 1]), at(field.at[now, 1, b], -1)
            inverse, inverse_node = [at(diag.at[c, b]) for c in range(3)], at(node.at[b])
            strip = (at(gS.at[0, 0]), at(gS.at[1, 0]), at(phiS.at[1]), at(sS.at[0, 1]), at(sS.at[1, 1]),
                     at(fieldS.at[now, 2, 0]))
            return (g_own, g_x, g_y, p, p_x, p_y, s_own, r, old, mass, e, e_x, e_y, curl, f, f_x, f_y, inverse,
                    inverse_node, strip)

        def work(x, values):
            (g_own, g_x, g_y, p, p_x, p_y, s_own, r, old, mass, e, e_x, e_y, curl, f, f_x, f_y, inverse,
             inverse_node, strip) = values
            w = curl_back(g_own, g_y[0], z_down(g_own[0], strip[0], x), g_x[0],
                          z_down(g_own[1], strip[1], x), g_x[1], g_y[1])
            up = (p_x, p_y, z_up(p, strip[2], x))
            u = [s_own[c] + (up[c] - p) for c in range(3)]
            v = [((w[c] + mass[c] * u[c]) - r[c]) - weight * old[c] for c in range(3)]
            flux = fluxes(curl, e, e_y[0], z_up(e[0], strip[3], x + 2), e_x[0],
                          z_up(e[1], strip[4], x + 2), e_x[1], e_y[1])
            q = ((f_x - f[0]) + (f_y - f[1])) + (z_down(f[2], strip[5], x + 5) - f[2])
            return r, u, v, flux, q * inverse_node, [f[c] * inverse[c] for c in range(3)]

        def write(x, results, sums):
            r, u, v, flux, potential, scaled = results
            i = x + OFF
            inside = (x >= 4) & (x < 12)
            to = jnp.where(inside, x - 4, 8)
            for c in range(3):
                put(field.at[later, c, i], v[c])
                put(g.at[c, i + 2], flux[c])
                put(s.at[c, i + 5], scaled[c])
            put(phi.at[i + 5], potential)
            sums = list(sums)
            for c in range(3):
                precond[k, c, to] = u[c]
                for n, prod in ((0, r[c] * u[c]), (1, v[c] * u[c])):
                    ends = jnp.where(below_half, prod[32:40], prod[0:8])
                    part = ((prod[8:16] + prod[16:24]) + prod[24:32]) + ends
                    sums[n] = sums[n] + jnp.where(inside, part, 0.0)
            return tuple(sums)

        def rows(n, sums):
            x = 2 * n + k - 3
            first, second = read(x), read(x + 1)
            first, second = work(x, first), work(x + 1, second)
            return write(x + 1, second, write(x, first, sums))

        zero = jnp.zeros((8, 128), f32)
        sums = lax.fori_loop(0, 9 - k, rows, (zero, zero))
        dots[2 * k] = sums[0]
        dots[2 * k + 1] = sums[1]
        return 0

    lax.fori_loop(0, 4, operator_step, 0)

    row_lane = lax.broadcasted_iota(jnp.int32, (1, 128), 1) // 16
    parts = [jnp.sum(dots[d], axis=0, keepdims=True) for d in range(8)]
    for shift in (64, 32, 16):
        parts = [t + pltpu.roll(t, shift, 1) for t in parts]
    moments = parts[0]
    for d in range(1, 8):
        moments = jnp.where(row_lane == d, parts[d], moments)
    partial[...] = jnp.broadcast_to(moments, partial.shape)

    def look(x, _):
        for c in range(3):
            sink[x, c] = s[c, x + OFF, 16:24] + g[c, x + OFF, 16:24]
        sink[x, 3] = phi[x + OFF, 16:24]
        return 0

    lax.fori_loop(0, 2, look, 0)


def finish(everyone, field, precond, solution_out, residual_out):
    total = jnp.sum(everyone[...], axis=0, keepdims=True)
    lane = lax.broadcasted_iota(jnp.int32, (1, 128), 1)
    dots = [jnp.broadcast_to(jnp.sum(jnp.where(lane // 16 == d, total, 0.0), axis=1, keepdims=True), (8, 128))
            for d in range(8)]
    size = [1.0] + [2.0 ** (1 - k) for k in range(1, 9)]
    moment = [dots[0], dots[1]]
    for k in range(1, 4):
        moment.append((dots[2 * k] * (2.0 / size[k] ** 2) - moment[0]) * size[2 * k])
        moment.append((dots[2 * k + 1] * (2.0 / (size[k] * size[k + 1])) - moment[1]) * size[2 * k + 1])
    row, earlier = moment, None
    alpha, beta = [row[1] / row[0]], [None]
    for k in range(1, 4):
        following = [None] * 8
        for l in range(k, 8 - k):
            t = row[l + 1] - alpha[k - 1] * row[l] + WEIGHT[l if l < 2 else 2] * row[l - 1]
            if k > 1:
                t = t - beta[k - 1] * earlier[l]
            following[l] = t
        alpha.append(following[k + 1] / following[k] - row[k] / row[k - 1])
        beta.append(following[k] / row[k - 1])
        row, earlier = following, row
    zero = jnp.zeros((8, 128), jnp.float32)
    older, newer = [zero] * 6, [zero + 1.0] + [zero] * 5
    value_older, value = zero, zero + 1.0
    weight = lambda l: WEIGHT[min(l, 2)]
    for k in range(4):
        nxt = []
        for l in range(6):
            t = -alpha[k] * newer[l]
            if l > 0:
                t = t + newer[l - 1]
            if l < 5:
                t = t + weight(l + 1) * newer[l + 1]
            if k > 0:
                t = t - beta[k] * older[l]
            nxt.append(t)
        step = (-1.0 - alpha[k]) * value
        if k > 0:
            step = step - beta[k] * value_older
        older, newer, value_older, value = newer, nxt, value, step
    inverse = 1.0 / value
    e = [newer[l] * inverse for l in range(5)]
    S = [None] * 4
    S[3] = -e[4]
    S[2] = -e[3] - S[3]
    S[1] = -e[2] - S[2] - weight(3) * S[3]
    S[0] = -e[1] - S[1] - weight(2) * S[2]
    e = [v[0:1] for v in e]
    S = [v[0:1] for v in S]

    def combine(x, _):
        rows, first = pl.ds(OWN, 32), pl.ds(OWN - LO, 32)
        for c in range(3):
            v = [field[k, c, x + OFF + 4, rows, :] for k in range(5)]
            u = [precond[k, c, x, first, :] for k in range(4)]
            residual_out[c, x] = (e[0] * v[0] + e[1] * v[1]) + (e[2] * v[2] + e[3] * v[3]) + e[4] * v[4]
            solution_out[c, x] = (S[0] * u[0] + S[1] * u[1]) + (S[2] * u[2] + S[3] * u[3])
        return 0

    lax.fori_loop(0, 8, combine, 0)


def shape(*dims):
    return jax.ShapeDtypeStruct(dims, jnp.float32)


def call(kernel, outs, ins, mib, scratch=(), flops=1000000):
    return pl.pallas_call(
        kernel, out_shape=outs, in_specs=[VMEM] * len(ins), out_specs=jax.tree.map(lambda _: VMEM, outs),
        scratch_shapes=list(scratch),
        compiler_params=pltpu.CompilerParams(vmem_limit_bytes=mib << 20),
        cost_estimate=pl.CostEstimate(flops=flops, bytes_accessed=1 << 20, transcendentals=0))(*ins)


def exchange(low, high, axis):
    n = lax.axis_size(axis)
    up = [(i, (i + 1) % n) for i in range(n)]
    return lax.ppermute(high, axis, up), lax.ppermute(low, axis, [(j, i) for i, j in up])


def body(right, mass, curl):
    face = (shape(3, 8, 32, 128),) + (shape(3, 4, 32, 128),) * 2
    b, *ends = call(load, face, (right,), 8)
    b = (b,) + exchange(*ends, "gx")
    c, *ends = call(load, face, (curl,), 8)
    c = (c,) + exchange(*ends, "gx")
    m, *ends = call(load_mass, face, (mass, c[0]), 8)
    m = (m,) + exchange(*ends, "gx")
    ends = (shape(9, 4, 8, 128),) * 2
    y_own = exchange(*call(pack_y_own, ends, (b[0], m[0], c[0]), 8), "gy")
    columns = (shape(9, ROWS, 128),) * 2
    extended = (shape(3, X, Y, 128), shape(6, X, Y, 128))
    own = call(pack_z_own, columns + (shape(3, 8, ROWS, 128), shape(6, 8, ROWS, 128)), (b[0], m[0], c[0]), 8, flops=20000000)
    y_halo = exchange(*call(pack_y_halo, ends, (own[0],) + b[1:] + m[1:] + c[1:], 8), "gy")
    low, high, *middle = call(pack_z_middle, columns + extended, b[1:] + m[1:] + c[1:] + tuple(own), 8, flops=20000000)
    low, high, *ends, field, coef = call(
        pack_z_edge, columns + (shape(5, ROWS, 128),) * 2 + (shape(3, 16, 16, 128), shape(6, 16, 16, 128)),
        y_own + y_halo + (low, high, *middle), 8)
    sides = (low, high) + exchange(*ends, "gz")
    block = call(invert, extended + (shape(3, X, Y, 128), shape(X, Y, 128)), (*middle, field, coef), 8, flops=20000000)

    def held(*dims):
        return pltpu.VMEM(dims + (Y, 128), jnp.float32)

    axes = ("gx", "gy", "gz")
    devices = lax.axis_size(axes)
    vectors, precond, rows, _ = call(
        main, (shape(5, 3, X, Y, 128), shape(4, 3, 9, ROWS, 128), shape(devices, 128), shape(2, 4, 8, 128)),
        tuple(block) + sides, 20,
        [held(3, X), held(X), held(3, X), held(X), held(3, X),
         held(5, 3, 2), held(6, 2), held(3, 2), held(2), held(3, 2), held(2), held(3, 2), pltpu.VMEM((8, 8, 128), jnp.float32)])
    everyone = lax.all_to_all(rows.reshape(devices, 1, 128), axes, 0, 0, tiled=True).reshape(devices, 128)
    return call(finish, (shape(3, 8, 32, 128),) * 2, (everyone, vectors, precond), 16)


def solution(mesh):
    spec = P(None, "gx", "gy", "gz")
    return jax.shard_map(body, mesh=mesh, in_specs=(spec,) * 3, out_specs=(spec,) * 2, check_vma=False)
```

```python
import jax
import jax.numpy as jnp
from jax import lax
from jax.experimental import pallas as pl
from jax.experimental.pallas import tpu as pltpu
from jax.sharding import PartitionSpec as P


X, Y = 24, 56
OFF, OWN = 4, 12
LO, ROWS = 8, 40
WEIGHT = (0.0, 0.5, 0.25, 0.25, 0.25)
VMEM = pl.BlockSpec(memory_space=pltpu.VMEM)


def load(source, own, low, high):
    def move(c, _):
        for to, x in ((low, 0), (high, 4)):
            value = source[c, x : x + 4]
            own[c, x : x + 4] = value
            to[c] = value
        return 0

    lax.fori_loop(0, 3, move, 0)


def load_mass(source, curl, own, low, high):
    load(source, own, low, high)
    high[1, 0] = source[1, 4] + curl[2, 3]
    high[2, 0] = source[2, 4] + curl[1, 3]


def pack_y(pairs, *refs):
    refs, (low, high) = refs[:-2], refs[-2:]
    n = len(refs) // 3
    sub = lax.broadcasted_iota(jnp.int32, (8, 128), 0)

    def tile(field, c, p, half, y):
        return pairs(refs[field * n : field * n + n], c, p, half, y)

    def pack(c, _):
        for field in range(3):
            for p in range(4):
                a, b = tile(field, c, p, 0, 0), tile(field, c, p, 1, 0)
                low[3 * field + c, p] = jnp.where(sub < 4, a, pltpu.roll(b, 4, 0))
                a, b = tile(field, c, p, 0, 24), tile(field, c, p, 1, 24)
                high[3 * field + c, p] = jnp.where(sub < 4, pltpu.roll(a, 4, 0), b)
        return 0

    lax.fori_loop(0, 3, pack, 0)

    def corrected(i, _):
        c, other = 2 * i, 2 - 2 * i
        for p in range(4):
            a = pltpu.roll(tile(2, other, p, 0, 24), 5, 0)
            b = pltpu.roll(tile(2, other, p, 1, 24), 1, 0)
            high[3 + c, p] = high[3 + c, p] + jnp.where(sub == 0, a, jnp.where(sub == 4, b, 0.0))
        return 0

    lax.fori_loop(0, 2, corrected, 0)


def pack_y_own(*refs):
    pack_y(lambda own, c, p, half, y: own[0][c, p + 4 * half, y : y + 8], *refs)


def pack_y_halo(after, *refs):
    pack_y(lambda ends, c, p, half, y: ends[half][c, p, y : y + 8], *refs)


def all_strips(field, coef, octets, low, high, xs=range(16), before=None):
    group = lax.broadcasted_iota(jnp.int32, (8, 128), 1) >> 2
    each, x0, start, begin, stride = octets

    def three(i, _):
        c, o = i // each, i % each
        here = pl.ds(pl.multiple_of(start + 8 * o, 8), 8)
        to = pl.ds(pl.multiple_of(begin + stride * o, 8), 8)
        done = []
        for source, comp, dest in ((field, c, c), (coef, c, 3 + c), (coef, 3 + c, 6 + c)):
            first, last = (jnp.zeros((8, 128), jnp.float32),) * 2
            if before:
                first, last = before[0][dest, to, :], before[1][dest, to, :]
            for x in xs:
                t = source[comp, x0 + x, here, :]
                first = jnp.where(group == 2 * x + 1, pltpu.roll(t, 8 * x + 4, 1), first)
                last = jnp.where(group == 2 * x, pltpu.roll(t, (8 * x + 4) % 128, 1), last)
            done.append((dest, first, last))
        for dest, first, last in done:
            low[dest, to, :] = first
            high[dest, to, :] = last
        return 0

    lax.fori_loop(0, 3 * each, three, 0)
    lane = lax.broadcasted_iota(jnp.int32, (8, 128), 1)

    def corrected(o, _):
        here = pl.ds(pl.multiple_of(start + 8 * o, 8), 8)
        to = pl.ds(pl.multiple_of(begin + stride * o, 8), 8)
        lasts = []
        for which in range(2):
            last = jnp.zeros((8, 128), jnp.float32)
            for x in xs:
                t = coef[4 - which, x0 + x, here, :]
                last = jnp.where(lane == 8 * x, pltpu.roll(t, (8 * x + 5) % 128, 1), last)
            lasts.append(high[3 + which, to, :] + last)
        for which in range(2):
            high[3 + which, to, :] = lasts[which]
        return 0

    lax.fori_loop(0, each, corrected, 0)


def pack_z_own(right, mass, curl, low, high, field, coef):
    def assemble(c, _):
        for to, source in ((field.at[c], right), (coef.at[c], mass), (coef.at[3 + c], curl)):
            to[:, 4:36] = source[c]
        return 0

    lax.fori_loop(0, 3, assemble, 0)
    all_strips(field, coef, (3, -4, 8, 8, 8), low, high, range(4, 12))


def pack_z_middle(*refs):
    blocks = refs[0:2], refs[2:4], refs[4:6]
    own_low, own_high, own_field, own_coef, low, high, field, coef = refs[6:]

    def assemble(c, _):
        for n, (below, above) in enumerate(blocks):
            to = field.at[c] if n == 0 else coef.at[3 * n - 3 + c]
            own = own_field.at[c] if n == 0 else own_coef.at[3 * n - 3 + c]
            to[OFF : OFF + 4, OWN : OWN + 32] = below[c]
            to[OFF + 4 : OFF + 12, LO : LO + ROWS] = own[...]
            to[OFF + 12 : OFF + 16, OWN : OWN + 32] = above[c]
        return 0

    lax.fori_loop(0, 3, assemble, 0)
    ends = (0, 1, 2, 3, 12, 13, 14, 15)
    all_strips(field, coef, (3, OFF, 16, 8, 8), low, high, ends, (own_low, own_high))


def pack_z_edge(own_low, own_high, halo_low, halo_high, middle_low, middle_high, middle_field, middle_coef,
                low, high, send_low, send_high, field, coef):
    sub = lax.broadcasted_iota(jnp.int32, (8, 128), 0)

    def assemble(c, _):
        for n in range(3):
            to = field.at[c] if n == 0 else coef.at[3 * n - 3 + c]
            source = middle_field.at[c] if n == 0 else middle_coef.at[3 * n - 3 + c]
            comp = 3 * n + c
            for p in range(4):
                for lows, highs, x0, x1 in ((halo_low, halo_high, p, p + 12), (own_low, own_high, p + 4, p + 8)):
                    lower, upper = lows[comp, p], highs[comp, p]
                    to[x0, 0:8] = jnp.where(sub < 4, lower, source[OFF + x0, 8:16])
                    to[x1, 0:8] = jnp.where(sub < 4, pltpu.roll(lower, 4, 0), source[OFF + x1, 8:16])
                    to[x0, 8:16] = jnp.where(sub < 4, source[OFF + x0, 40:48], pltpu.roll(upper, 4, 0))
                    to[x1, 8:16] = jnp.where(sub < 4, source[OFF + x1, 40:48], upper)
        return 0

    lax.fori_loop(0, 3, assemble, 0)
    all_strips(field, coef, (2, 0, 0, 0, 32), low, high)
    for comp in range(9):
        low[comp, 8:32] = middle_low[comp, 8:32]
        high[comp, 8:32] = middle_high[comp, 8:32]
    for n in range(5):
        down, up = low[n], high[n]
        if n < 4:
            down, up = down + pltpu.roll(low[n + 5], 124, 1), up + pltpu.roll(high[n + 5], 4, 1)
        send_low[n] = down
        send_high[n] = up


def at(ref, dy=0):
    return ref[pl.ds(LO + dy, ROWS), :]


def put(ref, value):
    ref[pl.ds(LO, ROWS), :] = value


def diagonals(m, c, cy, cx, cz, mx, my, mz):
    d0 = m[0] + c[1] + cz[1] + c[2] + cy[2]
    d1 = m[1] + c[2] + cx[2] + c[0] + cz[0]
    d2 = m[2] + c[0] + cy[0] + c[1] + cx[1]
    dn = m[0] + mx + m[1] + my + m[2] + mz
    return 1.0 / d0, 1.0 / d1, 1.0 / d2, 1.0 / dn


def invert(field_middle, coef_middle, field_edge, coef_edge, field, coef, diag, node):
    def assemble(c, _):
        coef[c, OFF - 1] = jnp.zeros((Y, 128), jnp.float32)
        for x in range(OFF, OFF + 16):
            coef[c, x, 0:8] = jnp.zeros((8, 128), jnp.float32)
            coef[c, x, 16:40] = coef_middle[c, x, 16:40]
            coef[c, x, 8:16] = coef_edge[c, x - OFF, 0:8]
            coef[c, x, 40:48] = coef_edge[c, x - OFF, 8:16]
        return 0

    def assemble_field(c, _):
        for x in range(OFF, OFF + 16):
            field[c, x, 16:40] = field_middle[c, x, 16:40]
            field[c, x, 8:16] = field_edge[c, x - OFF, 0:8]
            field[c, x, 40:48] = field_edge[c, x - OFF, 8:16]
        return 0

    lax.fori_loop(0, 6, assemble, 0)
    lax.fori_loop(0, 3, assemble_field, 0)

    def row(x, _):
        i = x + OFF
        m = [at(coef.at[c, i]) for c in range(3)]
        c_ = [at(coef.at[3 + c, i]) for c in range(3)]
        cy = [at(coef.at[3 + c, i], -1) for c in range(3)]
        cx = [at(coef.at[3 + c, i - 1]) for c in range(3)]
        cz = [pltpu.roll(c_[c], 1, 1) for c in range(2)]
        out = diagonals(m, c_, cy, cx, cz, at(coef.at[0, i - 1]), at(coef.at[1, i], -1), pltpu.roll(m[2], 1, 1))
        for c in range(3):
            put(diag.at[c, i], out[c])
        put(node.at[i], out[3])
        return 0

    lax.fori_loop(0, 16, row, 0)


def main(field_in, coef, diag_in, node_in, zown_low, zown_high, zlow, zhigh, field, precond, partial, sink,
         diag, node, s, phi, g, fieldS, coefS, diagS, nodeS, sS, phiS, gS, dots):
    f32 = jnp.float32
    lane = lax.broadcasted_iota(jnp.int32, (ROWS, 128), 1)
    first_lane, last_lane = lane == 0, lane == 127
    below_half = lax.broadcasted_iota(jnp.int32, (8, 128), 0) < 4

    def z_up(value, strip, x):
        return jnp.where(last_lane, pltpu.roll(strip, (123 - 8 * x) & 127, 1), pltpu.roll(value, 127, 1))

    def z_down(value, strip, x):
        return jnp.where(first_lane, pltpu.roll(strip, (125 - 8 * x) & 127, 1), pltpu.roll(value, 1, 1))

    upper = (lane & 4) != 0
    for comp in range(9):
        lower_part, upper_part = zlow[comp % 5], zhigh[comp % 5]
        if comp >= 5:
            lower_part, upper_part = pltpu.roll(lower_part, 124, 1), pltpu.roll(upper_part, 4, 1)
        for t, value in ((0, jnp.where(upper, zown_low[comp], lower_part)),
                         (1, jnp.where(upper, upper_part, zown_high[comp]))):
            put(fieldS.at[0, comp, t] if comp < 3 else coefS.at[comp - 3, t], value)
            if comp >= 3:
                coefS[comp - 3, t, 0:8] = jnp.zeros((8, 128), f32)

    def setup_strip(t, _):
        m = [at(coefS.at[c, t]) for c in range(3)]
        c_ = [at(coefS.at[3 + c, t]) for c in range(3)]
        cy = [at(coefS.at[3 + c, t], -1) for c in range(3)]
        cx = [jnp.where(lane < 8, 0.0, pltpu.roll(v, 8, 1)) for v in c_]
        cz = [jnp.where((lane & 7) == 0, 0.0, pltpu.roll(v, 1, 1)) for v in c_]
        out = diagonals(m, c_, cy, cx, cz, pltpu.roll(m[0], 8, 1), at(coefS.at[1, t], -1), pltpu.roll(m[2], 1, 1))
        for c in range(3):
            put(diagS.at[c, t], out[c])
        put(nodeS.at[t], out[3])
        return 0

    for t in range(2):
        setup_strip(t, 0)

    def setup(n, _):
        ready = []
        for x in (4 * n, 4 * n + 1, 4 * n + 2, 4 * n + 3):
            i = x + OFF
            ready.append((i, [at(field_in.at[c, i]) for c in range(3)], [
                jnp.where(first_lane, pltpu.roll(at(diagS.at[c, 0]), 124 - 8 * x, 1), at(diag_in.at[c, i]))
                for c in range(3)], jnp.where(first_lane, pltpu.roll(at(nodeS.at[0]), 124 - 8 * x, 1), at(node_in.at[i]))))
        for i, fields, diags, nodes in ready:
            for c in range(3):
                put(field.at[0, c, i], fields[c])
                put(diag.at[c, i], diags[c])
            put(node.at[i], nodes)
        return 0

    lax.fori_loop(0, 4, setup, 0)

    def fluxes(coefs, e, e0y, e0z, e1x, e1z, e2x, e2y):
        return (coefs[0] * ((e2y - e[2]) - (e1z - e[1])),
                coefs[1] * ((e0z - e[0]) - (e2x - e[2])),
                coefs[2] * ((e1x - e[1]) - (e0y - e[0])))

    def curl_back(gv, g0y, g0z, g1x, g1z, g2x, g2y):
        return ((g1z - gv[1]) - (g2y - gv[2]), (g2x - gv[2]) - (g0z - gv[0]), (g0y - gv[0]) - (g1x - gv[1]))

    def operator_step(k, _):
        now, later, before = k, k + 1, jnp.maximum(k - 1, 0)
        weight = jnp.where(k == 0, 0.0, jnp.where(k == 1, 0.5, 0.25))

        pending = []

        def hold(ref, value):
            pending.append((ref, value))

        def strip_first(t, _):
            r = [at(fieldS.at[now, c, t]) for c in range(3)]
            q = ((pltpu.roll(r[0], 8, 1) - r[0]) + (at(fieldS.at[now, 1, t], -1) - r[1])) + (pltpu.roll(r[2], 1, 1) - r[2])
            hold(phiS.at[t], q * at(nodeS.at[t]))
            for c in range(3):
                hold(sS.at[c, t], r[c] * at(diagS.at[c, t]))
            return 0

        def strip_second(t, _):
            e = [at(sS.at[c, t]) for c in range(3)]
            out = fluxes([at(coefS.at[3 + c, t]) for c in range(3)], e,
                         at(sS.at[0, t], 1), pltpu.roll(e[0], 127, 1), pltpu.roll(e[1], 120, 1),
                         pltpu.roll(e[1], 127, 1), pltpu.roll(e[2], 120, 1), at(sS.at[2, t], 1))
            for c in range(3):
                hold(gS.at[c, t], out[c])
            return 0

        def strip_third(t, _):
            gv = [at(gS.at[c, t]) for c in range(3)]
            w = curl_back(gv, at(gS.at[0, t], -1), pltpu.roll(gv[0], 1, 1), pltpu.roll(gv[1], 8, 1),
                          pltpu.roll(gv[1], 1, 1), pltpu.roll(gv[2], 8, 1), at(gS.at[2, t], -1))
            p = at(phiS.at[t])
            up = (pltpu.roll(p, 120, 1), at(phiS.at[t], 1), pltpu.roll(p, 127, 1))
            for c in range(3):
                u = at(sS.at[c, t]) + (up[c] - p)
                hold(fieldS.at[later, c, t], (w[c] + at(coefS.at[c, t]) * u - at(fieldS.at[now, c, t]))
                    - weight * at(fieldS.at[before, c, t]))
            return 0

        for part in (strip_first, strip_second, strip_third):
            pending.clear()
            for t in range(2):
                part(t, 0)
            for ref, value in pending:
                put(ref, value)

        ready = []
        for n_row in range(2):
            x = n_row + k
            b = x + OFF
            f = [at(field.at[now, c, b]) for c in range(3)]
            q = ((at(field.at[now, 0, b - 1]) - f[0]) + (at(field.at[now, 1, b], -1) - f[1])) + (
                z_down(f[2], at(fieldS.at[now, 2, 0]), x) - f[2])
            ready.append((b, [f[c] * at(diag.at[c, b]) for c in range(3)], q * at(node.at[b])))
        for b, scaled, potential in ready:
            for c in range(3):
                put(s.at[c, b], scaled[c])
            put(phi.at[b], potential)

        def read(x):
            i = x + OFF
            g_own = [at(g.at[c, i]) for c in range(3)]
            g_x = [at(g.at[c, i - 1]) for c in (1, 2)]
            g_y = [at(g.at[c, i], -1) for c in (0, 2)]
            p, p_x, p_y = at(phi.at[i]), at(phi.at[i + 1]), at(phi.at[i], 1)
            s_own = [at(s.at[c, i]) for c in range(3)]
            r = [at(field.at[now, c, i]) for c in range(3)]
            old = [at(field.at[before, c, i]) for c in range(3)]
            mass = [at(coef.at[c, i]) for c in range(3)]
            a = i + 2
            e = [at(s.at[c, a]) for c in range(3)]
            e_x = [at(s.at[c, a + 1]) for c in (1, 2)]
            e_y = [at(s.at[c, a], 1) for c in (0, 2)]
            curl = [at(coef.at[3 + c, a]) for c in range(3)]
            b = i + 5
            f = [at(field.at[now, c, b]) for c in range(3)]
            f_x, f_y = at(field.at[now, 0, b - 1]), at(field.at[now, 1, b], -1)
            inverse, inverse_node = [at(diag.at[c, b]) for c in range(3)], at(node.at[b])
            strip = (at(gS.at[0, 0]), at(gS.at[1, 0]), at(phiS.at[1]), at(sS.at[0, 1]), at(sS.at[1, 1]),
                     at(fieldS.at[now, 2, 0]))
            return (g_own, g_x, g_y, p, p_x, p_y, s_own, r, old, mass, e, e_x, e_y, curl, f, f_x, f_y, inverse,
                    inverse_node, strip)

        def work(x, values):
            (g_own, g_x, g_y, p, p_x, p_y, s_own, r, old, mass, e, e_x, e_y, curl, f, f_x, f_y, inverse,
             inverse_node, strip) = values
            w = curl_back(g_own, g_y[0], z_down(g_own[0], strip[0], x), g_x[0],
                          z_down(g_own[1], strip[1], x), g_x[1], g_y[1])
            up = (p_x, p_y, z_up(p, strip[2], x))
            u = [s_own[c] + (up[c] - p) for c in range(3)]
            v = [((w[c] + mass[c] * u[c]) - r[c]) - weight * old[c] for c in range(3)]
            flux = fluxes(curl, e, e_y[0], z_up(e[0], strip[3], x + 2), e_x[0],
                          z_up(e[1], strip[4], x + 2), e_x[1], e_y[1])
            q = ((f_x - f[0]) + (f_y - f[1])) + (z_down(f[2], strip[5], x + 5) - f[2])
            return r, u, v, flux, q * inverse_node, [f[c] * inverse[c] for c in range(3)]

        def write(x, results, sums):
            r, u, v, flux, potential, scaled = results
            i = x + OFF
            inside = (x >= 4) & (x < 12)
            to = jnp.where(inside, x - 4, 8)
            for c in range(3):
                put(field.at[later, c, i], v[c])
                put(g.at[c, i + 2], flux[c])
                put(s.at[c, i + 5], scaled[c])
            put(phi.at[i + 5], potential)
            sums = list(sums)
            for c in range(3):
                precond[k, c, to] = u[c]
                for n, prod in ((0, r[c] * u[c]), (1, v[c] * u[c])):
                    ends = jnp.where(below_half, prod[32:40], prod[0:8])
                    part = ((prod[8:16] + prod[16:24]) + prod[24:32]) + ends
                    sums[n] = sums[n] + jnp.where(inside, part, 0.0)
            return tuple(sums)

        def rows(n, sums):
            x = 2 * n + k - 3
            first, second = read(x), read(x + 1)
            first, second = work(x, first), work(x + 1, second)
            return write(x + 1, second, write(x, first, sums))

        zero = jnp.zeros((8, 128), f32)
        sums = lax.fori_loop(0, 9 - k, rows, (zero, zero))
        dots[2 * k] = sums[0]
        dots[2 * k + 1] = sums[1]
        return 0

    lax.fori_loop(0, 4, operator_step, 0)

    row_lane = lax.broadcasted_iota(jnp.int32, (1, 128), 1) // 16
    parts = [jnp.sum(dots[d], axis=0, keepdims=True) for d in range(8)]
    for shift in (64, 32, 16):
        parts = [t + pltpu.roll(t, shift, 1) for t in parts]
    moments = parts[0]
    for d in range(1, 8):
        moments = jnp.where(row_lane == d, parts[d], moments)
    partial[...] = jnp.broadcast_to(moments, partial.shape)

    def look(x, _):
        for c in range(3):
            sink[x, c] = s[c, x + OFF, 16:24] + g[c, x + OFF, 16:24]
        sink[x, 3] = phi[x + OFF, 16:24]
        return 0

    lax.fori_loop(0, 2, look, 0)


def finish(everyone, field, precond, solution_out, residual_out):
    total = jnp.sum(everyone[...], axis=0, keepdims=True)
    lane = lax.broadcasted_iota(jnp.int32, (1, 128), 1)
    dots = [jnp.broadcast_to(jnp.sum(jnp.where(lane // 16 == d, total, 0.0), axis=1, keepdims=True), (8, 128))
            for d in range(8)]
    size = [1.0] + [2.0 ** (1 - k) for k in range(1, 9)]
    moment = [dots[0], dots[1]]
    for k in range(1, 4):
        moment.append((dots[2 * k] * (2.0 / size[k] ** 2) - moment[0]) * size[2 * k])
        moment.append((dots[2 * k + 1] * (2.0 / (size[k] * size[k + 1])) - moment[1]) * size[2 * k + 1])
    row, earlier = moment, None
    alpha, beta = [row[1] / row[0]], [None]
    for k in range(1, 4):
        following = [None] * 8
        for l in range(k, 8 - k):
            t = row[l + 1] - alpha[k - 1] * row[l] + WEIGHT[l if l < 2 else 2] * row[l - 1]
            if k > 1:
                t = t - beta[k - 1] * earlier[l]
            following[l] = t
        alpha.append(following[k + 1] / following[k] - row[k] / row[k - 1])
        beta.append(following[k] / row[k - 1])
        row, earlier = following, row
    zero = jnp.zeros((8, 128), jnp.float32)
    older, newer = [zero] * 6, [zero + 1.0] + [zero] * 5
    value_older, value = zero, zero + 1.0
    weight = lambda l: WEIGHT[min(l, 2)]
    for k in range(4):
        nxt = []
        for l in range(6):
            t = -alpha[k] * newer[l]
            if l > 0:
                t = t + newer[l - 1]
            if l < 5:
                t = t + weight(l + 1) * newer[l + 1]
            if k > 0:
                t = t - beta[k] * older[l]
            nxt.append(t)
        step = (-1.0 - alpha[k]) * value
        if k > 0:
            step = step - beta[k] * value_older
        older, newer, value_older, value = newer, nxt, value, step
    inverse = 1.0 / value
    e = [newer[l] * inverse for l in range(5)]
    S = [None] * 4
    S[3] = -e[4]
    S[2] = -e[3] - S[3]
    S[1] = -e[2] - S[2] - weight(3) * S[3]
    S[0] = -e[1] - S[1] - weight(2) * S[2]
    e = [v[0:1] for v in e]
    S = [v[0:1] for v in S]

    def combine(x, _):
        rows, first = pl.ds(OWN, 32), pl.ds(OWN - LO, 32)
        for c in range(3):
            v = [field[k, c, x + OFF + 4, rows, :] for k in range(5)]
            u = [precond[k, c, x, first, :] for k in range(4)]
            residual_out[c, x] = (e[0] * v[0] + e[1] * v[1]) + (e[2] * v[2] + e[3] * v[3]) + e[4] * v[4]
            solution_out[c, x] = (S[0] * u[0] + S[1] * u[1]) + (S[2] * u[2] + S[3] * u[3])
        return 0

    lax.fori_loop(0, 8, combine, 0)


def shape(*dims):
    return jax.ShapeDtypeStruct(dims, jnp.float32)


def call(kernel, outs, ins, mib, scratch=(), flops=1000000):
    return pl.pallas_call(
        kernel, out_shape=outs, in_specs=[VMEM] * len(ins), out_specs=jax.tree.map(lambda _: VMEM, outs),
        scratch_shapes=list(scratch),
        compiler_params=pltpu.CompilerParams(vmem_limit_bytes=mib << 20),
        cost_estimate=pl.CostEstimate(flops=flops, bytes_accessed=1 << 20, transcendentals=0))(*ins)


def exchange(low, high, axis):
    n = lax.axis_size(axis)
    up = [(i, (i + 1) % n) for i in range(n)]
    return lax.ppermute(high, axis, up), lax.ppermute(low, axis, [(j, i) for i, j in up])


def body(right, mass, curl):
    face = (shape(3, 8, 32, 128),) + (shape(3, 4, 32, 128),) * 2
    b, *ends = call(load, face, (right,), 8)
    b = (b,) + exchange(*ends, "gx")
    c, *ends = call(load, face, (curl,), 8)
    c = (c,) + exchange(*ends, "gx")
    m, *ends = call(load_mass, face, (mass, c[0]), 8)
    m = (m,) + exchange(*ends, "gx")
    ends = (shape(9, 4, 8, 128),) * 2
    y_own = exchange(*call(pack_y_own, ends, (b[0], m[0], c[0]), 8), "gy")
    columns = (shape(9, ROWS, 128),) * 2
    extended = (shape(3, X, Y, 128), shape(6, X, Y, 128))
    own = call(pack_z_own, columns + (shape(3, 8, ROWS, 128), shape(6, 8, ROWS, 128)), (b[0], m[0], c[0]), 8, flops=20000000)
    y_halo = exchange(*call(pack_y_halo, ends, (own[0],) + b[1:] + m[1:] + c[1:], 8), "gy")
    low, high, *middle = call(pack_z_middle, columns + extended, b[1:] + m[1:] + c[1:] + tuple(own), 8, flops=20000000)
    low, high, *ends, field, coef = call(
        pack_z_edge, columns + (shape(5, ROWS, 128),) * 2 + (shape(3, 16, 16, 128), shape(6, 16, 16, 128)),
        y_own + y_halo + (low, high, *middle), 8)
    sides = (low, high) + exchange(*ends, "gz")
    block = call(invert, extended + (shape(3, X, Y, 128), shape(X, Y, 128)), (*middle, field, coef), 8, flops=20000000)

    def held(*dims):
        return pltpu.VMEM(dims + (Y, 128), jnp.float32)

    axes = ("gx", "gy", "gz")
    devices = lax.axis_size(axes)
    vectors, precond, rows, _ = call(
        main, (shape(5, 3, X, Y, 128), shape(4, 3, 9, ROWS, 128), shape(devices, 128), shape(2, 4, 8, 128)),
        tuple(block) + sides, 20,
        [held(3, X), held(X), held(3, X), held(X), held(3, X),
         held(5, 3, 2), held(6, 2), held(3, 2), held(2), held(3, 2), held(2), held(3, 2), pltpu.VMEM((8, 8, 128), jnp.float32)])
    everyone = lax.all_to_all(rows.reshape(devices, 1, 128), axes, 0, 0, tiled=True).reshape(devices, 128)
    return call(finish, (shape(3, 8, 32, 128),) * 2, (everyone, vectors, precond), 16)


def solution(mesh):
    spec = P(None, "gx", "gy", "gz")
    return jax.shard_map(body, mesh=mesh, in_specs=(spec,) * 3, out_specs=(spec,) * 2, check_vma=False)
```
